32 devices in a mesh: dp: 1 (over z), tp: 4 (over y), cp: 8 (over x, core).
Axes of the slice: x: 4, y: 4, z: 1, core: 2. Of those that a mesh axis runs over, the one named last changes fastest.
The devices are a block of a 4x4x8 slice.
Arguments:
- x: bfloat16 [4096, 5120], P(('dp', 'cp'))
- doc_ids: int32 [4096], P(('dp', 'cp'))
- w_query: bfloat16 [5120, 4096], P(None, 'tp')
- w_key: bfloat16 [5120, 1024], P(None, 'tp')
- w_value: bfloat16 [5120, 1024], P(None, 'tp')
- w_out: bfloat16 [4096, 5120], P('tp')
Outputs:
- output: bfloat16 [4096, 5120], P(('dp', 'cp'))
All inputs are finite; a program needn't handle non-finite values.
Results may differ from the reference program's by a relative error of at most 0.00717162.
Values are sent between devices in bfloat16 or wider.
A program may use at most 768 MiB of HBM per device.

```python
import jax
import jax.numpy as jnp
from jax import lax

SEQ_LEN = 4096
BLOCK_LEN = 256
DOC_BREAKS = 32
D = 5120
HEADS = 32
KV_HEADS = 8
HEAD = 128


def setup_inputs(seed: int = 0, part: int = 0) -> dict:
    shared_keys = jax.random.split(jax.random.key(seed), 4)
    part_keys = jax.random.split(jax.random.fold_in(jax.random.key(seed + 1), part), 4)
    x = jax.random.normal(part_keys[0], (SEQ_LEN, D), jnp.float32).astype(jnp.bfloat16)
    span_len = jax.random.randint(part_keys[1], (), SEQ_LEN // 3, 2 * SEQ_LEN // 3 + 1)
    span_start = jax.random.randint(part_keys[2], (), 0, SEQ_LEN - span_len + 1)
    breaks = jax.random.randint(part_keys[3], (DOC_BREAKS,), 1, SEQ_LEN)
    inside = (breaks > span_start) & (breaks < span_start + span_len)
    start_flags = jnp.zeros((SEQ_LEN,), jnp.int32).at[breaks].add(jnp.where(inside, 0, 1))
    doc_ids = jnp.cumsum(start_flags).astype(jnp.int32)
    w_query = (jax.random.normal(shared_keys[0], (D, HEADS * HEAD), jnp.float32) * (1.5 / D ** 0.5)).astype(jnp.bfloat16)
    w_key = (jax.random.normal(shared_keys[1], (D, KV_HEADS * HEAD), jnp.float32) * (1.5 / D ** 0.5)).astype(jnp.bfloat16)
    w_value = (jax.random.normal(shared_keys[2], (D, KV_HEADS * HEAD), jnp.float32) / D ** 0.5).astype(jnp.bfloat16)
    w_out = (jax.random.normal(shared_keys[3], (HEADS * HEAD, D), jnp.float32) * (2.0 / (HEADS * HEAD) ** 0.5)).astype(jnp.bfloat16)
    return {'x': x, 'doc_ids': doc_ids, 'w_query': w_query, 'w_key': w_key, 'w_value': w_value, 'w_out': w_out}


def block_update(soft_state, q_blk, k_blk, v_blk, allowed):
    run_max, run_sum, out_acc = soft_state
    scores = jnp.einsum('qhgd,khd->qhgk', q_blk.astype(jnp.float32), k_blk.astype(jnp.float32)) * (HEAD ** -0.5)
    scores = jnp.where(allowed[:, None, None, :], scores, -jnp.inf)
    new_max = jnp.maximum(run_max, jnp.max(scores, axis=-1))
    safe_max = jnp.where(new_max == -jnp.inf, 0.0, new_max)
    prob_vals = jnp.exp(scores - safe_max[..., None])
    rescale = jnp.exp(run_max - safe_max)
    run_sum = run_sum * rescale + jnp.sum(prob_vals, axis=-1)
    out_acc = out_acc * rescale[..., None] + jnp.einsum('qhgk,khd->qhgd', prob_vals, v_blk.astype(jnp.float32))
    return new_max, run_sum, out_acc


def reference(x, doc_ids, w_query, w_key, w_value, w_out):
    q_per_kv = HEADS // KV_HEADS
    n_blocks = SEQ_LEN // BLOCK_LEN
    q_all = jnp.dot(x, w_query, preferred_element_type=jnp.float32).astype(jnp.bfloat16).reshape(n_blocks, BLOCK_LEN, KV_HEADS, q_per_kv, HEAD)
    k_all = jnp.dot(x, w_key, preferred_element_type=jnp.float32).astype(jnp.bfloat16).reshape(n_blocks, BLOCK_LEN, KV_HEADS, HEAD)
    v_all = jnp.dot(x, w_value, preferred_element_type=jnp.float32).astype(jnp.bfloat16).reshape(n_blocks, BLOCK_LEN, KV_HEADS, HEAD)
    seg_blocks = doc_ids.reshape(n_blocks, BLOCK_LEN)
    pos_blocks = jnp.arange(SEQ_LEN).reshape(n_blocks, BLOCK_LEN)

    def query_block(q_inputs):
        q_blk, seg_q, pos_q = q_inputs

        def key_step(soft_state, k_inputs):
            k_blk, v_blk, seg_k, pos_k = k_inputs
            active = (pos_k[0] <= pos_q[BLOCK_LEN - 1]) & (seg_k[BLOCK_LEN - 1] >= seg_q[0])
            allowed = (seg_q[:, None] == seg_k[None, :]) & (pos_q[:, None] >= pos_k[None, :])
            new_state = lax.cond(active, lambda same_state: block_update(same_state, q_blk, k_blk, v_blk, allowed), lambda same_state: same_state, soft_state)
            return new_state, None

        init_state = (jnp.full((BLOCK_LEN, KV_HEADS, q_per_kv), -jnp.inf, jnp.float32), jnp.zeros((BLOCK_LEN, KV_HEADS, q_per_kv), jnp.float32), jnp.zeros((BLOCK_LEN, KV_HEADS, q_per_kv, HEAD), jnp.float32))
        final_state = lax.scan(key_step, init_state, (k_all, v_all, seg_blocks, pos_blocks))[0]
        run_sum = final_state[1]
        out_acc = final_state[2]
        return (out_acc / run_sum[..., None]).astype(jnp.bfloat16).reshape(BLOCK_LEN, HEADS * HEAD)

    heads_out = lax.map(query_block, (q_all, seg_blocks, pos_blocks)).reshape(SEQ_LEN, HEADS * HEAD)
    return jnp.dot(heads_out, w_out, preferred_element_type=jnp.float32).astype(jnp.bfloat16)
```

```python
import functools

import jax
import jax.numpy as jnp
from jax import lax
from jax.experimental import pallas as pl
from jax.experimental.pallas import tpu as pltpu
from jax.sharding import PartitionSpec as P

HEAD_DIM = 128
COL_TILE = 256
MESH = pl.DeviceIdType.MESH
SCALE = HEAD_DIM**-0.5 * 1.4426950408889634
NEG_INF = float("-inf")


class Sems:
    def __init__(self, ref):
        self.ref, self.names = ref, {}

    def __getitem__(self, name):
        return self.ref.at[self.names.setdefault(name, len(self.names))]


def kernel(tp, cp, x_hbm, seg_in, wq_hbm, wk_hbm, wv_hbm, wo_hbm, y_hbm,
           x_v, wkv_v, wq_v, w_full, kv_all, segs, seg_col, q_v, o_all, y_own, relay_up, relay_dn,
           m_s, l_s, acc_s, load_sem, send_sem, recv_sem):
    t, p = lax.axis_index("tp"), lax.axis_index("cp")
    chips = cp // 2
    col, core = p // 2, lax.rem(p, 2)
    up, dn, far = lax.rem(t + 1, tp), lax.rem(t + tp - 1, tp), lax.rem(t + 2, tp)
    right_chip, left_chip, far_chip = lax.rem(col + 1, chips), lax.rem(col + chips - 1, chips), lax.rem(col + 2, chips)
    right, left, across = right_chip * 2 + core, left_chip * 2 + core, far_chip * 2 + core
    mate = col * 2 + 1 - core
    mate_right, mate_left, mate_across = right_chip * 2 + 1 - core, left_chip * 2 + 1 - core, far_chip * 2 + 1 - core

    rows = x_v.shape[0]
    heads = q_v.shape[0]
    groups = kv_all.shape[1]
    per_group = heads // groups
    head_cols = heads * HEAD_DIM
    y_cols = y_own.shape[1]
    piece = head_cols // cp
    half = piece // 2
    half_rows = rows // 2

    loads, sends, recvs = Sems(load_sem), Sems(send_sem), Sems(recv_sem)
    waiting = []

    def at_tp(i):
        return {"tp": i, "cp": p}

    def at_cp(i):
        return {"tp": t, "cp": i}

    def send(src, dst, name, dev):
        c = pltpu.make_async_remote_copy(src_ref=src, dst_ref=dst, send_sem=sends[(name, len(waiting))],
                                         recv_sem=recvs[name], device_id=dev, device_id_type=MESH)
        c.start()
        waiting.append(c)

    def arrived(dst, name):
        pltpu.make_async_remote_copy(src_ref=dst, dst_ref=dst, send_sem=sends[0], recv_sem=recvs[name],
                                     device_id=at_cp(p), device_id_type=MESH).wait_recv()

    def load(src, dst, name):
        c = pltpu.make_async_copy(src, dst, loads[name])
        c.start()
        return c

    load_x = load(x_hbm, x_v, "x")
    load_k = load(wk_hbm, wkv_v.at[0], "k")
    load_v = load(wv_hbm, wkv_v.at[1], "v")
    q_tiles = head_cols // COL_TILE
    load_q = [load(wq_hbm.at[:, pl.ds(n * COL_TILE, COL_TILE)], wq_v.at[n], ("q", n)) for n in range(q_tiles)]
    own_cols = pl.ds(pl.multiple_of(t * y_cols, 128), y_cols)
    load_o = load(wo_hbm.at[:, own_cols], w_full.at[pl.ds(pl.multiple_of(t * head_cols, 128), head_cols), :], "o")

    barrier = pltpu.get_barrier_semaphore()
    peers = [at_tp(up), at_tp(dn)] + [at_cp(lax.rem(p + k, cp)) for k in range(1, cp)]
    for dev in peers:
        pl.semaphore_signal(barrier, inc=1, device_id=dev, device_id_type=MESH)
    pl.semaphore_wait(barrier, len(peers))

    for k in range(1, cp):
        send(seg_in, segs.at[p], ("seg", k), at_cp(lax.rem(p + k, cp)))
    load_seg = load(seg_in, segs.at[p], "seg")

    def w_rows(owner, share, k=None):
        start = owner * head_cols + share * piece
        if k is None:
            return w_full.at[pl.ds(pl.multiple_of(start, 16), piece), :]
        return w_full.at[pl.ds(pl.multiple_of(start + k * half, 16), half), :]

    def w_src(dest, k=None):
        cols = pl.ds(pl.multiple_of(dest * y_cols, 128), y_cols)
        if k is None:
            return wo_hbm.at[pl.ds(pl.multiple_of(p * piece, 16), piece), cols]
        return wo_hbm.at[pl.ds(pl.multiple_of(p * piece + k * half, 16), half), cols]

    send(w_src(far, 0), relay_up, "w_relay_up", at_tp(up))
    send(w_src(far, 1), relay_dn, "w_relay_dn", at_tp(dn))
    send(w_src(up), w_rows(t, p), "w_from_dn", at_tp(up))
    send(w_src(dn), w_rows(t, p), "w_from_up", at_tp(dn))

    def ring_start(part, tag):
        send(part(p), part(p), (tag, "L"), at_cp(right))
        send(part(p), part(p), (tag, "R"), at_cp(left))
        send(part(p), part(p), (tag, "M"), at_cp(mate))

    def ring_near(part, tag):
        arrived(part(left), (tag, "L"))
        send(part(left, 0), part(left, 0), (tag, "far0"), at_cp(right))
        send(part(left), part(left), (tag, "ML"), at_cp(mate))
        arrived(part(right), (tag, "R"))
        send(part(right, 1), part(right, 1), (tag, "far1"), at_cp(left))
        send(part(right), part(right), (tag, "MR"), at_cp(mate))

    def ring_far(part, tag):
        arrived(part(across, 0), (tag, "far0"))
        arrived(part(across, 1), (tag, "far1"))
        send(part(across), part(across), (tag, "MF"), at_cp(mate))

    def kv_part(g):
        return lambda owner, k=None: kv_all.at[owner, g] if k is None else kv_all.at[owner, g, k]

    def project(w_ref, store):
        @pl.loop(0, rows // half_rows)
        def _(i):
            r = pl.ds(pl.multiple_of(i * half_rows, 16), half_rows)
            store(r, jnp.dot(x_v[r, :], w_ref[...], preferred_element_type=jnp.float32).astype(jnp.bfloat16))

    load_x.wait()
    load_k.wait()

    def store_k(kind):
        def store(r, val):
            for g in range(groups):
                kv_all[p, g, kind, r, :] = val[:, g * HEAD_DIM:(g + 1) * HEAD_DIM]
        return store

    project(wkv_v.at[0], store_k(0))
    load_v.wait()
    project(wkv_v.at[1], store_k(1))
    ring_start(kv_part(0), ("kv", 0))

    def q_tile(n):
        load_q[n].wait()

        def store(r, val):
            for k in range(COL_TILE // HEAD_DIM):
                q_v[n * (COL_TILE // HEAD_DIM) + k, r, :] = val[:, k * HEAD_DIM:(k + 1) * HEAD_DIM]
        project(wq_v.at[n], store)

    q_tile(0)
    arrived(relay_up, "w_relay_up")
    send(relay_up, w_rows(dn, p, 0), "w_far0", at_tp(up))
    arrived(relay_dn, "w_relay_dn")
    send(relay_dn, w_rows(up, p, 1), "w_far1", at_tp(dn))
    for n in range(1, q_tiles):
        q_tile(n)

    seg_col[...] = jnp.broadcast_to(seg_in[...], (HEAD_DIM, rows)).T

    def wide(v, n):
        return jnp.concatenate([v] * (n // v.shape[1]), axis=1)

    def visit(g, block, diagonal):
        seg_k = segs[block]

        @pl.loop(0, per_group)
        def _(h):
            for i in range(2):
                r = slice(i * half_rows, (i + 1) * half_rows)
                s = lax.dot_general(q_v[g * per_group + h, r, :], kv_all[block, g, 0], (((1,), (1,)), ((), ())),
                                    preferred_element_type=jnp.float32)
                allowed = wide(seg_col[r, :], rows) == seg_k
                if diagonal:
                    allowed &= (lax.broadcasted_iota(jnp.int32, s.shape, 0) + i * half_rows
                                >= lax.broadcasted_iota(jnp.int32, s.shape, 1))
                s = jnp.where(allowed, s * SCALE, NEG_INF)
                top = jnp.max(s, axis=1, keepdims=True)
                if diagonal:
                    new_max = jnp.broadcast_to(top, (half_rows, HEAD_DIM))
                else:
                    old_max = m_s[h, r, :]
                    new_max = jnp.maximum(old_max, top)
                prob = jnp.exp2(s - wide(new_max, rows))
                part = prob[:, :HEAD_DIM]
                for k in range(1, rows // HEAD_DIM):
                    part += prob[:, k * HEAD_DIM:(k + 1) * HEAD_DIM]
                out = jnp.dot(prob.astype(jnp.bfloat16), kv_all[block, g, 1], preferred_element_type=jnp.float32)
                if not diagonal:
                    rescale = jnp.exp2(old_max - new_max)
                    part += l_s[h, r, :] * rescale
                    out += acc_s[h, r, :] * rescale
                m_s[h, r, :] = new_max
                l_s[h, r, :] = part
                acc_s[h, r, :] = out

    def visit_chip(g, first_chip, both):
        chips_here = [first_chip] if both is None else [first_chip, both]

        @pl.loop(0, 2 * len(chips_here))
        def _(i):
            chip = chips_here[0] if both is None else jnp.where(i < 2, chips_here[0], chips_here[1])
            block = chip * 2 + lax.rem(i, 2)

            @pl.when(block < p)
            def _():
                visit(g, block, False)

    def o_cols(owner, h):
        return o_all.at[:, pl.ds(pl.multiple_of(owner * head_cols + h * HEAD_DIM, 128), HEAD_DIM)]

    def o_relay(h):
        arrived(o_cols(dn, h), ("o", h, "D"))
        arrived(o_cols(up, h), ("o", h, "U"))
        if h % 2 == 0:
            send(o_cols(dn, h), o_cols(dn, h), ("o", h, "F"), at_tp(up))
        else:
            send(o_cols(up, h), o_cols(up, h), ("o", h, "F"), at_tp(dn))

    load_seg.wait()
    for k in range(1, cp):
        arrived(segs.at[lax.rem(p + cp - k, cp)], ("seg", k))

    for g in range(groups):
        part, tag = kv_part(g), ("kv", g)
        visit(g, p, True)
        ring_near(part, tag)
        if g + 1 < groups:
            ring_start(kv_part(g + 1), ("kv", g + 1))
        arrived(part(mate), (tag, "M"))
        arrived(part(mate_left), (tag, "ML"))
        arrived(part(mate_right), (tag, "MR"))

        @pl.when(core == 1)
        def _():
            visit(g, mate, False)
        visit_chip(g, left_chip, right_chip)
        ring_far(part, tag)
        arrived(part(mate_across), (tag, "MF"))
        visit_chip(g, far_chip, None)
        for k in range(per_group):
            h = g * per_group + k
            total = jnp.sum(l_s[k], axis=1, keepdims=True)
            o_all[:, pl.ds(pl.multiple_of(t * head_cols + h * HEAD_DIM, 128), HEAD_DIM)] = (
                acc_s[k] / total).astype(jnp.bfloat16)
            send(o_cols(t, h), o_cols(t, h), ("o", h, "D"), at_tp(up))
            send(o_cols(t, h), o_cols(t, h), ("o", h, "U"), at_tp(dn))
        if g == 0:
            arrived(w_rows(dn, p), "w_from_dn")
            arrived(w_rows(up, p), "w_from_up")
            arrived(w_rows(far, p, 0), "w_far0")
            arrived(w_rows(far, p, 1), "w_far1")
            for j in range(1, tp):
                ring_start(w_part(w_rows, lax.rem(t + j, tp)), ("w", j))

    w_parts = [(w_part(w_rows, lax.rem(t + j, tp)), ("w", j)) for j in range(1, tp)]
    for part, tag in w_parts:
        ring_near(part, tag)
    for h in range(heads):
        o_relay(h)
    for part, tag in w_parts:
        ring_far(part, tag)
    for part, tag in w_parts:
        arrived(part(mate), (tag, "M"))
        arrived(part(mate_left), (tag, "ML"))
        arrived(part(mate_right), (tag, "MR"))
        arrived(part(mate_across), (tag, "MF"))
    for h in range(heads):
        arrived(o_cols(far, h), ("o", h, "F"))
    load_o.wait()

    def y_at(owner, n, k=None):
        cols = pl.ds(pl.multiple_of(owner * y_cols + n * COL_TILE, 128), COL_TILE)
        return y_hbm.at[:, cols] if k is None else y_hbm.at[pl.ds(k * half_rows, half_rows), cols]

    copies = []
    tiles = y_cols // COL_TILE
    for n in range(tiles):
        c = pl.ds(n * COL_TILE, COL_TILE)

        @pl.loop(0, 2)
        def _(i):
            r = pl.ds(pl.multiple_of(i * half_rows, 16), half_rows)
            y_own[r, c] = jnp.dot(o_all[r, :], w_full[:, c], preferred_element_type=jnp.float32).astype(jnp.bfloat16)
        send(y_own.at[:, c], y_at(t, n), ("y", n, "D"), at_tp(up))
        send(y_own.at[:, c], y_at(t, n), ("y", n, "U"), at_tp(dn))
        copies.append(load(y_own.at[:, c], y_at(t, n), ("y", n)))
    for n in range(tiles):
        arrived(y_at(dn, n), ("y", n, "D"))
        send(y_at(dn, n, 0), y_at(dn, n, 0), ("y", n, "F0"), at_tp(up))
        arrived(y_at(up, n), ("y", n, "U"))
        send(y_at(up, n, 1), y_at(up, n, 1), ("y", n, "F1"), at_tp(dn))
    for n in range(tiles):
        arrived(y_at(far, n, 0), ("y", n, "F0"))
        arrived(y_at(far, n, 1), ("y", n, "F1"))
    for c in copies:
        c.wait()
    for c in waiting:
        c.wait_send()


def w_part(w_rows, owner):
    return lambda share, k=None: w_rows(owner, share, k)


def solution(mesh):
    tp, cp = mesh.shape["tp"], mesh.shape["cp"]

    def local_attention(x_loc, seg_loc, w_query, w_key, w_value, w_out):
        rows, width = x_loc.shape
        heads = w_query.shape[1] // HEAD_DIM
        groups = w_key.shape[1] // HEAD_DIM
        head_cols = heads * HEAD_DIM
        y_cols = width // tp
        bf16, f32 = jnp.bfloat16, jnp.float32
        hbm = pl.BlockSpec(memory_space=pl.ANY)
        return pl.pallas_call(
            functools.partial(kernel, tp, cp),
            out_shape=jax.ShapeDtypeStruct((rows, width), bf16),
            in_specs=[hbm, pl.BlockSpec(memory_space=pltpu.VMEM), hbm, hbm, hbm, hbm],
            out_specs=hbm,
            scratch_shapes=[
                pltpu.VMEM((rows, width), bf16),
                pltpu.VMEM((2, width, groups * HEAD_DIM), bf16),
                pltpu.VMEM((head_cols // COL_TILE, width, COL_TILE), bf16),
                pltpu.VMEM((tp * head_cols, y_cols), bf16),
                pltpu.VMEM((cp, groups, 2, rows, HEAD_DIM), bf16),
                pltpu.VMEM((cp, 1, rows), jnp.int32),
                pltpu.VMEM((rows, HEAD_DIM), jnp.int32),
                pltpu.VMEM((heads, rows, HEAD_DIM), bf16),
                pltpu.VMEM((rows, tp * head_cols), bf16),
                pltpu.VMEM((rows, y_cols), bf16),
                pltpu.VMEM((head_cols // cp // 2, y_cols), bf16),
                pltpu.VMEM((head_cols // cp // 2, y_cols), bf16),
                pltpu.VMEM((heads // groups, rows, HEAD_DIM), f32),
                pltpu.VMEM((heads // groups, rows, HEAD_DIM), f32),
                pltpu.VMEM((heads // groups, rows, HEAD_DIM), f32),
                pltpu.SemaphoreType.DMA((32,)),
                pltpu.SemaphoreType.DMA((160,)),
                pltpu.SemaphoreType.DMA((160,)),
            ],
            compiler_params=pltpu.CompilerParams(collective_id=0, has_side_effects=True, vmem_limit_bytes=67043328),
        )(x_loc, seg_loc.reshape(1, rows), w_query, w_key, w_value, w_out)

    return jax.shard_map(local_attention, mesh=mesh, in_specs=(P(('dp', 'cp'), None), P(('dp', 'cp')), P(None, 'tp'), P(None, 'tp'), P(None, 'tp'), P('tp', None)), out_specs=P(('dp', 'cp'), None), check_vma=False)
```

```python
import functools

import jax
import jax.numpy as jnp
from jax import lax
from jax.experimental import pallas as pl
from jax.experimental.pallas import tpu as pltpu
from jax.sharding import PartitionSpec as P


HEAD_DIM = 128
COL_TILE = 256
MESH = pl.DeviceIdType.MESH
SCALE = HEAD_DIM**-0.5 * 1.4426950408889634
NEG_INF = float("-inf")


class Sems:
    def __init__(self, ref):
        self.ref, self.names = ref, {}

    def __getitem__(self, name):
        return self.ref.at[self.names.setdefault(name, len(self.names))]


def kernel(tp, cp, x_hbm, seg_in, wq_hbm, wk_hbm, wv_hbm, wo_hbm, y_hbm,
           x_v, wkv_v, wq_v, w_full, k_all, vt_all, segs, seg_col, bias, q_v, o_all, y_own, relay_up, relay_dn,
           m_s, l_s, acc_s, load_sem, send_sem, recv_sem):
    t, p = lax.axis_index("tp"), lax.axis_index("cp")
    chips = cp // 2
    col, core = p // 2, lax.rem(p, 2)
    up, dn, far = lax.rem(t + 1, tp), lax.rem(t + tp - 1, tp), lax.rem(t + 2, tp)
    right_chip, left_chip, far_chip = lax.rem(col + 1, chips), lax.rem(col + chips - 1, chips), lax.rem(col + 2, chips)
    right, left, across = right_chip * 2 + core, left_chip * 2 + core, far_chip * 2 + core
    mate = col * 2 + 1 - core
    mate_right, mate_left, mate_across = right_chip * 2 + 1 - core, left_chip * 2 + 1 - core, far_chip * 2 + 1 - core

    rows = x_v.shape[0]
    heads = q_v.shape[0]
    groups = k_all.shape[1]
    per_group = heads // groups
    head_cols = heads * HEAD_DIM
    y_cols = y_own.shape[1]
    piece = head_cols // cp
    half = piece // 2
    half_rows = rows // 2

    loads, sends, recvs = Sems(load_sem), Sems(send_sem), Sems(recv_sem)
    waiting = []

    def at_tp(i):
        return {"tp": i, "cp": p}

    def at_cp(i):
        return {"tp": t, "cp": i}

    def send(src, dst, name, dev):
        c = pltpu.make_async_remote_copy(src_ref=src, dst_ref=dst, send_sem=sends[(name, len(waiting))],
                                         recv_sem=recvs[name], device_id=dev, device_id_type=MESH)
        c.start()
        waiting.append(c)

    def arrived(dst, name):
        pltpu.make_async_remote_copy(src_ref=dst, dst_ref=dst, send_sem=sends[0], recv_sem=recvs[name],
                                     device_id=at_cp(p), device_id_type=MESH).wait_recv()

    def load(src, dst, name):
        c = pltpu.make_async_copy(src, dst, loads[name])
        c.start()
        return c

    load_x = load(x_hbm, x_v, "x")
    load_k = load(wk_hbm, wkv_v.at[0], "k")
    load_v = load(wv_hbm, wkv_v.at[1], "v")
    q_tiles = head_cols // COL_TILE

    barrier = pltpu.get_barrier_semaphore()
    peers = [at_tp(up), at_tp(dn)] + [at_cp(lax.rem(p + k, cp)) for k in range(1, cp)]
    for dev in peers:
        pl.semaphore_signal(barrier, inc=1, device_id=dev, device_id_type=MESH)
    pl.semaphore_wait(barrier, len(peers))

    for k in range(1, cp):
        send(seg_in, segs.at[p], ("seg", k), at_cp(lax.rem(p + k, cp)))
    load_seg = load(seg_in, segs.at[p], "seg")

    def w_rows(owner, share, k=None):
        start = owner * head_cols + share * piece
        if k is None:
            return w_full.at[pl.ds(pl.multiple_of(start, 16), piece), :]
        return w_full.at[pl.ds(pl.multiple_of(start + k * half, 16), half), :]

    def w_src(dest, k=None):
        cols = pl.ds(pl.multiple_of(dest * y_cols, 128), y_cols)
        if k is None:
            return wo_hbm.at[pl.ds(pl.multiple_of(p * piece, 16), piece), cols]
        return wo_hbm.at[pl.ds(pl.multiple_of(p * piece + k * half, 16), half), cols]

    send(w_src(far, 0), relay_up, "w_relay_up", at_tp(up))
    send(w_src(far, 1), relay_dn, "w_relay_dn", at_tp(dn))
    send(w_src(up), w_rows(t, p), "w_from_dn", at_tp(up))
    send(w_src(dn), w_rows(t, p), "w_from_up", at_tp(dn))

    def send_all(refs, name, dev):
        for i, ref in enumerate(refs):
            send(ref, ref, (name, i), dev)

    def all_arrived(refs, name):
        for i, ref in enumerate(refs):
            arrived(ref, (name, i))

    def ring_start(part, tag):
        send_all(part(p), (tag, "L"), at_cp(right))
        send_all(part(p), (tag, "R"), at_cp(left))
        send_all(part(p), (tag, "M"), at_cp(mate))

    def ring_near(part, tag):
        all_arrived(part(left), (tag, "L"))
        send_all(part(left, 0), (tag, "far0"), at_cp(right))
        send_all(part(left), (tag, "ML"), at_cp(mate))
        all_arrived(part(right), (tag, "R"))
        send_all(part(right, 1), (tag, "far1"), at_cp(left))
        send_all(part(right), (tag, "MR"), at_cp(mate))

    def ring_far(part, tag):
        all_arrived(part(across, 0), (tag, "far0"))
        all_arrived(part(across, 1), (tag, "far1"))
        send_all(part(across), (tag, "MF"), at_cp(mate))

    def mates_near(part, tag):
        all_arrived(part(mate), (tag, "M"))
        all_arrived(part(mate_left), (tag, "ML"))
        all_arrived(part(mate_right), (tag, "MR"))

    def kv_part(g):
        def part(owner, k=None):
            both = [k_all.at[owner, g], vt_all.at[owner, g]]
            return both if k is None else both[k:k + 1]
        return part

    def w_part(owner):
        def part(share, k=None):
            return [w_rows(owner, share, k)]
        return part

    def project(w_ref, store):
        @pl.loop(0, rows // half_rows)
        def _(i):
            r = pl.ds(pl.multiple_of(i * half_rows, 16), half_rows)
            store(r, jnp.dot(x_v[r, :], w_ref[...], preferred_element_type=jnp.float32))

    with jax.named_scope("wait_x"):
        load_x.wait()
        load_k.wait()
    load_q = [load(wq_hbm.at[:, pl.ds(n * COL_TILE, COL_TILE)], wq_v.at[n], ("q", n)) for n in range(q_tiles)]
    own_cols = pl.ds(pl.multiple_of(t * y_cols, 128), y_cols)
    load_o = load(wo_hbm.at[:, own_cols], w_full.at[pl.ds(pl.multiple_of(t * head_cols, 128), head_cols), :], "o")

    def store_k(r, val):
        for g in range(groups):
            k_all[p, g, r, :] = val[:, g * HEAD_DIM:(g + 1) * HEAD_DIM].astype(jnp.bfloat16)

    def store_v(r, val):
        for g in range(groups):
            vt_all[p, g, :, r] = val[:, g * HEAD_DIM:(g + 1) * HEAD_DIM].T.astype(jnp.bfloat16)

    with jax.named_scope("proj_kv"):
        project(wkv_v.at[0], store_k)
        load_v.wait()
        project(wkv_v.at[1], store_v)
    ring_start(kv_part(0), ("kv", 0))

    def q_tile(n):
        load_q[n].wait()

        def store(r, val):
            for k in range(COL_TILE // HEAD_DIM):
                q_v[n * (COL_TILE // HEAD_DIM) + k, r, :] = val[:, k * HEAD_DIM:(k + 1) * HEAD_DIM].astype(jnp.bfloat16)
        with jax.named_scope(f"q{n}"):
            project(wq_v.at[n], store)

    def wide(v, n):
        return jnp.concatenate([v] * (n // v.shape[1]), axis=1)

    def set_bias(block, diagonal):
        seg_col[...] = jnp.broadcast_to(segs[block] if not diagonal else seg_in[...], (HEAD_DIM, rows)).T

        @pl.loop(0, rows // HEAD_DIM)
        def _(i):
            r = pl.ds(pl.multiple_of(i * HEAD_DIM, HEAD_DIM), HEAD_DIM)
            allowed = wide(seg_col[r, :], rows) == seg_in[...]
            if diagonal:
                allowed &= (lax.broadcasted_iota(jnp.int32, (HEAD_DIM, rows), 0) + i * HEAD_DIM
                            <= lax.broadcasted_iota(jnp.int32, (HEAD_DIM, rows), 1))
            bias[block, r, :] = jnp.where(allowed, 0.0, NEG_INF)

    def visit(g, block, diagonal):
        units = [(k, i) for k in range(2) for i in range(2)]

        @pl.loop(0, per_group // 2)
        def _(pair):
            def keys(i):
                return half_rows if diagonal and i == 0 else rows

            def scores(k, i):
                q = q_v[g * per_group + pair * 2 + k, i * half_rows:(i + 1) * half_rows, :]
                return lax.dot_general(k_all[block, g, :keys(i), :], q, (((1,), (1,)), ((), ())),
                                       preferred_element_type=jnp.float32)

            def absorb(s, k, i):
                h, c = pair * 2 + k, slice(i * half_rows, (i + 1) * half_rows)
                s = s + bias[block, :keys(i), c]
                new_max = jnp.max(s, axis=0, keepdims=True)
                if not diagonal:
                    old_max = m_s[h, :, c]
                    new_max = jnp.maximum(old_max, new_max)
                prob = jnp.exp2(s * SCALE - new_max * SCALE)
                total = jnp.sum(prob, axis=0, keepdims=True)
                out = jnp.dot(vt_all[block, g, :, :keys(i)], prob.astype(jnp.bfloat16), preferred_element_type=jnp.float32)
                if not diagonal:
                    rescale = jnp.exp2((old_max - new_max) * SCALE)
                    total += l_s[h, :, c] * rescale
                    out += acc_s[h, :, c] * rescale
                m_s[h, :, c] = new_max
                l_s[h, :, c] = total
                acc_s[h, :, c] = out

            ahead = scores(*units[0])
            for n, unit in enumerate(units):
                now = ahead
                if n + 1 < len(units):
                    ahead = scores(*units[n + 1])
                absorb(now, *unit)

    def visit_all(g, count, block_of):
        @pl.loop(0, count)
        def _(i):
            block = block_of(i)

            @pl.when(block < p)
            def _():
                if g == 0:
                    set_bias(block, False)
                visit(g, block, False)

    def visit_near(g):
        chip_of = lambda i: jnp.where(i < 2, left_chip, right_chip)
        visit_all(g, 5, lambda i: jnp.where(i == 4, mate, chip_of(i) * 2 + lax.rem(i, 2)))

    def visit_far(g):
        visit_all(g, 2, lambda i: far_chip * 2 + i)

    def o_cols(owner, h):
        return o_all.at[:, pl.ds(pl.multiple_of(owner * head_cols + h * HEAD_DIM, 128), HEAD_DIM)]

    def o_finish(g):
        for k in range(per_group):
            h = g * per_group + k
            o_all[:, pl.ds(pl.multiple_of(t * head_cols + h * HEAD_DIM, 128), HEAD_DIM)] = (
                acc_s[k] / l_s[k]).T.astype(jnp.bfloat16)
            send(o_cols(t, h), o_cols(t, h), ("o", h, "D"), at_tp(up))
            send(o_cols(t, h), o_cols(t, h), ("o", h, "U"), at_tp(dn))

    def o_relay(h):
        arrived(o_cols(dn, h), ("o", h, "D"))
        arrived(o_cols(up, h), ("o", h, "U"))
        if h % 2 == 0:
            send(o_cols(dn, h), o_cols(dn, h), ("o", h, "F"), at_tp(up))
        else:
            send(o_cols(up, h), o_cols(up, h), ("o", h, "F"), at_tp(dn))

    kv = [(kv_part(g), ("kv", g)) for g in range(groups)]
    w = [(w_part(lax.rem(t + j, tp)), ("w", j)) for j in range(1, tp)]

    q_tile(0)
    q_tile(1)
    with jax.named_scope("diag0"):
        set_bias(p, True)
        visit(0, p, True)
    q_tile(2)
    with jax.named_scope("kv0_near"):
        ring_near(*kv[0])
    ring_start(*kv[1])
    with jax.named_scope("w_relay"):
        arrived(relay_up, "w_relay_up")
        send(relay_up, w_rows(dn, p, 0), "w_far0", at_tp(up))
        arrived(relay_dn, "w_relay_dn")
        send(relay_dn, w_rows(up, p, 1), "w_far1", at_tp(dn))
    q_tile(3)
    with jax.named_scope("kv0_mate"):
        load_seg.wait()
        for k in range(1, cp):
            arrived(segs.at[lax.rem(p + cp - k, cp)], ("seg", k))
        mates_near(*kv[0])
    with jax.named_scope("near0"):
        visit_near(0)
    with jax.named_scope("w_tp"):
        arrived(w_rows(dn, p), "w_from_dn")
        arrived(w_rows(up, p), "w_from_up")
        arrived(w_rows(far, p, 0), "w_far0")
        arrived(w_rows(far, p, 1), "w_far1")
    with jax.named_scope("kv1_near"):
        ring_near(*kv[1])
    with jax.named_scope("kv0_far"):
        ring_far(*kv[0])
        all_arrived(kv[0][0](mate_across), (kv[0][1], "MF"))
    for part in w:
        ring_start(*part)
    with jax.named_scope("far0"):
        visit_far(0)
    with jax.named_scope("o_fin0"):
        o_finish(0)
    with jax.named_scope("diag1"):
        visit(1, p, True)
    with jax.named_scope("kv1_far"):
        ring_far(*kv[1])
        mates_near(*kv[1])
    with jax.named_scope("near1"):
        visit_near(1)
    with jax.named_scope("kv1_mate"):
        all_arrived(kv[1][0](mate_across), (kv[1][1], "MF"))
    with jax.named_scope("far1"):
        visit_far(1)
    with jax.named_scope("o_fin1"):
        o_finish(1)
    with jax.named_scope("o_relay_a"):
        for h in range(per_group):
            o_relay(h)
    with jax.named_scope("w_near"):
        for part in w:
            ring_near(*part)
    with jax.named_scope("o_relay_b"):
        for h in range(per_group, heads):
            o_relay(h)
    with jax.named_scope("w_far"):
        for part in w:
            ring_far(*part)
    with jax.named_scope("w_mate"):
        for part, tag in w:
            mates_near(part, tag)
            all_arrived(part(mate_across), (tag, "MF"))
    with jax.named_scope("o_far"):
        for h in range(heads):
            arrived(o_cols(far, h), ("o", h, "F"))
        load_o.wait()

    def y_at(owner, n, k=None):
        cols = pl.ds(pl.multiple_of(owner * y_cols + n * COL_TILE, 128), COL_TILE)
        return y_hbm.at[:, cols] if k is None else y_hbm.at[pl.ds(k * half_rows, half_rows), cols]

    copies = []
    tiles = y_cols // COL_TILE
    for n in range(tiles):
        c = pl.ds(n * COL_TILE, COL_TILE)

        @pl.loop(0, 2)
        def _(i):
          with jax.named_scope("y_mm"):
            r = pl.ds(pl.multiple_of(i * half_rows, 16), half_rows)
            y_own[r, c] = jnp.dot(o_all[r, :], w_full[:, c], preferred_element_type=jnp.float32).astype(jnp.bfloat16)
        send(y_own.at[:, c], y_at(t, n), ("y", n, "D"), at_tp(up))
        send(y_own.at[:, c], y_at(t, n), ("y", n, "U"), at_tp(dn))
        copies.append(load(y_own.at[:, c], y_at(t, n), ("y", n)))
    for n in range(tiles):
      with jax.named_scope(f"y_relay{n}"):
        arrived(y_at(dn, n), ("y", n, "D"))
        send(y_at(dn, n, 0), y_at(dn, n, 0), ("y", n, "F0"), at_tp(up))
        arrived(y_at(up, n), ("y", n, "U"))
        send(y_at(up, n, 1), y_at(up, n, 1), ("y", n, "F1"), at_tp(dn))
    for n in range(tiles):
      with jax.named_scope(f"y_far{n}"):
        arrived(y_at(far, n, 0), ("y", n, "F0"))
        arrived(y_at(far, n, 1), ("y", n, "F1"))
    for c in copies:
        c.wait()
    for c in waiting:
        c.wait_send()


def solution(mesh):
    tp, cp = mesh.shape["tp"], mesh.shape["cp"]

    def local_attention(x_loc, seg_loc, w_query, w_key, w_value, w_out):
        rows, width = x_loc.shape
        heads = w_query.shape[1] // HEAD_DIM
        groups = w_key.shape[1] // HEAD_DIM
        head_cols = heads * HEAD_DIM
        y_cols = width // tp
        bf16, f32 = jnp.bfloat16, jnp.float32
        hbm = pl.BlockSpec(memory_space=pl.ANY)
        return pl.pallas_call(
            functools.partial(kernel, tp, cp),
            out_shape=jax.ShapeDtypeStruct((rows, width), bf16),
            in_specs=[hbm, pl.BlockSpec(memory_space=pltpu.VMEM), hbm, hbm, hbm, hbm],
            out_specs=hbm,
            scratch_shapes=[
                pltpu.VMEM((rows, width), bf16),
                pltpu.VMEM((2, width, groups * HEAD_DIM), bf16),
                pltpu.VMEM((head_cols // COL_TILE, width, COL_TILE), bf16),
                pltpu.VMEM((tp * head_cols, y_cols), bf16),
                pltpu.VMEM((cp, groups, rows, HEAD_DIM), bf16),
                pltpu.VMEM((cp, groups, HEAD_DIM, rows), bf16),
                pltpu.VMEM((cp, 1, rows), jnp.int32),
                pltpu.VMEM((rows, HEAD_DIM), jnp.int32),
                pltpu.VMEM((cp, rows, rows), f32),
                pltpu.VMEM((heads, rows, HEAD_DIM), bf16),
                pltpu.VMEM((rows, tp * head_cols), bf16),
                pltpu.VMEM((rows, y_cols), bf16),
                pltpu.VMEM((head_cols // cp // 2, y_cols), bf16),
                pltpu.VMEM((head_cols // cp // 2, y_cols), bf16),
                pltpu.VMEM((heads // groups, 1, rows), f32),
                pltpu.VMEM((heads // groups, 1, rows), f32),
                pltpu.VMEM((heads // groups, HEAD_DIM, rows), f32),
                pltpu.SemaphoreType.DMA((32,)),
                pltpu.SemaphoreType.DMA((224,)),
                pltpu.SemaphoreType.DMA((224,)),
            ],
            compiler_params=pltpu.CompilerParams(collective_id=0, has_side_effects=True, vmem_limit_bytes=67043328),
        )(x_loc, seg_loc.reshape(1, rows), w_query, w_key, w_value, w_out)

    return jax.shard_map(local_attention, mesh=mesh, in_specs=(P(('dp', 'cp'), None), P(('dp', 'cp')), P(None, 'tp'), P(None, 'tp'), P(None, 'tp'), P('tp', None)), out_specs=P(('dp', 'cp'), None), check_vma=False)
```

```python
import functools

import jax
import jax.numpy as jnp
from jax import lax
from jax.experimental import pallas as pl
from jax.experimental.pallas import tpu as pltpu
from jax.sharding import PartitionSpec as P


HEAD_DIM = 128
COL_TILE = 256
MESH = pl.DeviceIdType.MESH
SCALE = HEAD_DIM**-0.5 * 1.4426950408889634
NEG_INF = float("-inf")


class Sems:
    def __init__(self, ref):
        self.ref, self.names = ref, {}

    def __getitem__(self, name):
        return self.ref.at[self.names.setdefault(name, len(self.names))]


def kernel(tp, cp, x_hbm, seg_in, wq_hbm, wk_hbm, wv_hbm, wo_hbm, y_hbm,
           x_v, wkv_v, wq_v, w_full, k_all, vt_all, segs, seg_col, bias, k_mask, s_even, s_odd, q_v, o_all, y_own, relay_up, relay_dn,
           m_s, l_s, acc_s, load_sem, send_sem, recv_sem):
    t, p = lax.axis_index("tp"), lax.axis_index("cp")
    chips = cp // 2
    col, core = p // 2, lax.rem(p, 2)
    up, dn, far = lax.rem(t + 1, tp), lax.rem(t + tp - 1, tp), lax.rem(t + 2, tp)
    right_chip, left_chip, far_chip = lax.rem(col + 1, chips), lax.rem(col + chips - 1, chips), lax.rem(col + 2, chips)
    right, left, across = right_chip * 2 + core, left_chip * 2 + core, far_chip * 2 + core
    mate = col * 2 + 1 - core
    mate_right, mate_left, mate_across = right_chip * 2 + 1 - core, left_chip * 2 + 1 - core, far_chip * 2 + 1 - core

    rows = x_v.shape[0]
    heads = q_v.shape[0]
    groups = k_all.shape[1]
    per_group = heads // groups
    head_cols = heads * HEAD_DIM
    y_cols = y_own.shape[1]
    piece = head_cols // cp
    half = piece // 2
    half_rows = rows // 2

    loads, sends, recvs = Sems(load_sem), Sems(send_sem), Sems(recv_sem)
    waiting = []

    def at_tp(i):
        return {"tp": i, "cp": p}

    def at_cp(i):
        return {"tp": t, "cp": i}

    def send(src, dst, name, dev):
        c = pltpu.make_async_remote_copy(src_ref=src, dst_ref=dst, send_sem=sends[(name, len(waiting))],
                                         recv_sem=recvs[name], device_id=dev, device_id_type=MESH)
        c.start()
        waiting.append(c)

    def arrived(dst, name):
        pltpu.make_async_remote_copy(src_ref=dst, dst_ref=dst, send_sem=sends[0], recv_sem=recvs[name],
                                     device_id=at_cp(p), device_id_type=MESH).wait_recv()

    def load(src, dst, name):
        c = pltpu.make_async_copy(src, dst, loads[name])
        c.start()
        return c

    load_x = load(x_hbm, x_v, "x")
    load_k = load(wk_hbm, wkv_v.at[0], "k")
    load_v = load(wv_hbm, wkv_v.at[1], "v")
    q_tiles = head_cols // COL_TILE

    barrier = pltpu.get_barrier_semaphore()
    peers = [at_tp(up), at_tp(dn)] + [at_cp(lax.rem(p + k, cp)) for k in range(1, cp)]
    for dev in peers:
        pl.semaphore_signal(barrier, inc=1, device_id=dev, device_id_type=MESH)
    pl.semaphore_wait(barrier, len(peers))

    for k in range(1, cp):
        send(seg_in, segs.at[p], ("seg", k), at_cp(lax.rem(p + k, cp)))
    load_seg = load(seg_in, segs.at[p], "seg")

    def w_rows(owner, share, k=None):
        start = owner * head_cols + share * piece
        if k is None:
            return w_full.at[pl.ds(pl.multiple_of(start, 16), piece), :]
        return w_full.at[pl.ds(pl.multiple_of(start + k * half, 16), half), :]

    def w_src(dest, k=None):
        cols = pl.ds(pl.multiple_of(dest * y_cols, 128), y_cols)
        if k is None:
            return wo_hbm.at[pl.ds(pl.multiple_of(p * piece, 16), piece), cols]
        return wo_hbm.at[pl.ds(pl.multiple_of(p * piece + k * half, 16), half), cols]

    send(w_src(far, 0), relay_up, "w_relay_up", at_tp(up))
    send(w_src(far, 1), relay_dn, "w_relay_dn", at_tp(dn))
    send(w_src(up), w_rows(t, p), "w_from_dn", at_tp(up))
    send(w_src(dn), w_rows(t, p), "w_from_up", at_tp(dn))

    def send_all(refs, name, dev):
        for i, ref in enumerate(refs):
            send(ref, ref, (name, i), dev)

    def all_arrived(refs, name):
        for i, ref in enumerate(refs):
            arrived(ref, (name, i))

    def ring_start(part, tag):
        send_all(part(p), (tag, "L"), at_cp(right))
        send_all(part(p), (tag, "R"), at_cp(left))
        send_all(part(p), (tag, "M"), at_cp(mate))

    def ring_near(part, tag):
        all_arrived(part(left), (tag, "L"))
        send_all(part(left, 0), (tag, "far0"), at_cp(right))
        send_all(part(left), (tag, "ML"), at_cp(mate))
        all_arrived(part(right), (tag, "R"))
        send_all(part(right, 1), (tag, "far1"), at_cp(left))
        send_all(part(right), (tag, "MR"), at_cp(mate))

    def ring_far(part, tag):
        all_arrived(part(across, 0), (tag, "far0"))
        all_arrived(part(across, 1), (tag, "far1"))
        send_all(part(across), (tag, "MF"), at_cp(mate))

    def mates_near(part, tag):
        all_arrived(part(mate), (tag, "M"))
        all_arrived(part(mate_left), (tag, "ML"))
        all_arrived(part(mate_right), (tag, "MR"))

    def kv_part(g):
        def part(owner, k=None):
            both = [k_all.at[owner, g], vt_all.at[owner, g]]
            return both if k is None else both[k:k + 1]
        return part

    def w_part(owner):
        def part(share, k=None):
            return [w_rows(owner, share, k)]
        return part

    def project(w_ref, store):
        @pl.loop(0, rows // half_rows)
        def _(i):
            r = pl.ds(pl.multiple_of(i * half_rows, 16), half_rows)
            store(r, jnp.dot(x_v[r, :], w_ref[...], preferred_element_type=jnp.float32))

    with jax.named_scope("wait_x"):
        load_x.wait()
        load_k.wait()
    load_q = [load(wq_hbm.at[:, pl.ds(n * COL_TILE, COL_TILE)], wq_v.at[n], ("q", n)) for n in range(q_tiles)]
    own_cols = pl.ds(pl.multiple_of(t * y_cols, 128), y_cols)
    load_o = load(wo_hbm.at[:, own_cols], w_full.at[pl.ds(pl.multiple_of(t * head_cols, 128), head_cols), :], "o")

    def store_k(r, val):
        for g in range(groups):
            k_all[p, g, r, :] = val[:, g * HEAD_DIM:(g + 1) * HEAD_DIM].astype(jnp.bfloat16)

    def store_v(r, val):
        for g in range(groups):
            vt_all[p, g, :, r] = val[:, g * HEAD_DIM:(g + 1) * HEAD_DIM].T.astype(jnp.bfloat16)

    with jax.named_scope("proj_kv"):
        project(wkv_v.at[0], store_k)
        load_v.wait()
        project(wkv_v.at[1], store_v)
    ring_start(kv_part(0), ("kv", 0))

    def q_tile(n):
        load_q[n].wait()

        def store(r, val):
            for k in range(COL_TILE // HEAD_DIM):
                q_v[n * (COL_TILE // HEAD_DIM) + k, r, :HEAD_DIM] = val[:, k * HEAD_DIM:(k + 1) * HEAD_DIM].astype(jnp.bfloat16)
        with jax.named_scope(f"q{n}"):
            project(wq_v.at[n], store)

    def wide(v, n):
        return jnp.concatenate([v] * (n // v.shape[1]), axis=1)

    lane = lax.broadcasted_iota(jnp.int32, (rows, HEAD_DIM), 1)
    first_doc = seg_in[:, :1]

    def set_bias():
        seg_col[...] = jnp.broadcast_to(seg_in[...], (HEAD_DIM, rows)).T

        @pl.loop(0, rows // HEAD_DIM)
        def _(i):
            r = pl.ds(pl.multiple_of(i * HEAD_DIM, HEAD_DIM), HEAD_DIM)
            allowed = wide(seg_col[r, :], rows) == seg_in[...]
            allowed &= (lax.broadcasted_iota(jnp.int32, (HEAD_DIM, rows), 0) + i * HEAD_DIM
                        <= lax.broadcasted_iota(jnp.int32, (HEAD_DIM, rows), 1))
            bias[r, :] = jnp.where(allowed, 0.0, NEG_INF)

    def set_mask(block):
        of_key = jnp.broadcast_to(segs[block], (HEAD_DIM, rows)).T
        shut = (of_key != first_doc) & (lane == 0)
        k_mask[block] = jnp.where(shut, NEG_INF, 0.0).astype(jnp.bfloat16)

    def visit(g, block, diagonal):
        units = [(h, i) for h in range(per_group) for i in range(2)]
        scratch = [s_even, s_odd]

        def keys(i):
            return half_rows if diagonal and i == 0 else rows

        def scores(n):
            h, i = units[n]
            c = slice(i * half_rows, (i + 1) * half_rows)
            q = q_v[g * per_group + h, c, :]
            k = k_all[block, g, :keys(i), :]
            if diagonal:
                s = lax.dot_general(k, q[:, :HEAD_DIM], (((1,), (1,)), ((), ())), preferred_element_type=jnp.float32)
                s += bias[:keys(i), c]
            else:
                k = jnp.concatenate([k, k_mask[block]], axis=1)
                s = lax.dot_general(k, q, (((1,), (1,)), ((), ())), preferred_element_type=jnp.float32)
            scratch[n % 2][:keys(i), :] = s
            return jnp.max(s, axis=0, keepdims=True)

        def absorb(n, top):
            h, i = units[n]
            c = slice(i * half_rows, (i + 1) * half_rows)
            if diagonal:
                new_max = shift = top
            else:
                in_first = seg_in[:, c] == first_doc
                old_max = m_s[h, :, c]
                new_max = jnp.where(in_first, jnp.maximum(old_max, top), old_max)
                shift = jnp.where(in_first, new_max, -NEG_INF)
            prob = jnp.exp2(scratch[n % 2][:keys(i), :] * SCALE - shift * SCALE)
            total = jnp.sum(prob, axis=0, keepdims=True)
            out = jnp.dot(vt_all[block, g, :, :keys(i)], prob.astype(jnp.bfloat16), preferred_element_type=jnp.float32)
            if not diagonal:
                rescale = jnp.exp2((old_max - new_max) * SCALE)
                total += l_s[h, :, c] * rescale
                out += acc_s[h, :, c] * rescale
            m_s[h, :, c] = new_max
            l_s[h, :, c] = total
            acc_s[h, :, c] = out

        top = scores(0)
        for n in range(len(units)):
            ahead = scores(n + 1) if n + 1 < len(units) else None
            absorb(n, top)
            top = ahead

    def visit_all(g, count, block_of):
        @pl.loop(0, count)
        def _(i):
            block = block_of(i)

            @pl.when(block < p)
            def _():
                if g == 0:
                    set_mask(block)
                visit(g, block, False)

    def visit_near(g):
        chip_of = lambda i: jnp.where(i < 2, left_chip, right_chip)
        visit_all(g, 5, lambda i: jnp.where(i == 4, mate, chip_of(i) * 2 + lax.rem(i, 2)))

    def visit_far(g):
        visit_all(g, 2, lambda i: far_chip * 2 + i)

    def o_cols(owner, h):
        return o_all.at[:, pl.ds(pl.multiple_of(owner * head_cols + h * HEAD_DIM, 128), HEAD_DIM)]

    def o_finish(g):
        for k in range(per_group):
            h = g * per_group + k
            o_all[:, pl.ds(pl.multiple_of(t * head_cols + h * HEAD_DIM, 128), HEAD_DIM)] = (
                acc_s[k] / l_s[k]).T.astype(jnp.bfloat16)
            send(o_cols(t, h), o_cols(t, h), ("o", h, "D"), at_tp(up))
            send(o_cols(t, h), o_cols(t, h), ("o", h, "U"), at_tp(dn))

    def o_relay(h):
        arrived(o_cols(dn, h), ("o", h, "D"))
        arrived(o_cols(up, h), ("o", h, "U"))
        if h % 2 == 0:
            send(o_cols(dn, h), o_cols(dn, h), ("o", h, "F"), at_tp(up))
        else:
            send(o_cols(up, h), o_cols(up, h), ("o", h, "F"), at_tp(dn))

    kv = [(kv_part(g), ("kv", g)) for g in range(groups)]
    w = [(w_part(lax.rem(t + j, tp)), ("w", j)) for j in range(1, tp)]

    q_v[:, :, HEAD_DIM:] = jnp.where(lax.broadcasted_iota(jnp.int32, (heads, rows, HEAD_DIM), 2) == 0, 1.0, 0.0).astype(jnp.bfloat16)
    q_tile(0)
    q_tile(1)
    with jax.named_scope("diag0"):
        set_bias()
        visit(0, p, True)
    q_tile(2)
    with jax.named_scope("kv0_near"):
        ring_near(*kv[0])
    ring_start(*kv[1])
    with jax.named_scope("w_relay"):
        arrived(relay_up, "w_relay_up")
        send(relay_up, w_rows(dn, p, 0), "w_far0", at_tp(up))
        arrived(relay_dn, "w_relay_dn")
        send(relay_dn, w_rows(up, p, 1), "w_far1", at_tp(dn))
    q_tile(3)
    with jax.named_scope("kv0_mate"):
        load_seg.wait()
        for k in range(1, cp):
            arrived(segs.at[lax.rem(p + cp - k, cp)], ("seg", k))
        mates_near(*kv[0])
    with jax.named_scope("near0"):
        visit_near(0)
    with jax.named_scope("w_tp"):
        arrived(w_rows(dn, p), "w_from_dn")
        arrived(w_rows(up, p), "w_from_up")
        arrived(w_rows(far, p, 0), "w_far0")
        arrived(w_rows(far, p, 1), "w_far1")
    with jax.named_scope("kv1_near"):
        ring_near(*kv[1])
    with jax.named_scope("kv0_far"):
        ring_far(*kv[0])
        all_arrived(kv[0][0](mate_across), (kv[0][1], "MF"))
    for part in w:
        ring_start(*part)
    with jax.named_scope("far0"):
        visit_far(0)
    with jax.named_scope("o_fin0"):
        o_finish(0)
    with jax.named_scope("diag1"):
        visit(1, p, True)
    with jax.named_scope("kv1_far"):
        ring_far(*kv[1])
        mates_near(*kv[1])
    with jax.named_scope("near1"):
        visit_near(1)
    with jax.named_scope("kv1_mate"):
        all_arrived(kv[1][0](mate_across), (kv[1][1], "MF"))
    with jax.named_scope("far1"):
        visit_far(1)
    with jax.named_scope("o_fin1"):
        o_finish(1)
    with jax.named_scope("o_relay_a"):
        for h in range(per_group):
            o_relay(h)
    with jax.named_scope("w_near"):
        for part in w:
            ring_near(*part)
    with jax.named_scope("o_relay_b"):
        for h in range(per_group, heads):
            o_relay(h)
    with jax.named_scope("w_far"):
        for part in w:
            ring_far(*part)
    with jax.named_scope("w_mate"):
        for part, tag in w:
            mates_near(part, tag)
            all_arrived(part(mate_across), (tag, "MF"))
    with jax.named_scope("o_far"):
        for h in range(heads):
            arrived(o_cols(far, h), ("o", h, "F"))
        load_o.wait()

    def y_at(owner, n, k=None):
        cols = pl.ds(pl.multiple_of(owner * y_cols + n * COL_TILE, 128), COL_TILE)
        return y_hbm.at[:, cols] if k is None else y_hbm.at[pl.ds(k * half_rows, half_rows), cols]

    copies = []
    tiles = y_cols // COL_TILE
    for n in range(tiles):
        c = pl.ds(n * COL_TILE, COL_TILE)

        @pl.loop(0, 2)
        def _(i):
          with jax.named_scope("y_mm"):
            r = pl.ds(pl.multiple_of(i * half_rows, 16), half_rows)
            y_own[r, c] = jnp.dot(o_all[r, :], w_full[:, c], preferred_element_type=jnp.float32).astype(jnp.bfloat16)
        send(y_own.at[:, c], y_at(t, n), ("y", n, "D"), at_tp(up))
        send(y_own.at[:, c], y_at(t, n), ("y", n, "U"), at_tp(dn))
        copies.append(load(y_own.at[:, c], y_at(t, n), ("y", n)))
    for n in range(tiles):
      with jax.named_scope(f"y_relay{n}"):
        arrived(y_at(dn, n), ("y", n, "D"))
        send(y_at(dn, n, 0), y_at(dn, n, 0), ("y", n, "F0"), at_tp(up))
        arrived(y_at(up, n), ("y", n, "U"))
        send(y_at(up, n, 1), y_at(up, n, 1), ("y", n, "F1"), at_tp(dn))
    for n in range(tiles):
      with jax.named_scope(f"y_far{n}"):
        arrived(y_at(far, n, 0), ("y", n, "F0"))
        arrived(y_at(far, n, 1), ("y", n, "F1"))
    for c in copies:
        c.wait()
    for c in waiting:
        c.wait_send()


def solution(mesh):
    tp, cp = mesh.shape["tp"], mesh.shape["cp"]

    def local_attention(x_loc, seg_loc, w_query, w_key, w_value, w_out):
        rows, width = x_loc.shape
        heads = w_query.shape[1] // HEAD_DIM
        groups = w_key.shape[1] // HEAD_DIM
        head_cols = heads * HEAD_DIM
        y_cols = width // tp
        bf16, f32 = jnp.bfloat16, jnp.float32
        hbm = pl.BlockSpec(memory_space=pl.ANY)
        return pl.pallas_call(
            functools.partial(kernel, tp, cp),
            out_shape=jax.ShapeDtypeStruct((rows, width), bf16),
            in_specs=[hbm, pl.BlockSpec(memory_space=pltpu.VMEM), hbm, hbm, hbm, hbm],
            out_specs=hbm,
            scratch_shapes=[
                pltpu.VMEM((rows, width), bf16),
                pltpu.VMEM((2, width, groups * HEAD_DIM), bf16),
                pltpu.VMEM((head_cols // COL_TILE, width, COL_TILE), bf16),
                pltpu.VMEM((tp * head_cols, y_cols), bf16),
                pltpu.VMEM((cp, groups, rows, HEAD_DIM), bf16),
                pltpu.VMEM((cp, groups, HEAD_DIM, rows), bf16),
                pltpu.VMEM((cp, 1, rows), jnp.int32),
                pltpu.VMEM((rows, HEAD_DIM), jnp.int32),
                pltpu.VMEM((rows, rows), f32),
                pltpu.VMEM((cp, rows, HEAD_DIM), bf16),
                pltpu.VMEM((rows, rows // 2), f32),
                pltpu.VMEM((rows, rows // 2), f32),
                pltpu.VMEM((heads, rows, 2 * HEAD_DIM), bf16),
                pltpu.VMEM((rows, tp * head_cols), bf16),
                pltpu.VMEM((rows, y_cols), bf16),
                pltpu.VMEM((head_cols // cp // 2, y_cols), bf16),
                pltpu.VMEM((head_cols // cp // 2, y_cols), bf16),
                pltpu.VMEM((heads // groups, 1, rows), f32),
                pltpu.VMEM((heads // groups, 1, rows), f32),
                pltpu.VMEM((heads // groups, HEAD_DIM, rows), f32),
                pltpu.SemaphoreType.DMA((32,)),
                pltpu.SemaphoreType.DMA((224,)),
                pltpu.SemaphoreType.DMA((224,)),
            ],
            compiler_params=pltpu.CompilerParams(collective_id=0, has_side_effects=True, vmem_limit_bytes=67043328),
        )(x_loc, seg_loc.reshape(1, rows), w_query, w_key, w_value, w_out)

    return jax.shard_map(local_attention, mesh=mesh, in_specs=(P(('dp', 'cp'), None), P(('dp', 'cp')), P(None, 'tp'), P(None, 'tp'), P(None, 'tp'), P('tp', None)), out_specs=P(('dp', 'cp'), None), check_vma=False)
```

```python
import functools

import jax
import jax.numpy as jnp
from jax import lax
from jax.experimental import pallas as pl
from jax.experimental.pallas import tpu as pltpu
from jax.sharding import PartitionSpec as P


HEAD_DIM = 128
COL_TILE = 256
PAIR = 2
MESH = pl.DeviceIdType.MESH
SCALE = HEAD_DIM**-0.5 * 1.4426950408889634
NEG_INF = float("-inf")


class Sems:
    def __init__(self, ref):
        self.ref, self.names = ref, {}

    def __getitem__(self, name):
        return self.ref.at[self.names.setdefault(name, len(self.names))]


def kernel(tp, cp, x_hbm, seg_in, wq_hbm, wk_hbm, wv_hbm, wo_hbm, y_hbm,
           x_v, wkv_v, wq_v, w_full, k_all, vt_all, segs, seg_col, bias, k_mask, s_even, s_odd, q_v, o_all, y_own, relay_up, relay_dn,
           m_s, l_s, acc_s, load_sem, send_sem, recv_sem):
    t, p = lax.axis_index("tp"), lax.axis_index("cp")
    chips = cp // 2
    col, core = p // 2, lax.rem(p, 2)
    up, dn, far = lax.rem(t + 1, tp), lax.rem(t + tp - 1, tp), lax.rem(t + 2, tp)
    right_chip, left_chip, far_chip = lax.rem(col + 1, chips), lax.rem(col + chips - 1, chips), lax.rem(col + 2, chips)
    right, left, across = right_chip * 2 + core, left_chip * 2 + core, far_chip * 2 + core
    mate = col * 2 + 1 - core
    mate_right, mate_left, mate_across = right_chip * 2 + 1 - core, left_chip * 2 + 1 - core, far_chip * 2 + 1 - core

    rows = x_v.shape[0]
    heads = q_v.shape[0]
    groups = k_all.shape[1]
    per_group = heads // groups
    head_cols = heads * HEAD_DIM
    y_cols = y_own.shape[1]
    piece = head_cols // cp
    half = piece // 2
    half_rows = rows // 2

    loads, sends, recvs = Sems(load_sem), Sems(send_sem), Sems(recv_sem)
    waiting = []

    def at_tp(i):
        return {"tp": i, "cp": p}

    def at_cp(i):
        return {"tp": t, "cp": i}

    def send(src, dst, name, dev):
        c = pltpu.make_async_remote_copy(src_ref=src, dst_ref=dst, send_sem=sends[(name, len(waiting))],
                                         recv_sem=recvs[name], device_id=dev, device_id_type=MESH)
        c.start()
        waiting.append(c)

    def arrived(dst, name):
        pltpu.make_async_remote_copy(src_ref=dst, dst_ref=dst, send_sem=sends[0], recv_sem=recvs[name],
                                     device_id=at_cp(p), device_id_type=MESH).wait_recv()

    def load(src, dst, name):
        c = pltpu.make_async_copy(src, dst, loads[name])
        c.start()
        return c

    load_x = load(x_hbm, x_v, "x")
    load_k = load(wk_hbm, wkv_v.at[0], "k")
    load_v = load(wv_hbm, wkv_v.at[1], "v")
    q_tiles = head_cols // COL_TILE

    barrier = pltpu.get_barrier_semaphore()
    peers = [at_tp(up), at_tp(dn)] + [at_cp(lax.rem(p + k, cp)) for k in range(1, cp)]
    for dev in peers:
        pl.semaphore_signal(barrier, inc=1, device_id=dev, device_id_type=MESH)
    pl.semaphore_wait(barrier, len(peers))

    for k in range(1, cp):
        send(seg_in, segs.at[p], ("seg", k), at_cp(lax.rem(p + k, cp)))
    load_seg = load(seg_in, segs.at[p], "seg")

    def w_rows(owner, share, start, count):
        return w_full.at[pl.ds(pl.multiple_of(owner * head_cols + share * piece + start, 16), count), :]

    def w_src(dest, share, start, count):
        return wo_hbm.at[pl.ds(pl.multiple_of(share * piece + start, 16), count),
                         pl.ds(pl.multiple_of(dest * y_cols, 128), y_cols)]

    w_parts = [("own", p, piece), ("far", across, half)]

    def relay_buf(buf, kind):
        return buf.at[pl.ds(0, half)] if kind == "own" else buf.at[pl.ds(half, half // 2)]

    for kind, share, count in w_parts:
        n = count // 2
        send(w_src(far, share, 0, n), relay_buf(relay_up, kind), ("w_relay_up", kind), at_tp(up))
        send(w_src(far, share, n, n), relay_buf(relay_dn, kind), ("w_relay_dn", kind), at_tp(dn))
        send(w_src(up, share, 0, count), w_rows(t, share, 0, count), ("w_from_dn", kind), at_tp(up))
        send(w_src(dn, share, 0, count), w_rows(t, share, 0, count), ("w_from_up", kind), at_tp(dn))

    def w_relay():
        for kind, share, count in w_parts:
            n = count // 2
            arrived(relay_buf(relay_up, kind), ("w_relay_up", kind))
            send(relay_buf(relay_up, kind), w_rows(dn, share, 0, n), ("w_far0", kind), at_tp(up))
            arrived(relay_buf(relay_dn, kind), ("w_relay_dn", kind))
            send(relay_buf(relay_dn, kind), w_rows(up, share, n, n), ("w_far1", kind), at_tp(dn))

    def w_over_tp():
        for kind, share, count in w_parts:
            n = count // 2
            arrived(w_rows(dn, share, 0, count), ("w_from_dn", kind))
            arrived(w_rows(up, share, 0, count), ("w_from_up", kind))
            arrived(w_rows(far, share, 0, n), ("w_far0", kind))
            arrived(w_rows(far, share, n, n), ("w_far1", kind))

    def send_all(refs, name, dev):
        for i, ref in enumerate(refs):
            send(ref, ref, (name, i), dev)

    def all_arrived(refs, name):
        for i, ref in enumerate(refs):
            arrived(ref, (name, i))

    def ring_start(part, tag):
        send_all(part(p), (tag, "L"), at_cp(right))
        send_all(part(p), (tag, "R"), at_cp(left))
        send_all(part(p), (tag, "M"), at_cp(mate))

    def ring_near(part, tag):
        all_arrived(part(left), (tag, "L"))
        send_all(part(left, 0), (tag, "far0"), at_cp(right))
        send_all(part(left), (tag, "ML"), at_cp(mate))
        all_arrived(part(right), (tag, "R"))
        send_all(part(right, 1), (tag, "far1"), at_cp(left))
        send_all(part(right), (tag, "MR"), at_cp(mate))

    def ring_far(part, tag):
        all_arrived(part(across, 0), (tag, "far0"))
        all_arrived(part(across, 1), (tag, "far1"))
        send_all(part(across), (tag, "MF"), at_cp(mate))

    def mates_near(part, tag):
        all_arrived(part(mate), (tag, "M"))
        all_arrived(part(mate_left), (tag, "ML"))
        all_arrived(part(mate_right), (tag, "MR"))

    def kv_part(g):
        def part(owner, k=None):
            both = [k_all.at[owner, g], vt_all.at[owner, g]]
            return both if k is None else both[k:k + 1]
        return part

    def w_part(owner):
        def part(share, k=None):
            return [w_rows(owner, share, 0, piece) if k is None else w_rows(owner, share, half + k * half // 2, half // 2)]
        return part

    def project(w_ref, store):
        @pl.loop(0, rows // half_rows)
        def _(i):
            r = pl.ds(pl.multiple_of(i * half_rows, 16), half_rows)
            store(r, jnp.dot(x_v[r, :], w_ref[...], preferred_element_type=jnp.float32))

    with jax.named_scope("wait_x"):
        load_x.wait()
        load_k.wait()
    load_q = [load(wq_hbm.at[:, pl.ds(n * COL_TILE, COL_TILE)], wq_v.at[n], ("q", n)) for n in range(q_tiles)]
    own_cols = pl.ds(pl.multiple_of(t * y_cols, 128), y_cols)
    load_o = load(wo_hbm.at[:, own_cols], w_full.at[pl.ds(pl.multiple_of(t * head_cols, 128), head_cols), :], "o")

    def store_k(r, val):
        for g in range(groups):
            k_all[p, g, r, :] = val[:, g * HEAD_DIM:(g + 1) * HEAD_DIM].astype(jnp.bfloat16)

    def store_v(r, val):
        for g in range(groups):
            vt_all[p, g, :, r] = val[:, g * HEAD_DIM:(g + 1) * HEAD_DIM].T.astype(jnp.bfloat16)

    with jax.named_scope("proj_kv"):
        project(wkv_v.at[0], store_k)
        load_v.wait()
        project(wkv_v.at[1], store_v)
    ring_start(kv_part(0), ("kv", 0))

    def q_tile(n):
        load_q[n].wait()

        def store(r, val):
            for k in range(COL_TILE // HEAD_DIM):
                q_v[n * (COL_TILE // HEAD_DIM) + k, r, :HEAD_DIM] = val[:, k * HEAD_DIM:(k + 1) * HEAD_DIM].astype(jnp.bfloat16)
        with jax.named_scope(f"q{n}"):
            project(wq_v.at[n], store)

    def wide(v, n):
        return jnp.concatenate([v] * (n // v.shape[1]), axis=1)

    lane = lax.broadcasted_iota(jnp.int32, (rows, HEAD_DIM), 1)
    first_doc = seg_in[:, :1]

    def set_bias():
        seg_col[...] = jnp.broadcast_to(seg_in[...], (HEAD_DIM, rows)).T

        @pl.loop(0, rows // HEAD_DIM)
        def _(i):
            r = pl.ds(pl.multiple_of(i * HEAD_DIM, HEAD_DIM), HEAD_DIM)
            allowed = wide(seg_col[r, :], rows) == seg_in[...]
            allowed &= (lax.broadcasted_iota(jnp.int32, (HEAD_DIM, rows), 0) + i * HEAD_DIM
                        <= lax.broadcasted_iota(jnp.int32, (HEAD_DIM, rows), 1))
            bias[r, :] = jnp.where(allowed, 0.0, NEG_INF)

    def set_mask(block):
        of_key = jnp.broadcast_to(segs[block], (HEAD_DIM, rows)).T
        shut = (of_key != first_doc) & (lane == 0)
        k_mask[block] = jnp.where(shut, NEG_INF, 0.0).astype(jnp.bfloat16)

    def visit(pair, blocks, diagonal=False):
        g = pair * PAIR // per_group
        units = [(block, h, i) for block in blocks for h in range(PAIR) for i in range(2)]
        scratch = [s_even, s_odd]

        def keys(i):
            return half_rows if diagonal and i == 0 else rows

        def scores(n):
            block, h, i = units[n]
            c = slice(i * half_rows, (i + 1) * half_rows)
            q = q_v[pair * PAIR + h, c, :]
            k = k_all[block, g, :keys(i), :]
            if diagonal:
                s = lax.dot_general(k, q[:, :HEAD_DIM], (((1,), (1,)), ((), ())), preferred_element_type=jnp.float32)
                s += bias[:keys(i), c]
            else:
                k = jnp.concatenate([k, k_mask[block]], axis=1)
                s = lax.dot_general(k, q, (((1,), (1,)), ((), ())), preferred_element_type=jnp.float32)
            scratch[n % 2][:keys(i), :] = s
            return jnp.max(s, axis=0, keepdims=True)

        def absorb(n, top):
            block, h, i = units[n]
            c = slice(i * half_rows, (i + 1) * half_rows)
            if diagonal:
                new_max = shift = top
            else:
                in_first = seg_in[:, c] == first_doc
                old_max = m_s[h, :, c]
                new_max = jnp.where(in_first, jnp.maximum(old_max, top), old_max)
                shift = jnp.where(in_first, new_max, -NEG_INF)
            prob = jnp.exp2(scratch[n % 2][:keys(i), :] * SCALE - shift * SCALE)
            total = jnp.sum(prob, axis=0, keepdims=True)
            out = jnp.dot(vt_all[block, g, :, :keys(i)], prob.astype(jnp.bfloat16), preferred_element_type=jnp.float32)
            if not diagonal:
                rescale = jnp.exp2((old_max - new_max) * SCALE)
                total += l_s[h, :, c] * rescale
                out += acc_s[h, :, c] * rescale
            m_s[h, :, c] = new_max
            l_s[h, :, c] = total
            acc_s[h, :, c] = out

        top = scores(0)
        for n in range(len(units)):
            ahead = scores(n + 1) if n + 1 < len(units) else None
            absorb(n, top)
            top = ahead

    def visit_mate(pair):
        @pl.when(core == 1)
        def _():
            if pair == 0:
                set_mask(mate)
            visit(pair, [mate])

    def visit_chips(pair, count, chip_of):
        @pl.loop(0, count)
        def _(i):
            chip = chip_of(i)

            @pl.when(chip < col)
            def _():
                if pair == 0:
                    set_mask(chip * 2)
                    set_mask(chip * 2 + 1)
                visit(pair, [chip * 2, chip * 2 + 1])

    def visit_near(pair):
        visit_mate(pair)
        visit_chips(pair, 2, lambda i: jnp.where(i == 0, left_chip, right_chip))

    def visit_far(pair):
        visit_chips(pair, 1, lambda i: far_chip + i)

    def visit_all(pair):
        visit_mate(pair)
        visit_chips(pair, chips, lambda i: i)

    def o_cols(owner, h):
        return o_all.at[:, pl.ds(pl.multiple_of(owner * head_cols + h * HEAD_DIM, 128), HEAD_DIM)]

    def o_finish(pair):
        for k in range(PAIR):
            h = pair * PAIR + k
            o_all[:, pl.ds(pl.multiple_of(t * head_cols + h * HEAD_DIM, 128), HEAD_DIM)] = (
                acc_s[k] / l_s[k]).T.astype(jnp.bfloat16)
            send(o_cols(t, h), o_cols(t, h), ("o", h, "D"), at_tp(up))
            send(o_cols(t, h), o_cols(t, h), ("o", h, "U"), at_tp(dn))

    def o_relay(h):
        arrived(o_cols(dn, h), ("o", h, "D"))
        arrived(o_cols(up, h), ("o", h, "U"))
        if h % 2 == 0:
            send(o_cols(dn, h), o_cols(dn, h), ("o", h, "F"), at_tp(up))
        else:
            send(o_cols(up, h), o_cols(up, h), ("o", h, "F"), at_tp(dn))

    kv = [(kv_part(g), ("kv", g)) for g in range(groups)]
    w = [(w_part(lax.rem(t + j, tp)), ("w", j)) for j in range(1, tp)]

    q_v[:, :, HEAD_DIM:] = jnp.where(lax.broadcasted_iota(jnp.int32, (heads, rows, HEAD_DIM), 2) == 0, 1.0, 0.0).astype(jnp.bfloat16)
    scope = jax.named_scope

    def o_relay_pair(pair):
        with scope(f"o_relay{pair}"):
            for k in range(PAIR):
                o_relay(pair * PAIR + k)

    q_tile(0)
    with scope("diag0"):
        set_bias()
        visit(0, [p], diagonal=True)
    with scope("w_relay"):
        w_relay()
    q_tile(1)
    q_tile(2)
    with scope("kv0_near"):
        ring_near(*kv[0])
        ring_start(*kv[1])
    with scope("kv0_mate"):
        load_seg.wait()
        for k in range(1, cp):
            arrived(segs.at[lax.rem(p + cp - k, cp)], ("seg", k))
        mates_near(*kv[0])
    with scope("near0"):
        visit_near(0)
    with scope("w_tp"):
        w_over_tp()
        ring_start(*w[0])
    with scope("kv0_far"):
        ring_far(*kv[0])
    q_tile(3)
    with scope("kv0_mf"):
        all_arrived(kv[0][0](mate_across), (kv[0][1], "MF"))
    with scope("far0"):
        visit_far(0)
    with scope("o_fin0"):
        o_finish(0)
    with scope("kv1_near"):
        ring_near(*kv[1])
    with scope("pair1"):
        visit(1, [p], diagonal=True)
        visit_all(1)
        o_finish(1)
    ring_start(*w[1])
    ring_start(*w[2])
    o_relay_pair(0)
    with scope("diag2"):
        visit(2, [p], diagonal=True)
    with scope("kv1_mate"):
        mates_near(*kv[1])
    with scope("near2"):
        visit_near(2)
    with scope("kv1_far"):
        ring_far(*kv[1])
        all_arrived(kv[1][0](mate_across), (kv[1][1], "MF"))
    with scope("far2"):
        visit_far(2)
        o_finish(2)
    with scope("w1_near"):
        ring_near(*w[0])
    o_relay_pair(1)
    with scope("pair3"):
        visit(3, [p], diagonal=True)
        visit_all(3)
        o_finish(3)
    with scope("w2_near"):
        ring_near(*w[1])
    o_relay_pair(2)
    with scope("w3_near"):
        ring_near(*w[2])
    o_relay_pair(3)
    with scope("w_far"):
        for part in w:
            ring_far(*part)
    with scope("w_mate"):
        for part, tag in w:
            mates_near(part, tag)
            all_arrived(part(mate_across), (tag, "MF"))
    with scope("o_far"):
        for h in range(heads):
            arrived(o_cols(far, h), ("o", h, "F"))
        load_o.wait()

    def y_at(owner, n, k=None):
        cols = pl.ds(pl.multiple_of(owner * y_cols + n * COL_TILE, 128), COL_TILE)
        return y_hbm.at[:, cols] if k is None else y_hbm.at[pl.ds(k * half_rows, half_rows), cols]

    copies = []
    tiles = y_cols // COL_TILE
    for n in range(tiles):
        c = pl.ds(n * COL_TILE, COL_TILE)

        @pl.loop(0, 2)
        def _(i):
          with jax.named_scope("y_mm"):
            r = pl.ds(pl.multiple_of(i * half_rows, 16), half_rows)
            y_own[r, c] = jnp.dot(o_all[r, :], w_full[:, c], preferred_element_type=jnp.float32).astype(jnp.bfloat16)
        send(y_own.at[:, c], y_at(t, n), ("y", n, "D"), at_tp(up))
        send(y_own.at[:, c], y_at(t, n), ("y", n, "U"), at_tp(dn))
        copies.append(load(y_own.at[:, c], y_at(t, n), ("y", n)))
    for n in range(tiles):
      with jax.named_scope(f"y_relay{n}"):
        arrived(y_at(dn, n), ("y", n, "D"))
        send(y_at(dn, n, 0), y_at(dn, n, 0), ("y", n, "F0"), at_tp(up))
        arrived(y_at(up, n), ("y", n, "U"))
        send(y_at(up, n, 1), y_at(up, n, 1), ("y", n, "F1"), at_tp(dn))
    for n in range(tiles):
      with jax.named_scope(f"y_far{n}"):
        arrived(y_at(far, n, 0), ("y", n, "F0"))
        arrived(y_at(far, n, 1), ("y", n, "F1"))
    for c in copies:
        c.wait()
    for c in waiting:
        c.wait_send()


def solution(mesh):
    tp, cp = mesh.shape["tp"], mesh.shape["cp"]

    def local_attention(x_loc, seg_loc, w_query, w_key, w_value, w_out):
        rows, width = x_loc.shape
        heads = w_query.shape[1] // HEAD_DIM
        groups = w_key.shape[1] // HEAD_DIM
        head_cols = heads * HEAD_DIM
        y_cols = width // tp
        bf16, f32 = jnp.bfloat16, jnp.float32
        hbm = pl.BlockSpec(memory_space=pl.ANY)
        return pl.pallas_call(
            functools.partial(kernel, tp, cp),
            out_shape=jax.ShapeDtypeStruct((rows, width), bf16),
            in_specs=[hbm, pl.BlockSpec(memory_space=pltpu.VMEM), hbm, hbm, hbm, hbm],
            out_specs=hbm,
            scratch_shapes=[
                pltpu.VMEM((rows, width), bf16),
                pltpu.VMEM((2, width, groups * HEAD_DIM), bf16),
                pltpu.VMEM((head_cols // COL_TILE, width, COL_TILE), bf16),
                pltpu.VMEM((tp * head_cols, y_cols), bf16),
                pltpu.VMEM((cp, groups, rows, HEAD_DIM), bf16),
                pltpu.VMEM((cp, groups, HEAD_DIM, rows), bf16),
                pltpu.VMEM((cp, 1, rows), jnp.int32),
                pltpu.VMEM((rows, HEAD_DIM), jnp.int32),
                pltpu.VMEM((rows, rows), f32),
                pltpu.VMEM((cp, rows, HEAD_DIM), bf16),
                pltpu.VMEM((rows, rows // 2), f32),
                pltpu.VMEM((rows, rows // 2), f32),
                pltpu.VMEM((heads, rows, 2 * HEAD_DIM), bf16),
                pltpu.VMEM((rows, tp * head_cols), bf16),
                pltpu.VMEM((rows, y_cols), bf16),
                pltpu.VMEM((head_cols // cp * 3 // 4, y_cols), bf16),
                pltpu.VMEM((head_cols // cp * 3 // 4, y_cols), bf16),
                pltpu.VMEM((PAIR, 1, rows), f32),
                pltpu.VMEM((PAIR, 1, rows), f32),
                pltpu.VMEM((PAIR, HEAD_DIM, rows), f32),
                pltpu.SemaphoreType.DMA((32,)),
                pltpu.SemaphoreType.DMA((224,)),
                pltpu.SemaphoreType.DMA((224,)),
            ],
            compiler_params=pltpu.CompilerParams(collective_id=0, has_side_effects=True, vmem_limit_bytes=67043328),
        )(x_loc, seg_loc.reshape(1, rows), w_query, w_key, w_value, w_out)

    return jax.shard_map(local_attention, mesh=mesh, in_specs=(P(('dp', 'cp'), None), P(('dp', 'cp')), P(None, 'tp'), P(None, 'tp'), P(None, 'tp'), P('tp', None)), out_specs=P(('dp', 'cp'), None), check_vma=False)
```

```python
import functools

import jax
import jax.numpy as jnp
from jax import lax
from jax.experimental import pallas as pl
from jax.experimental.pallas import tpu as pltpu
from jax.sharding import PartitionSpec as P


HEAD_DIM = 128
COL_TILE = 256
DEPTH_CUTS = 4
PAIR = 2
MESH = pl.DeviceIdType.MESH
SCALE = HEAD_DIM**-0.5 * 1.4426950408889634
NEG_INF = float("-inf")


class Sems:
    def __init__(self, ref):
        self.ref, self.names = ref, {}

    def __getitem__(self, name):
        return self.ref.at[self.names.setdefault(name, len(self.names))]


def kernel(tp, cp, x_hbm, seg_in, wq_hbm, wk_hbm, wv_hbm, wo_hbm, y_hbm,
           x_v, wkv_v, wq_v, w_full, k_all, vt_all, segs, seg_col, bias, k_mask, s_even, s_odd, kv_acc, q_v, o_all, y_own, relay_up, relay_dn,
           m_s, l_s, acc_s, load_sem, send_sem, recv_sem):
    t, p = lax.axis_index("tp"), lax.axis_index("cp")
    chips = cp // 2
    col, core = p // 2, lax.rem(p, 2)
    up, dn, far = lax.rem(t + 1, tp), lax.rem(t + tp - 1, tp), lax.rem(t + 2, tp)
    right_chip, left_chip, far_chip = lax.rem(col + 1, chips), lax.rem(col + chips - 1, chips), lax.rem(col + 2, chips)
    right, left, across = right_chip * 2 + core, left_chip * 2 + core, far_chip * 2 + core
    mate = col * 2 + 1 - core
    mate_right, mate_left, mate_across = right_chip * 2 + 1 - core, left_chip * 2 + 1 - core, far_chip * 2 + 1 - core

    rows = x_v.shape[0]
    heads = q_v.shape[0]
    groups = k_all.shape[1]
    per_group = heads // groups
    head_cols = heads * HEAD_DIM
    y_cols = y_own.shape[1]
    piece = head_cols // cp
    half = piece // 2
    half_rows = rows // 2

    loads, sends, recvs = Sems(load_sem), Sems(send_sem), Sems(recv_sem)
    waiting = []

    def at_tp(i):
        return {"tp": i, "cp": p}

    def at_cp(i):
        return {"tp": t, "cp": i}

    def send(src, dst, name, dev):
        c = pltpu.make_async_remote_copy(src_ref=src, dst_ref=dst, send_sem=sends[(name, len(waiting))],
                                         recv_sem=recvs[name], device_id=dev, device_id_type=MESH)
        c.start()
        waiting.append(c)

    def arrived(dst, name):
        pltpu.make_async_remote_copy(src_ref=dst, dst_ref=dst, send_sem=sends[0], recv_sem=recvs[name],
                                     device_id=at_cp(p), device_id_type=MESH).wait_recv()

    def load(src, dst, name):
        c = pltpu.make_async_copy(src, dst, loads[name])
        c.start()
        return c

    depth = x_v.shape[1] // DEPTH_CUTS
    cuts = [pl.ds(i * depth, depth) for i in range(DEPTH_CUTS)]
    load_kv = [(load(x_hbm.at[:, c], x_v.at[:, c], ("x", i)), load(wk_hbm.at[c, :], wkv_v.at[0, c, :], ("k", i)),
                load(wv_hbm.at[c, :], wkv_v.at[1, c, :], ("v", i))) for i, c in enumerate(cuts)]
    q_tiles = head_cols // COL_TILE

    barrier = pltpu.get_barrier_semaphore()
    peers = [at_tp(up), at_tp(dn)] + [at_cp(lax.rem(p + k, cp)) for k in range(1, cp)]
    for dev in peers:
        pl.semaphore_signal(barrier, inc=1, device_id=dev, device_id_type=MESH)
    pl.semaphore_wait(barrier, len(peers))

    for k in range(1, cp):
        send(seg_in, segs.at[p], ("seg", k), at_cp(lax.rem(p + k, cp)))
    load_seg = load(seg_in, segs.at[p], "seg")

    def w_rows(owner, share, start, count):
        return w_full.at[pl.ds(pl.multiple_of(owner * head_cols + share * piece + start, 16), count), :]

    def w_src(dest, share, start, count):
        return wo_hbm.at[pl.ds(pl.multiple_of(share * piece + start, 16), count),
                         pl.ds(pl.multiple_of(dest * y_cols, 128), y_cols)]

    w_parts = [("own", p, piece), ("far", across, half)]

    def relay_buf(buf, kind):
        return buf.at[pl.ds(0, half)] if kind == "own" else buf.at[pl.ds(half, half // 2)]

    for kind, share, count in w_parts:
        n = count // 2
        send(w_src(far, share, 0, n), relay_buf(relay_up, kind), ("w_relay_up", kind), at_tp(up))
        send(w_src(far, share, n, n), relay_buf(relay_dn, kind), ("w_relay_dn", kind), at_tp(dn))

    def w_relay():
        for kind, share, count in w_parts:
            n = count // 2
            arrived(relay_buf(relay_up, kind), ("w_relay_up", kind))
            send(relay_buf(relay_up, kind), w_rows(dn, share, 0, n), ("w_far0", kind), at_tp(up))
            arrived(relay_buf(relay_dn, kind), ("w_relay_dn", kind))
            send(relay_buf(relay_dn, kind), w_rows(up, share, n, n), ("w_far1", kind), at_tp(dn))
            send(w_src(up, share, 0, count), w_rows(t, share, 0, count), ("w_from_dn", kind), at_tp(up))
            send(w_src(dn, share, 0, count), w_rows(t, share, 0, count), ("w_from_up", kind), at_tp(dn))

    def w_over_tp():
        for kind, share, count in w_parts:
            n = count // 2
            arrived(w_rows(dn, share, 0, count), ("w_from_dn", kind))
            arrived(w_rows(up, share, 0, count), ("w_from_up", kind))
            arrived(w_rows(far, share, 0, n), ("w_far0", kind))
            arrived(w_rows(far, share, n, n), ("w_far1", kind))

    def send_all(refs, name, dev):
        for i, ref in enumerate(refs):
            send(ref, ref, (name, i), dev)

    def all_arrived(refs, name):
        for i, ref in enumerate(refs):
            arrived(ref, (name, i))

    def ring_start(part, tag):
        send_all(part(p), (tag, "L"), at_cp(right))
        send_all(part(p), (tag, "R"), at_cp(left))
        send_all(part(p), (tag, "M"), at_cp(mate))

    def ring_near(part, tag):
        all_arrived(part(left), (tag, "L"))
        send_all(part(left, 0), (tag, "far0"), at_cp(right))
        send_all(part(left), (tag, "ML"), at_cp(mate))
        all_arrived(part(right), (tag, "R"))
        send_all(part(right, 1), (tag, "far1"), at_cp(left))
        send_all(part(right), (tag, "MR"), at_cp(mate))

    def ring_far(part, tag):
        all_arrived(part(across, 0), (tag, "far0"))
        all_arrived(part(across, 1), (tag, "far1"))
        send_all(part(across), (tag, "MF"), at_cp(mate))

    def mates_near(part, tag):
        all_arrived(part(mate), (tag, "M"))
        all_arrived(part(mate_left), (tag, "ML"))
        all_arrived(part(mate_right), (tag, "MR"))

    def kv_part(g):
        def part(owner, k=None):
            both = [k_all.at[owner, g], vt_all.at[owner, g]]
            return both if k is None else both[k:k + 1]
        return part

    def w_part(owner):
        def part(share, k=None):
            return [w_rows(owner, share, 0, piece) if k is None else w_rows(owner, share, half + k * half // 2, half // 2)]
        return part

    def project(w_ref, store):
        @pl.loop(0, rows // half_rows)
        def _(i):
            r = pl.ds(pl.multiple_of(i * half_rows, 16), half_rows)
            store(r, jnp.dot(x_v[r, :], w_ref[...], preferred_element_type=jnp.float32))

    def store_k(r, val):
        for g in range(groups):
            k_all[p, g, r, :] = val[:, g * HEAD_DIM:(g + 1) * HEAD_DIM].astype(jnp.bfloat16)

    def store_v(r, val):
        for g in range(groups):
            vt_all[p, g, :, r] = val[:, g * HEAD_DIM:(g + 1) * HEAD_DIM].T.astype(jnp.bfloat16)

    for i, c in enumerate(cuts):
        with jax.named_scope("wait_x"):
            for copy in load_kv[i]:
                copy.wait()
        with jax.named_scope("proj_kv"):
            @pl.loop(0, 2)
            def _(half_of):
                r = pl.ds(pl.multiple_of(half_of * half_rows, 16), half_rows)
                for kind, store in enumerate((store_k, store_v)):
                    val = jnp.dot(x_v[r, c], wkv_v[kind, c, :], preferred_element_type=jnp.float32)
                    if i > 0:
                        val += kv_acc[kind, r, :]
                    if i + 1 < len(cuts):
                        kv_acc[kind, r, :] = val
                    else:
                        store(r, val)
    load_q = [load(wq_hbm.at[:, pl.ds(n * COL_TILE, COL_TILE)], wq_v.at[n], ("q", n)) for n in range(q_tiles)]
    own_cols = pl.ds(pl.multiple_of(t * y_cols, 128), y_cols)
    load_o = load(wo_hbm.at[:, own_cols], w_full.at[pl.ds(pl.multiple_of(t * head_cols, 128), head_cols), :], "o")

    ring_start(kv_part(0), ("kv", 0))

    def q_tile(n):
        load_q[n].wait()

        def store(r, val):
            for k in range(COL_TILE // HEAD_DIM):
                q_v[n * (COL_TILE // HEAD_DIM) + k, r, :HEAD_DIM] = val[:, k * HEAD_DIM:(k + 1) * HEAD_DIM].astype(jnp.bfloat16)
        with jax.named_scope(f"q{n}"):
            project(wq_v.at[n], store)

    def wide(v, n):
        return jnp.concatenate([v] * (n // v.shape[1]), axis=1)

    lane = lax.broadcasted_iota(jnp.int32, (rows, HEAD_DIM), 1)
    first_doc = seg_in[:, :1]

    def set_bias():
        seg_col[...] = jnp.broadcast_to(seg_in[...], (HEAD_DIM, rows)).T

        @pl.loop(0, rows // HEAD_DIM)
        def _(i):
            r = pl.ds(pl.multiple_of(i * HEAD_DIM, HEAD_DIM), HEAD_DIM)
            allowed = wide(seg_col[r, :], rows) == seg_in[...]
            allowed &= (lax.broadcasted_iota(jnp.int32, (HEAD_DIM, rows), 0) + i * HEAD_DIM
                        <= lax.broadcasted_iota(jnp.int32, (HEAD_DIM, rows), 1))
            bias[r, :] = jnp.where(allowed, 0.0, NEG_INF)

    def set_mask(block):
        of_key = jnp.broadcast_to(segs[block], (HEAD_DIM, rows)).T
        shut = (of_key != first_doc) & (lane == 0)
        k_mask[block] = jnp.where(shut, NEG_INF, 0.0).astype(jnp.bfloat16)

    def visit(pair, blocks, diagonal=False):
        g = pair * PAIR // per_group
        units = [(block, h, i) for block in blocks for h in range(PAIR) for i in range(2)]
        scratch = [s_even, s_odd]

        def keys(i):
            return half_rows if diagonal and i == 0 else rows

        def scores(n):
            block, h, i = units[n]
            c = slice(i * half_rows, (i + 1) * half_rows)
            q = q_v[pair * PAIR + h, c, :]
            k = k_all[block, g, :keys(i), :]
            if diagonal:
                s = lax.dot_general(k, q[:, :HEAD_DIM], (((1,), (1,)), ((), ())), preferred_element_type=jnp.float32)
                s += bias[:keys(i), c]
            else:
                k = jnp.concatenate([k, k_mask[block]], axis=1)
                s = lax.dot_general(k, q, (((1,), (1,)), ((), ())), preferred_element_type=jnp.float32)
            scratch[n % 2][:keys(i), :] = s
            return jnp.max(s, axis=0, keepdims=True)

        def absorb(n, top):
            block, h, i = units[n]
            c = slice(i * half_rows, (i + 1) * half_rows)
            if diagonal:
                new_max = shift = top
            else:
                in_first = seg_in[:, c] == first_doc
                old_max = m_s[h, :, c]
                new_max = jnp.where(in_first, jnp.maximum(old_max, top), old_max)
                shift = jnp.where(in_first, new_max, -NEG_INF)
            prob = jnp.exp2(scratch[n % 2][:keys(i), :] * SCALE - shift * SCALE)
            total = jnp.sum(prob, axis=0, keepdims=True)
            out = jnp.dot(vt_all[block, g, :, :keys(i)], prob.astype(jnp.bfloat16), preferred_element_type=jnp.float32)
            if not diagonal:
                rescale = jnp.exp2((old_max - new_max) * SCALE)
                total += l_s[h, :, c] * rescale
                out += acc_s[h, :, c] * rescale
            m_s[h, :, c] = new_max
            l_s[h, :, c] = total
            acc_s[h, :, c] = out

        top = scores(0)
        for n in range(len(units)):
            ahead = scores(n + 1) if n + 1 < len(units) else None
            absorb(n, top)
            top = ahead

    def visit_mate(pair):
        @pl.when(core == 1)
        def _():
            if pair == 0:
                set_mask(mate)
            visit(pair, [mate])

    def visit_chips(pair, count, chip_of):
        @pl.loop(0, count)
        def _(i):
            chip = chip_of(i)

            @pl.when(chip < col)
            def _():
                if pair == 0:
                    set_mask(chip * 2)
                    set_mask(chip * 2 + 1)
                visit(pair, [chip * 2, chip * 2 + 1])

    def visit_near(pair):
        visit_mate(pair)
        visit_chips(pair, 2, lambda i: jnp.where(i == 0, left_chip, right_chip))

    def visit_far(pair):
        visit_chips(pair, 1, lambda i: far_chip + i)

    def visit_all(pair):
        visit_mate(pair)
        visit_chips(pair, chips, lambda i: i)

    def o_cols(owner, h):
        return o_all.at[:, pl.ds(pl.multiple_of(owner * head_cols + h * HEAD_DIM, 128), HEAD_DIM)]

    def o_finish(pair):
        for k in range(PAIR):
            h = pair * PAIR + k
            o_all[:, pl.ds(pl.multiple_of(t * head_cols + h * HEAD_DIM, 128), HEAD_DIM)] = (
                acc_s[k] / l_s[k]).T.astype(jnp.bfloat16)
            send(o_cols(t, h), o_cols(t, h), ("o", h, "D"), at_tp(up))
            send(o_cols(t, h), o_cols(t, h), ("o", h, "U"), at_tp(dn))

    def o_relay(h):
        arrived(o_cols(dn, h), ("o", h, "D"))
        arrived(o_cols(up, h), ("o", h, "U"))
        if h % 2 == 0:
            send(o_cols(dn, h), o_cols(dn, h), ("o", h, "F"), at_tp(up))
        else:
            send(o_cols(up, h), o_cols(up, h), ("o", h, "F"), at_tp(dn))

    kv = [(kv_part(g), ("kv", g)) for g in range(groups)]
    w = [(w_part(lax.rem(t + j, tp)), ("w", j)) for j in range(1, tp)]

    q_v[:, :, HEAD_DIM:] = jnp.where(lax.broadcasted_iota(jnp.int32, (heads, rows, HEAD_DIM), 2) == 0, 1.0, 0.0).astype(jnp.bfloat16)
    scope = jax.named_scope

    def o_relay_pair(pair):
        with scope(f"o_relay{pair}"):
            for k in range(PAIR):
                o_relay(pair * PAIR + k)

    with scope("w_relay"):
        w_relay()
    q_tile(0)
    with scope("diag0"):
        set_bias()
        visit(0, [p], diagonal=True)
    q_tile(1)
    q_tile(2)
    with scope("kv0_near"):
        ring_near(*kv[0])
        ring_start(*kv[1])
    with scope("kv0_mate"):
        load_seg.wait()
        for k in range(1, cp):
            arrived(segs.at[lax.rem(p + cp - k, cp)], ("seg", k))
        mates_near(*kv[0])
    with scope("near0"):
        visit_near(0)
    with scope("kv0_far"):
        ring_far(*kv[0])
    q_tile(3)
    with scope("kv0_mf"):
        all_arrived(kv[0][0](mate_across), (kv[0][1], "MF"))
    with scope("far0"):
        visit_far(0)
    with scope("o_fin0"):
        o_finish(0)
    with scope("kv1_near"):
        ring_near(*kv[1])
    with scope("w_tp"):
        w_over_tp()
        ring_start(*w[0])
    with scope("pair1"):
        visit(1, [p], diagonal=True)
        visit_all(1)
        o_finish(1)
    ring_start(*w[1])
    ring_start(*w[2])
    o_relay_pair(0)
    with scope("diag2"):
        visit(2, [p], diagonal=True)
    with scope("kv1_mate"):
        mates_near(*kv[1])
    with scope("near2"):
        visit_near(2)
    with scope("kv1_far"):
        ring_far(*kv[1])
        all_arrived(kv[1][0](mate_across), (kv[1][1], "MF"))
    with scope("far2"):
        visit_far(2)
        o_finish(2)
    with scope("w1_near"):
        ring_near(*w[0])
    o_relay_pair(1)
    with scope("pair3"):
        visit(3, [p], diagonal=True)
        visit_all(3)
        o_finish(3)
    with scope("w2_near"):
        ring_near(*w[1])
    o_relay_pair(2)
    with scope("w3_near"):
        ring_near(*w[2])
    o_relay_pair(3)
    with scope("w_far"):
        for part in w:
            ring_far(*part)
    with scope("w_mate"):
        for part, tag in w:
            mates_near(part, tag)
            all_arrived(part(mate_across), (tag, "MF"))
    with scope("o_far"):
        for h in range(heads):
            arrived(o_cols(far, h), ("o", h, "F"))
        load_o.wait()

    def y_at(owner, n, k=None):
        cols = pl.ds(pl.multiple_of(owner * y_cols + n * COL_TILE, 128), COL_TILE)
        return y_hbm.at[:, cols] if k is None else y_hbm.at[pl.ds(k * half_rows, half_rows), cols]

    copies = []
    tiles = y_cols // COL_TILE
    for n in range(tiles):
        c = pl.ds(n * COL_TILE, COL_TILE)

        @pl.loop(0, 2)
        def _(i):
          with jax.named_scope("y_mm"):
            r = pl.ds(pl.multiple_of(i * half_rows, 16), half_rows)
            y_own[r, c] = jnp.dot(o_all[r, :], w_full[:, c], preferred_element_type=jnp.float32).astype(jnp.bfloat16)
        send(y_own.at[:, c], y_at(t, n), ("y", n, "D"), at_tp(up))
        send(y_own.at[:, c], y_at(t, n), ("y", n, "U"), at_tp(dn))
        copies.append(load(y_own.at[:, c], y_at(t, n), ("y", n)))
    for n in range(tiles):
      with jax.named_scope(f"y_relay{n}"):
        arrived(y_at(dn, n), ("y", n, "D"))
        send(y_at(dn, n, 0), y_at(dn, n, 0), ("y", n, "F0"), at_tp(up))
        arrived(y_at(up, n), ("y", n, "U"))
        send(y_at(up, n, 1), y_at(up, n, 1), ("y", n, "F1"), at_tp(dn))
    for n in range(tiles):
      with jax.named_scope(f"y_far{n}"):
        arrived(y_at(far, n, 0), ("y", n, "F0"))
        arrived(y_at(far, n, 1), ("y", n, "F1"))
    for c in copies:
        c.wait()
    for c in waiting:
        c.wait_send()


def solution(mesh):
    tp, cp = mesh.shape["tp"], mesh.shape["cp"]

    def local_attention(x_loc, seg_loc, w_query, w_key, w_value, w_out):
        rows, width = x_loc.shape
        heads = w_query.shape[1] // HEAD_DIM
        groups = w_key.shape[1] // HEAD_DIM
        head_cols = heads * HEAD_DIM
        y_cols = width // tp
        bf16, f32 = jnp.bfloat16, jnp.float32
        hbm = pl.BlockSpec(memory_space=pl.ANY)
        return pl.pallas_call(
            functools.partial(kernel, tp, cp),
            out_shape=jax.ShapeDtypeStruct((rows, width), bf16),
            in_specs=[hbm, pl.BlockSpec(memory_space=pltpu.VMEM), hbm, hbm, hbm, hbm],
            out_specs=hbm,
            scratch_shapes=[
                pltpu.VMEM((rows, width), bf16),
                pltpu.VMEM((2, width, groups * HEAD_DIM), bf16),
                pltpu.VMEM((head_cols // COL_TILE, width, COL_TILE), bf16),
                pltpu.VMEM((tp * head_cols, y_cols), bf16),
                pltpu.VMEM((cp, groups, rows, HEAD_DIM), bf16),
                pltpu.VMEM((cp, groups, HEAD_DIM, rows), bf16),
                pltpu.VMEM((cp, 1, rows), jnp.int32),
                pltpu.VMEM((rows, HEAD_DIM), jnp.int32),
                pltpu.VMEM((rows, rows), f32),
                pltpu.VMEM((cp, rows, HEAD_DIM), bf16),
                pltpu.VMEM((rows, rows // 2), f32),
                pltpu.VMEM((rows, rows // 2), f32),
                pltpu.VMEM((2, rows, groups * HEAD_DIM), f32),
                pltpu.VMEM((heads, rows, 2 * HEAD_DIM), bf16),
                pltpu.VMEM((rows, tp * head_cols), bf16),
                pltpu.VMEM((rows, y_cols), bf16),
                pltpu.VMEM((head_cols // cp * 3 // 4, y_cols), bf16),
                pltpu.VMEM((head_cols // cp * 3 // 4, y_cols), bf16),
                pltpu.VMEM((PAIR, 1, rows), f32),
                pltpu.VMEM((PAIR, 1, rows), f32),
                pltpu.VMEM((PAIR, HEAD_DIM, rows), f32),
                pltpu.SemaphoreType.DMA((32,)),
                pltpu.SemaphoreType.DMA((224,)),
                pltpu.SemaphoreType.DMA((224,)),
            ],
            compiler_params=pltpu.CompilerParams(collective_id=0, has_side_effects=True, vmem_limit_bytes=67043328),
        )(x_loc, seg_loc.reshape(1, rows), w_query, w_key, w_value, w_out)

    return jax.shard_map(local_attention, mesh=mesh, in_specs=(P(('dp', 'cp'), None), P(('dp', 'cp')), P(None, 'tp'), P(None, 'tp'), P(None, 'tp'), P('tp', None)), out_specs=P(('dp', 'cp'), None), check_vma=False)
```

```python
import functools

import jax
import jax.numpy as jnp
from jax import lax
from jax.experimental import pallas as pl
from jax.experimental.pallas import tpu as pltpu
from jax.sharding import PartitionSpec as P


HEAD_DIM = 128
COL_TILE = 256
DEPTH_CUTS = 4
PAIR = 2
MESH = pl.DeviceIdType.MESH
SCALE = HEAD_DIM**-0.5 * 1.4426950408889634
NEG_INF = float("-inf")


class Sems:
    def __init__(self, ref):
        self.ref, self.names = ref, {}

    def __getitem__(self, name):
        return self.ref.at[self.names.setdefault(name, len(self.names))]


def kernel(tp, cp, x_hbm, seg_in, wq_hbm, wk_hbm, wv_hbm, wo_hbm, y_ref,
           x_v, wkv_v, wq_v, w_full, k_all, vt_all, segs, seg_col, bias, k_mask, s_even, s_odd, kv_acc, q_v, o_all, relay_up, relay_dn,
           m_s, l_s, acc_s, load_sem, send_sem, recv_sem):
    t, p = lax.axis_index("tp"), lax.axis_index("cp")
    chips = cp // 2
    col, core = p // 2, lax.rem(p, 2)
    up, dn, far = lax.rem(t + 1, tp), lax.rem(t + tp - 1, tp), lax.rem(t + 2, tp)
    right_chip, left_chip, far_chip = lax.rem(col + 1, chips), lax.rem(col + chips - 1, chips), lax.rem(col + 2, chips)
    right, left, across = right_chip * 2 + core, left_chip * 2 + core, far_chip * 2 + core
    mate = col * 2 + 1 - core
    mate_right, mate_left, mate_across = right_chip * 2 + 1 - core, left_chip * 2 + 1 - core, far_chip * 2 + 1 - core

    rows = x_v.shape[0]
    heads = q_v.shape[0]
    groups = k_all.shape[1]
    per_group = heads // groups
    head_cols = heads * HEAD_DIM
    y_cols = w_full.shape[1]
    piece = head_cols // cp
    half = piece // 2
    half_rows = rows // 2

    loads, sends, recvs = Sems(load_sem), Sems(send_sem), Sems(recv_sem)
    waiting = []

    def at_tp(i):
        return {"tp": i, "cp": p}

    def at_cp(i):
        return {"tp": t, "cp": i}

    def send(src, dst, name, dev):
        c = pltpu.make_async_remote_copy(src_ref=src, dst_ref=dst, send_sem=sends[(name, len(waiting))],
                                         recv_sem=recvs[name], device_id=dev, device_id_type=MESH)
        c.start()
        waiting.append(c)

    def arrived(dst, name):
        pltpu.make_async_remote_copy(src_ref=dst, dst_ref=dst, send_sem=sends[0], recv_sem=recvs[name],
                                     device_id=at_cp(p), device_id_type=MESH).wait_recv()

    def load(src, dst, name):
        c = pltpu.make_async_copy(src, dst, loads[name])
        c.start()
        return c

    depth = x_v.shape[1] // DEPTH_CUTS
    cuts = [pl.ds(i * depth, depth) for i in range(DEPTH_CUTS)]
    load_kv = [(load(x_hbm.at[:, c], x_v.at[:, c], ("x", i)), load(wk_hbm.at[c, :], wkv_v.at[0, c, :], ("k", i)),
                load(wv_hbm.at[c, :], wkv_v.at[1, c, :], ("v", i))) for i, c in enumerate(cuts)]
    q_tiles = head_cols // COL_TILE

    barrier = pltpu.get_barrier_semaphore()
    peers = [at_tp(up), at_tp(dn)] + [at_cp(lax.rem(p + k, cp)) for k in range(1, cp)]
    for dev in peers:
        pl.semaphore_signal(barrier, inc=1, device_id=dev, device_id_type=MESH)

    def w_rows(owner, share, start, count):
        return w_full.at[pl.ds(pl.multiple_of(owner * head_cols + share * piece + start, 16), count), :]

    def w_src(dest, share, start, count):
        return wo_hbm.at[pl.ds(pl.multiple_of(share * piece + start, 16), count),
                         pl.ds(pl.multiple_of(dest * y_cols, 128), y_cols)]

    w_parts = [("own", p, piece), ("far", across, half)]

    def relay_buf(buf, kind):
        return buf.at[pl.ds(0, half)] if kind == "own" else buf.at[pl.ds(half, half // 2)]

    def w_to_relay(kind, share, count):
        n = count // 2
        send(w_src(far, share, 0, n), relay_buf(relay_up, kind), ("w_relay_up", kind), at_tp(up))
        send(w_src(far, share, n, n), relay_buf(relay_dn, kind), ("w_relay_dn", kind), at_tp(dn))

    def w_direct(kind, share, count):
        send(w_src(up, share, 0, count), w_rows(t, share, 0, count), ("w_from_dn", kind), at_tp(up))
        send(w_src(dn, share, 0, count), w_rows(t, share, 0, count), ("w_from_up", kind), at_tp(dn))

    def w_relay(kind, share, count):
        n = count // 2
        arrived(relay_buf(relay_up, kind), ("w_relay_up", kind))
        send(relay_buf(relay_up, kind), w_rows(dn, share, 0, n), ("w_far0", kind), at_tp(up))
        arrived(relay_buf(relay_dn, kind), ("w_relay_dn", kind))
        send(relay_buf(relay_dn, kind), w_rows(up, share, n, n), ("w_far1", kind), at_tp(dn))

    def w_over_tp(kind, share, count):
        n = count // 2
        arrived(w_rows(dn, share, 0, count), ("w_from_dn", kind))
        arrived(w_rows(up, share, 0, count), ("w_from_up", kind))
        arrived(w_rows(far, share, 0, n), ("w_far0", kind))
        arrived(w_rows(far, share, n, n), ("w_far1", kind))

    def send_all(refs, name, dev):
        for i, ref in enumerate(refs):
            send(ref, ref, (name, i), dev)

    def all_arrived(refs, name):
        for i, ref in enumerate(refs):
            arrived(ref, (name, i))

    def ring_start(part, tag):
        send_all(part(p), (tag, "L"), at_cp(right))
        send_all(part(p), (tag, "R"), at_cp(left))
        send_all(part(p), (tag, "M"), at_cp(mate))

    def ring_near(part, tag):
        all_arrived(part(left), (tag, "L"))
        send_all(part(left, 0), (tag, "far0"), at_cp(right))
        send_all(part(left), (tag, "ML"), at_cp(mate))
        all_arrived(part(right), (tag, "R"))
        send_all(part(right, 1), (tag, "far1"), at_cp(left))
        send_all(part(right), (tag, "MR"), at_cp(mate))

    def ring_far(part, tag):
        all_arrived(part(across, 0), (tag, "far0"))
        all_arrived(part(across, 1), (tag, "far1"))
        send_all(part(across), (tag, "MF"), at_cp(mate))

    def mates_near(part, tag):
        all_arrived(part(mate), (tag, "M"))
        all_arrived(part(mate_left), (tag, "ML"))
        all_arrived(part(mate_right), (tag, "MR"))

    def kv_part(g):
        def part(owner, k=None):
            both = [k_all.at[owner, g], vt_all.at[owner, g]]
            return both if k is None else both[k:k + 1]
        return part

    def w_part(owner):
        def part(share, k=None):
            return [w_rows(owner, share, 0, piece) if k is None else w_rows(owner, share, half + k * half // 2, half // 2)]
        return part

    def project(w_ref, store):
        @pl.loop(0, rows // half_rows)
        def _(i):
            r = pl.ds(pl.multiple_of(i * half_rows, 16), half_rows)
            store(r, jnp.dot(x_v[r, :], w_ref[...], preferred_element_type=jnp.float32))

    def store_k(r, val):
        for g in range(groups):
            k_all[p, g, r, :] = val[:, g * HEAD_DIM:(g + 1) * HEAD_DIM].astype(jnp.bfloat16)

    def store_v(r, val):
        for g in range(groups):
            vt_all[p, g, :, r] = val[:, g * HEAD_DIM:(g + 1) * HEAD_DIM].T.astype(jnp.bfloat16)

    for i, c in enumerate(cuts):
        with jax.named_scope("wait_x"):
            for copy in load_kv[i]:
                copy.wait()
        with jax.named_scope("proj_kv"):
            @pl.loop(0, 2)
            def _(half_of):
                r = pl.ds(pl.multiple_of(half_of * half_rows, 16), half_rows)
                for kind, store in enumerate((store_k, store_v)):
                    val = jnp.dot(x_v[r, c], wkv_v[kind, c, :], preferred_element_type=jnp.float32)
                    if i > 0:
                        val += kv_acc[kind, r, :]
                    if i + 1 < len(cuts):
                        kv_acc[kind, r, :] = val
                    else:
                        store(r, val)
        if i == 0:
            pl.semaphore_wait(barrier, len(peers))

            for k in range(1, cp):
                send(seg_in, segs.at[p], ("seg", k), at_cp(lax.rem(p + k, cp)))
            load_seg = load(seg_in, segs.at[p], "seg")


            w_to_relay(*w_parts[0])
    load_q = [load(wq_hbm.at[:, pl.ds(n * COL_TILE, COL_TILE)], wq_v.at[n], ("q", n)) for n in range(q_tiles)]
    own_cols = pl.ds(pl.multiple_of(t * y_cols, 128), y_cols)
    load_o = load(wo_hbm.at[:, own_cols], w_full.at[pl.ds(pl.multiple_of(t * head_cols, 128), head_cols), :], "o")

    ring_start(kv_part(0), ("kv", 0))

    def q_tile(n):
        load_q[n].wait()

        def store(r, val):
            for k in range(COL_TILE // HEAD_DIM):
                q_v[n * (COL_TILE // HEAD_DIM) + k, r, :HEAD_DIM] = val[:, k * HEAD_DIM:(k + 1) * HEAD_DIM].astype(jnp.bfloat16)
        with jax.named_scope(f"q{n}"):
            project(wq_v.at[n], store)

    def wide(v, n):
        return jnp.concatenate([v] * (n // v.shape[1]), axis=1)

    lane = lax.broadcasted_iota(jnp.int32, (rows, HEAD_DIM), 1)
    first_doc = seg_in[:, :1]

    def set_bias():
        seg_col[...] = jnp.broadcast_to(seg_in[...], (HEAD_DIM, rows)).T

        @pl.loop(0, rows // HEAD_DIM)
        def _(i):
            r = pl.ds(pl.multiple_of(i * HEAD_DIM, HEAD_DIM), HEAD_DIM)
            allowed = wide(seg_col[r, :], rows) == seg_in[...]
            allowed &= (lax.broadcasted_iota(jnp.int32, (HEAD_DIM, rows), 0) + i * HEAD_DIM
                        <= lax.broadcasted_iota(jnp.int32, (HEAD_DIM, rows), 1))
            bias[r, :] = jnp.where(allowed, 0.0, NEG_INF)

    def set_mask(block):
        of_key = jnp.broadcast_to(segs[block], (HEAD_DIM, rows)).T
        shut = (of_key != first_doc) & (lane == 0)
        k_mask[block] = jnp.where(shut, NEG_INF, 0.0).astype(jnp.bfloat16)

    def visit(pair, blocks, diagonal=False):
        g = pair * PAIR // per_group
        units = [(block, h, i) for block in blocks for h in range(PAIR) for i in range(2)]
        scratch = [s_even, s_odd]

        def keys(i):
            return half_rows if diagonal and i == 0 else rows

        def scores(n):
            block, h, i = units[n]
            c = slice(i * half_rows, (i + 1) * half_rows)
            q = q_v[pair * PAIR + h, c, :]
            k = k_all[block, g, :keys(i), :]
            if diagonal:
                s = lax.dot_general(k, q[:, :HEAD_DIM], (((1,), (1,)), ((), ())), preferred_element_type=jnp.float32)
                s += bias[:keys(i), c]
            else:
                k = jnp.concatenate([k, k_mask[block]], axis=1)
                s = lax.dot_general(k, q, (((1,), (1,)), ((), ())), preferred_element_type=jnp.float32)
            scratch[n % 2][:keys(i), :] = s
            return jnp.max(s, axis=0, keepdims=True)

        def absorb(n, top):
            block, h, i = units[n]
            c = slice(i * half_rows, (i + 1) * half_rows)
            if diagonal:
                new_max = shift = top
            else:
                in_first = seg_in[:, c] == first_doc
                old_max = m_s[h, :, c]
                new_max = jnp.where(in_first, jnp.maximum(old_max, top), old_max)
                shift = jnp.where(in_first, new_max, -NEG_INF)
            prob = jnp.exp2(scratch[n % 2][:keys(i), :] * SCALE - shift * SCALE)
            total = jnp.sum(prob, axis=0, keepdims=True)
            out = jnp.dot(vt_all[block, g, :, :keys(i)], prob.astype(jnp.bfloat16), preferred_element_type=jnp.float32)
            if not diagonal:
                rescale = jnp.exp2((old_max - new_max) * SCALE)
                total += l_s[h, :, c] * rescale
                out += acc_s[h, :, c] * rescale
            m_s[h, :, c] = new_max
            l_s[h, :, c] = total
            acc_s[h, :, c] = out

        top = scores(0)
        for n in range(len(units)):
            ahead = scores(n + 1) if n + 1 < len(units) else None
            absorb(n, top)
            top = ahead

    def visit_mate(pair):
        @pl.when(core == 1)
        def _():
            if pair == 0:
                set_mask(mate)
            visit(pair, [mate])

    def visit_chips(pair, count, chip_of):
        @pl.loop(0, count)
        def _(i):
            chip = chip_of(i)

            @pl.when(chip < col)
            def _():
                if pair == 0:
                    set_mask(chip * 2)
                    set_mask(chip * 2 + 1)
                visit(pair, [chip * 2, chip * 2 + 1])

    def visit_near(pair):
        visit_mate(pair)
        visit_chips(pair, 2, lambda i: jnp.where(i == 0, left_chip, right_chip))

    def visit_far(pair):
        visit_chips(pair, 1, lambda i: far_chip + i)

    def visit_all(pair):
        visit_mate(pair)
        visit_chips(pair, chips, lambda i: i)

    def o_cols(owner, h):
        return o_all.at[:, pl.ds(pl.multiple_of(owner * head_cols + h * HEAD_DIM, 128), HEAD_DIM)]

    def o_finish(pair):
        for k in range(PAIR):
            h = pair * PAIR + k
            o_all[:, pl.ds(pl.multiple_of(t * head_cols + h * HEAD_DIM, 128), HEAD_DIM)] = (
                acc_s[k] / l_s[k]).T.astype(jnp.bfloat16)
            send(o_cols(t, h), o_cols(t, h), ("o", h, "D"), at_tp(up))
            send(o_cols(t, h), o_cols(t, h), ("o", h, "U"), at_tp(dn))

    def o_relay(h):
        arrived(o_cols(dn, h), ("o", h, "D"))
        arrived(o_cols(up, h), ("o", h, "U"))
        if h % 2 == 0:
            send(o_cols(dn, h), o_cols(dn, h), ("o", h, "F"), at_tp(up))
        else:
            send(o_cols(up, h), o_cols(up, h), ("o", h, "F"), at_tp(dn))

    kv = [(kv_part(g), ("kv", g)) for g in range(groups)]
    w = [(w_part(lax.rem(t + j, tp)), ("w", j)) for j in range(1, tp)]

    q_v[:, :, HEAD_DIM:] = jnp.where(lax.broadcasted_iota(jnp.int32, (heads, rows, HEAD_DIM), 2) == 0, 1.0, 0.0).astype(jnp.bfloat16)
    scope = jax.named_scope

    def o_relay_pair(pair):
        with scope(f"o_relay{pair}"):
            for k in range(PAIR):
                o_relay(pair * PAIR + k)

    w_direct(*w_parts[0])
    q_tile(0)
    with scope("diag0"):
        set_bias()
        visit(0, [p], diagonal=True)
    with scope("w_relay_own"):
        w_relay(*w_parts[0])
        w_to_relay(*w_parts[1])
    q_tile(1)
    q_tile(2)
    with scope("kv0_near"):
        ring_near(*kv[0])
    with scope("kv0_mate"):
        load_seg.wait()
        for k in range(1, cp):
            arrived(segs.at[lax.rem(p + cp - k, cp)], ("seg", k))
        mates_near(*kv[0])
    with scope("near0"):
        visit_near(0)
    with scope("w_relay_far"):
        w_relay(*w_parts[1])
        w_direct(*w_parts[1])
    with scope("kv0_far"):
        ring_far(*kv[0])
        ring_start(*kv[1])
    with scope("w_tp_own"):
        w_over_tp(*w_parts[0])
        ring_start(*w[0])
    q_tile(3)
    with scope("kv0_mf"):
        all_arrived(kv[0][0](mate_across), (kv[0][1], "MF"))
    with scope("far0"):
        visit_far(0)
    with scope("o_fin0"):
        o_finish(0)
    with scope("pair1"):
        visit(1, [p], diagonal=True)
        visit_all(1)
        o_finish(1)
    with scope("kv1_near"):
        ring_near(*kv[1])
    ring_start(*w[1])
    o_relay_pair(0)
    with scope("diag2"):
        visit(2, [p], diagonal=True)
    with scope("kv1_mate"):
        mates_near(*kv[1])
    with scope("near2"):
        visit_near(2)
    with scope("kv1_far"):
        ring_far(*kv[1])
        all_arrived(kv[1][0](mate_across), (kv[1][1], "MF"))
    with scope("far2"):
        visit_far(2)
        o_finish(2)
    with scope("w1_near"):
        ring_near(*w[0])
    ring_start(*w[2])
    o_relay_pair(1)
    with scope("pair3"):
        visit(3, [p], diagonal=True)
        visit_all(3)
        o_finish(3)
    with scope("w2_near"):
        ring_near(*w[1])
    o_relay_pair(2)
    with scope("w3_near"):
        ring_near(*w[2])
    o_relay_pair(3)
    with scope("w_far"):
        w_over_tp(*w_parts[1])
        for part in w:
            ring_far(*part)
    with scope("w_mate"):
        for part, tag in w:
            mates_near(part, tag)
            all_arrived(part(mate_across), (tag, "MF"))
    with scope("o_far"):
        for h in range(heads):
            arrived(o_cols(far, h), ("o", h, "F"))
        load_o.wait()

    def y_at(owner, n, k=None):
        cols = pl.ds(pl.multiple_of(owner * y_cols + n * COL_TILE, 128), COL_TILE)
        return y_ref.at[:, cols] if k is None else y_ref.at[pl.ds(k * half_rows, half_rows), cols]

    tiles = y_cols // COL_TILE
    for n in range(tiles):
        @pl.loop(0, 2)
        def _(i):
            with scope("y_mm"):
                r = pl.ds(pl.multiple_of(i * half_rows, 16), half_rows)
                y_ref[r, pl.ds(pl.multiple_of(t * y_cols + n * COL_TILE, 128), COL_TILE)] = jnp.dot(
                    o_all[r, :], w_full[:, n * COL_TILE:(n + 1) * COL_TILE], preferred_element_type=jnp.float32).astype(jnp.bfloat16)
        send(y_at(t, n), y_at(t, n), ("y", n, "D"), at_tp(up))
        send(y_at(t, n), y_at(t, n), ("y", n, "U"), at_tp(dn))
    for n in range(tiles):
        with scope(f"y_relay{n}"):
            arrived(y_at(dn, n), ("y", n, "D"))
            send(y_at(dn, n, 0), y_at(dn, n, 0), ("y", n, "F0"), at_tp(up))
            arrived(y_at(up, n), ("y", n, "U"))
            send(y_at(up, n, 1), y_at(up, n, 1), ("y", n, "F1"), at_tp(dn))
    for n in range(tiles):
        with scope(f"y_far{n}"):
            arrived(y_at(far, n, 0), ("y", n, "F0"))
            arrived(y_at(far, n, 1), ("y", n, "F1"))
    with scope("drain"):
        for c in waiting:
            c.wait_send()


def solution(mesh):
    tp, cp = mesh.shape["tp"], mesh.shape["cp"]

    def local_attention(x_loc, seg_loc, w_query, w_key, w_value, w_out):
        rows, width = x_loc.shape
        heads = w_query.shape[1] // HEAD_DIM
        groups = w_key.shape[1] // HEAD_DIM
        head_cols = heads * HEAD_DIM
        y_cols = width // tp
        bf16, f32 = jnp.bfloat16, jnp.float32
        hbm = pl.BlockSpec(memory_space=pl.ANY)
        return pl.pallas_call(
            functools.partial(kernel, tp, cp),
            out_shape=pltpu.VMEM((rows, width), bf16),
            in_specs=[hbm, pl.BlockSpec(memory_space=pltpu.VMEM), hbm, hbm, hbm, hbm],
            out_specs=pl.BlockSpec(memory_space=pltpu.VMEM),
            scratch_shapes=[
                pltpu.VMEM((rows, width), bf16),
                pltpu.VMEM((2, width, groups * HEAD_DIM), bf16),
                pltpu.VMEM((head_cols // COL_TILE, width, COL_TILE), bf16),
                pltpu.VMEM((tp * head_cols, y_cols), bf16),
                pltpu.VMEM((cp, groups, rows, HEAD_DIM), bf16),
                pltpu.VMEM((cp, groups, HEAD_DIM, rows), bf16),
                pltpu.VMEM((cp, 1, rows), jnp.int32),
                pltpu.VMEM((rows, HEAD_DIM), jnp.int32),
                pltpu.VMEM((rows, rows), f32),
                pltpu.VMEM((cp, rows, HEAD_DIM), bf16),
                pltpu.VMEM((rows, rows // 2), f32),
                pltpu.VMEM((rows, rows // 2), f32),
                pltpu.VMEM((2, rows, groups * HEAD_DIM), f32),
                pltpu.VMEM((heads, rows, 2 * HEAD_DIM), bf16),
                pltpu.VMEM((rows, tp * head_cols), bf16),
                pltpu.VMEM((head_cols // cp * 3 // 4, y_cols), bf16),
                pltpu.VMEM((head_cols // cp * 3 // 4, y_cols), bf16),
                pltpu.VMEM((PAIR, 1, rows), f32),
                pltpu.VMEM((PAIR, 1, rows), f32),
                pltpu.VMEM((PAIR, HEAD_DIM, rows), f32),
                pltpu.SemaphoreType.DMA((32,)),
                pltpu.SemaphoreType.DMA((224,)),
                pltpu.SemaphoreType.DMA((224,)),
            ],
            compiler_params=pltpu.CompilerParams(collective_id=0, has_side_effects=True, vmem_limit_bytes=56 * 2**20),
        )(x_loc, seg_loc.reshape(1, rows), w_query, w_key, w_value, w_out)

    return jax.shard_map(local_attention, mesh=mesh, in_specs=(P(('dp', 'cp'), None), P(('dp', 'cp')), P(None, 'tp'), P(None, 'tp'), P(None, 'tp'), P('tp', None)), out_specs=P(('dp', 'cp'), None), check_vma=False)
```

```python
import functools

import jax
import jax.numpy as jnp
from jax import lax
from jax.experimental import pallas as pl
from jax.experimental.pallas import tpu as pltpu
from jax.sharding import PartitionSpec as P


HEAD_DIM = 128
COL_TILE = 256
DEPTH_CUTS = 4
PAIR = 2
MESH = pl.DeviceIdType.MESH
SCALE = HEAD_DIM**-0.5 * 1.4426950408889634
NEG_INF = float("-inf")


class Sems:
    def __init__(self, ref):
        self.ref, self.names = ref, {}

    def __getitem__(self, name):
        return self.ref.at[self.names.setdefault(name, len(self.names))]


def kernel(tp, cp, x_hbm, seg_in, wq_hbm, wk_hbm, wv_hbm, wo_hbm, y_ref,
           x_v, wkv_v, wq_v, w_full, k_all, vt_all, segs, seg_col, bias, k_mask, s_even, s_odd, kv_acc, q_v, o_all, y_own, relay_up, relay_dn,
           m_s, l_s, acc_s, load_sem, send_sem, recv_sem):
    t, p = lax.axis_index("tp"), lax.axis_index("cp")
    chips = cp // 2
    col, core = p // 2, lax.rem(p, 2)
    up, dn, far = lax.rem(t + 1, tp), lax.rem(t + tp - 1, tp), lax.rem(t + 2, tp)
    right_chip, left_chip, far_chip = lax.rem(col + 1, chips), lax.rem(col + chips - 1, chips), lax.rem(col + 2, chips)
    right, left, across = right_chip * 2 + core, left_chip * 2 + core, far_chip * 2 + core
    mate = col * 2 + 1 - core
    mate_right, mate_left, mate_across = right_chip * 2 + 1 - core, left_chip * 2 + 1 - core, far_chip * 2 + 1 - core

    rows = x_v.shape[0]
    heads = q_v.shape[0]
    groups = k_all.shape[1]
    per_group = heads // groups
    head_cols = heads * HEAD_DIM
    y_cols = w_full.shape[1]
    piece = head_cols // cp
    half = piece // 2
    half_rows = rows // 2

    loads, sends, recvs = Sems(load_sem), Sems(send_sem), Sems(recv_sem)
    waiting = []

    def at_tp(i):
        return {"tp": i, "cp": p}

    def at_cp(i):
        return {"tp": t, "cp": i}

    def send(src, dst, name, dev):
        c = pltpu.make_async_remote_copy(src_ref=src, dst_ref=dst, send_sem=sends[(name, len(waiting))],
                                         recv_sem=recvs[name], device_id=dev, device_id_type=MESH)
        c.start()
        waiting.append(c)

    def arrived(dst, name):
        pltpu.make_async_remote_copy(src_ref=dst, dst_ref=dst, send_sem=sends[0], recv_sem=recvs[name],
                                     device_id=at_cp(p), device_id_type=MESH).wait_recv()

    def load(src, dst, name):
        c = pltpu.make_async_copy(src, dst, loads[name])
        c.start()
        return c

    depth = x_v.shape[1] // DEPTH_CUTS
    cuts = [pl.ds(i * depth, depth) for i in range(DEPTH_CUTS)]
    load_kv = [(load(x_hbm.at[:, c], x_v.at[:, c], ("x", i)), load(wk_hbm.at[c, :], wkv_v.at[0, c, :], ("k", i)),
                load(wv_hbm.at[c, :], wkv_v.at[1, c, :], ("v", i))) for i, c in enumerate(cuts)]
    q_tiles = head_cols // COL_TILE

    barrier = pltpu.get_barrier_semaphore()
    peers = [at_tp(up), at_tp(dn)] + [at_cp(lax.rem(p + k, cp)) for k in range(1, cp)]
    for dev in peers:
        pl.semaphore_signal(barrier, inc=1, device_id=dev, device_id_type=MESH)

    def w_rows(owner, share, start, count):
        return w_full.at[pl.ds(pl.multiple_of(owner * head_cols + share * piece + start, 16), count), :]

    def w_src(dest, share, start, count):
        return wo_hbm.at[pl.ds(pl.multiple_of(share * piece + start, 16), count),
                         pl.ds(pl.multiple_of(dest * y_cols, 128), y_cols)]

    w_parts = [("own", p, piece), ("far", across, half)]

    def relay_buf(buf, kind):
        return buf.at[pl.ds(0, half)] if kind == "own" else buf.at[pl.ds(half, half // 2)]

    def w_to_relay(kind, share, count):
        n = count // 2
        send(w_src(far, share, 0, n), relay_buf(relay_up, kind), ("w_relay_up", kind), at_tp(up))
        send(w_src(far, share, n, n), relay_buf(relay_dn, kind), ("w_relay_dn", kind), at_tp(dn))

    def w_direct(kind, share, count):
        send(w_src(up, share, 0, count), w_rows(t, share, 0, count), ("w_from_dn", kind), at_tp(up))
        send(w_src(dn, share, 0, count), w_rows(t, share, 0, count), ("w_from_up", kind), at_tp(dn))

    def w_relay(kind, share, count):
        n = count // 2
        arrived(relay_buf(relay_up, kind), ("w_relay_up", kind))
        send(relay_buf(relay_up, kind), w_rows(dn, share, 0, n), ("w_far0", kind), at_tp(up))
        arrived(relay_buf(relay_dn, kind), ("w_relay_dn", kind))
        send(relay_buf(relay_dn, kind), w_rows(up, share, n, n), ("w_far1", kind), at_tp(dn))

    def w_over_tp(kind, share, count):
        n = count // 2
        arrived(w_rows(dn, share, 0, count), ("w_from_dn", kind))
        arrived(w_rows(up, share, 0, count), ("w_from_up", kind))
        arrived(w_rows(far, share, 0, n), ("w_far0", kind))
        arrived(w_rows(far, share, n, n), ("w_far1", kind))

    def send_all(refs, name, dev):
        for i, ref in enumerate(refs):
            send(ref, ref, (name, i), dev)

    def all_arrived(refs, name):
        for i, ref in enumerate(refs):
            arrived(ref, (name, i))

    def ring_start(part, tag):
        send_all(part(p), (tag, "L"), at_cp(right))
        send_all(part(p), (tag, "R"), at_cp(left))
        send_all(part(p), (tag, "M"), at_cp(mate))

    def ring_near(part, tag):
        all_arrived(part(left), (tag, "L"))
        send_all(part(left, 0), (tag, "far0"), at_cp(right))
        send_all(part(left), (tag, "ML"), at_cp(mate))
        all_arrived(part(right), (tag, "R"))
        send_all(part(right, 1), (tag, "far1"), at_cp(left))
        send_all(part(right), (tag, "MR"), at_cp(mate))

    def ring_far(part, tag):
        all_arrived(part(across, 0), (tag, "far0"))
        all_arrived(part(across, 1), (tag, "far1"))
        send_all(part(across), (tag, "MF"), at_cp(mate))

    def mates_near(part, tag):
        all_arrived(part(mate), (tag, "M"))
        all_arrived(part(mate_left), (tag, "ML"))
        all_arrived(part(mate_right), (tag, "MR"))

    def kv_part(g):
        def part(owner, k=None):
            both = [k_all.at[owner, g], vt_all.at[owner, g]]
            return both if k is None else both[k:k + 1]
        return part

    def w_part(owner):
        def part(share, k=None):
            return [w_rows(owner, share, 0, piece) if k is None else w_rows(owner, share, half + k * half // 2, half // 2)]
        return part

    def project(w_ref, store):
        @pl.loop(0, rows // half_rows)
        def _(i):
            r = pl.ds(pl.multiple_of(i * half_rows, 16), half_rows)
            store(r, jnp.dot(x_v[r, :], w_ref[...], preferred_element_type=jnp.float32))

    def store_k(r, val):
        for g in range(groups):
            k_all[p, g, r, :] = val[:, g * HEAD_DIM:(g + 1) * HEAD_DIM].astype(jnp.bfloat16)

    def store_v(r, val):
        for g in range(groups):
            vt_all[p, g, :, r] = val[:, g * HEAD_DIM:(g + 1) * HEAD_DIM].T.astype(jnp.bfloat16)

    for i, c in enumerate(cuts):
        with jax.named_scope("wait_x"):
            for copy in load_kv[i]:
                copy.wait()
        with jax.named_scope("proj_kv"):
            @pl.loop(0, 2)
            def _(half_of):
                r = pl.ds(pl.multiple_of(half_of * half_rows, 16), half_rows)
                for kind, store in enumerate((store_k, store_v)):
                    val = jnp.dot(x_v[r, c], wkv_v[kind, c, :], preferred_element_type=jnp.float32)
                    if i > 0:
                        val += kv_acc[kind, r, :]
                    if i + 1 < len(cuts):
                        kv_acc[kind, r, :] = val
                    else:
                        store(r, val)
        if i + 2 == len(cuts):
            pl.semaphore_wait(barrier, len(peers))

            for k in range(1, cp):
                send(seg_in, segs.at[p], ("seg", k), at_cp(lax.rem(p + k, cp)))
            load_seg = load(seg_in, segs.at[p], "seg")


            for part in w_parts:
                w_to_relay(*part)
    load_q = [load(wq_hbm.at[:, pl.ds(n * COL_TILE, COL_TILE)], wq_v.at[n], ("q", n)) for n in range(q_tiles)]
    own_cols = pl.ds(pl.multiple_of(t * y_cols, 128), y_cols)
    load_o = load(wo_hbm.at[:, own_cols], w_full.at[pl.ds(pl.multiple_of(t * head_cols, 128), head_cols), :], "o")

    ring_start(kv_part(0), ("kv", 0))

    def q_tile(n):
        load_q[n].wait()

        def store(r, val):
            for k in range(COL_TILE // HEAD_DIM):
                q_v[n * (COL_TILE // HEAD_DIM) + k, r, :HEAD_DIM] = val[:, k * HEAD_DIM:(k + 1) * HEAD_DIM].astype(jnp.bfloat16)
        with jax.named_scope(f"q{n}"):
            project(wq_v.at[n], store)

    def wide(v, n):
        return jnp.concatenate([v] * (n // v.shape[1]), axis=1)

    lane = lax.broadcasted_iota(jnp.int32, (rows, HEAD_DIM), 1)
    first_doc = seg_in[:, :1]

    def set_bias():
        seg_col[...] = jnp.broadcast_to(seg_in[...], (HEAD_DIM, rows)).T

        @pl.loop(0, rows // HEAD_DIM)
        def _(i):
            r = pl.ds(pl.multiple_of(i * HEAD_DIM, HEAD_DIM), HEAD_DIM)
            allowed = wide(seg_col[r, :], rows) == seg_in[...]
            allowed &= (lax.broadcasted_iota(jnp.int32, (HEAD_DIM, rows), 0) + i * HEAD_DIM
                        <= lax.broadcasted_iota(jnp.int32, (HEAD_DIM, rows), 1))
            bias[r, :] = jnp.where(allowed, 0.0, NEG_INF)

    def set_mask(block):
        of_key = jnp.broadcast_to(segs[block], (HEAD_DIM, rows)).T
        shut = (of_key != first_doc) & (lane == 0)
        k_mask[block] = jnp.where(shut, NEG_INF, 0.0).astype(jnp.bfloat16)

    def visit(pair, blocks, diagonal=False):
        g = pair * PAIR // per_group
        units = [(block, h, i) for block in blocks for h in range(PAIR) for i in range(2)]
        scratch = [s_even, s_odd]

        def keys(i):
            return half_rows if diagonal and i == 0 else rows

        def scores(n):
            block, h, i = units[n]
            c = slice(i * half_rows, (i + 1) * half_rows)
            q = q_v[pair * PAIR + h, c, :]
            k = k_all[block, g, :keys(i), :]
            if diagonal:
                s = lax.dot_general(k, q[:, :HEAD_DIM], (((1,), (1,)), ((), ())), preferred_element_type=jnp.float32)
                s += bias[:keys(i), c]
            else:
                k = jnp.concatenate([k, k_mask[block]], axis=1)
                s = lax.dot_general(k, q, (((1,), (1,)), ((), ())), preferred_element_type=jnp.float32)
            scratch[n % 2][:keys(i), :] = s
            return jnp.max(s, axis=0, keepdims=True)

        def absorb(n, top):
            block, h, i = units[n]
            c = slice(i * half_rows, (i + 1) * half_rows)
            if diagonal:
                new_max = shift = top
            else:
                in_first = seg_in[:, c] == first_doc
                old_max = m_s[h, :, c]
                new_max = jnp.where(in_first, jnp.maximum(old_max, top), old_max)
                shift = jnp.where(in_first, new_max, -NEG_INF)
            prob = jnp.exp2(scratch[n % 2][:keys(i), :] * SCALE - shift * SCALE)
            total = jnp.sum(prob, axis=0, keepdims=True)
            out = jnp.dot(vt_all[block, g, :, :keys(i)], prob.astype(jnp.bfloat16), preferred_element_type=jnp.float32)
            if not diagonal:
                rescale = jnp.exp2((old_max - new_max) * SCALE)
                total += l_s[h, :, c] * rescale
                out += acc_s[h, :, c] * rescale
            m_s[h, :, c] = new_max
            l_s[h, :, c] = total
            acc_s[h, :, c] = out

        top = scores(0)
        for n in range(len(units)):
            ahead = scores(n + 1) if n + 1 < len(units) else None
            absorb(n, top)
            top = ahead

    def visit_mate(pair):
        @pl.when(core == 1)
        def _():
            if pair == 0:
                set_mask(mate)
            visit(pair, [mate])

    def visit_chips(pair, count, chip_of):
        @pl.loop(0, count)
        def _(i):
            chip = chip_of(i)

            @pl.when(chip < col)
            def _():
                if pair == 0:
                    set_mask(chip * 2)
                    set_mask(chip * 2 + 1)
                visit(pair, [chip * 2, chip * 2 + 1])

    def visit_near(pair):
        visit_mate(pair)
        visit_chips(pair, 2, lambda i: jnp.where(i == 0, left_chip, right_chip))

    def visit_far(pair):
        visit_chips(pair, 1, lambda i: far_chip + i)

    def visit_all(pair):
        visit_mate(pair)
        visit_chips(pair, chips, lambda i: i)

    def o_cols(owner, h):
        return o_all.at[:, pl.ds(pl.multiple_of(owner * head_cols + h * HEAD_DIM, 128), HEAD_DIM)]

    def o_finish(pair):
        for k in range(PAIR):
            h = pair * PAIR + k
            o_all[:, pl.ds(pl.multiple_of(t * head_cols + h * HEAD_DIM, 128), HEAD_DIM)] = (
                acc_s[k] / l_s[k]).T.astype(jnp.bfloat16)
            send(o_cols(t, h), o_cols(t, h), ("o", h, "D"), at_tp(up))
            send(o_cols(t, h), o_cols(t, h), ("o", h, "U"), at_tp(dn))

    def o_relay(h):
        arrived(o_cols(dn, h), ("o", h, "D"))
        arrived(o_cols(up, h), ("o", h, "U"))
        if h % 2 == 0:
            send(o_cols(dn, h), o_cols(dn, h), ("o", h, "F"), at_tp(up))
        else:
            send(o_cols(up, h), o_cols(up, h), ("o", h, "F"), at_tp(dn))

    kv = [(kv_part(g), ("kv", g)) for g in range(groups)]
    w = [(w_part(lax.rem(t + j, tp)), ("w", j)) for j in range(1, tp)]

    q_v[:, :, HEAD_DIM:] = jnp.where(lax.broadcasted_iota(jnp.int32, (heads, rows, HEAD_DIM), 2) == 0, 1.0, 0.0).astype(jnp.bfloat16)
    scope = jax.named_scope

    def o_relay_pair(pair):
        with scope(f"o_relay{pair}"):
            for k in range(PAIR):
                o_relay(pair * PAIR + k)

    q_tile(0)
    w_direct(*w_parts[0])
    with scope("diag0"):
        set_bias()
        visit(0, [p], diagonal=True)
    with scope("w_relay"):
        for part in w_parts:
            w_relay(*part)
        w_direct(*w_parts[1])
    q_tile(1)
    q_tile(2)
    with scope("kv0_near"):
        ring_near(*kv[0])
    with scope("kv0_mate"):
        load_seg.wait()
        for k in range(1, cp):
            arrived(segs.at[lax.rem(p + cp - k, cp)], ("seg", k))
        mates_near(*kv[0])
        ring_start(*kv[1])
    with scope("near0"):
        visit_near(0)
    with scope("kv0_far"):
        ring_far(*kv[0])
    with scope("w_tp_own"):
        w_over_tp(*w_parts[0])
        ring_start(*w[0])
    q_tile(3)
    with scope("kv0_mf"):
        all_arrived(kv[0][0](mate_across), (kv[0][1], "MF"))
    with scope("far0"):
        visit_far(0)
    with scope("o_fin0"):
        o_finish(0)
    with scope("kv1_near"):
        ring_near(*kv[1])
        ring_start(*w[1])
    with scope("pair1"):
        visit(1, [p], diagonal=True)
        visit_all(1)
        o_finish(1)
    o_relay_pair(0)
    with scope("diag2"):
        visit(2, [p], diagonal=True)
    with scope("kv1_mate"):
        mates_near(*kv[1])
    with scope("near2"):
        visit_near(2)
    with scope("kv1_far"):
        ring_far(*kv[1])
        all_arrived(kv[1][0](mate_across), (kv[1][1], "MF"))
    with scope("far2"):
        visit_far(2)
        o_finish(2)
    with scope("w1_near"):
        ring_near(*w[0])
    ring_start(*w[2])
    o_relay_pair(1)
    with scope("pair3"):
        visit(3, [p], diagonal=True)
        visit_all(3)
        o_finish(3)
    with scope("w2_near"):
        ring_near(*w[1])
    o_relay_pair(2)
    with scope("w3_near"):
        ring_near(*w[2])
    o_relay_pair(3)
    with scope("w_far"):
        w_over_tp(*w_parts[1])
        for part in w:
            ring_far(*part)
    with scope("w_mate"):
        for part, tag in w:
            mates_near(part, tag)
            all_arrived(part(mate_across), (tag, "MF"))
    with scope("o_far"):
        for h in range(heads):
            arrived(o_cols(far, h), ("o", h, "F"))
        load_o.wait()

    def y_at(owner, n, k):
        return y_ref.at[pl.ds(k * half_rows, half_rows),
                        pl.ds(pl.multiple_of(owner * y_cols + n * COL_TILE, 128), COL_TILE)]

    tiles = [(n, k) for n in range(y_cols // COL_TILE) for k in range(2)]
    copies = []
    for n, k in tiles:
        r, c = slice(k * half_rows, (k + 1) * half_rows), slice(n * COL_TILE, (n + 1) * COL_TILE)
        with scope("y_mm"):
            y_own[r, c] = jnp.dot(o_all[r, :], w_full[:, c], preferred_element_type=jnp.float32).astype(jnp.bfloat16)
        send(y_own.at[r, c], y_at(t, n, k), ("y", n, k, "D"), at_tp(up))
        send(y_own.at[r, c], y_at(t, n, k), ("y", n, k, "U"), at_tp(dn))
        copies.append(load(y_own.at[r, c], y_at(t, n, k), ("y", n, k)))
    for n, k in tiles:
        with scope(f"y_relay{n}"):
            arrived(y_at(dn, n, k), ("y", n, k, "D"))
            if k == 0:
                send(y_at(dn, n, k), y_at(dn, n, k), ("y", n, k, "F"), at_tp(up))
            arrived(y_at(up, n, k), ("y", n, k, "U"))
            if k == 1:
                send(y_at(up, n, k), y_at(up, n, k), ("y", n, k, "F"), at_tp(dn))
    for n, k in tiles:
        with scope(f"y_far{n}"):
            arrived(y_at(far, n, k), ("y", n, k, "F"))
    for c in copies:
        c.wait()
    with scope("drain"):
        for c in waiting:
            c.wait_send()


def solution(mesh):
    tp, cp = mesh.shape["tp"], mesh.shape["cp"]

    def local_attention(x_loc, seg_loc, w_query, w_key, w_value, w_out):
        rows, width = x_loc.shape
        heads = w_query.shape[1] // HEAD_DIM
        groups = w_key.shape[1] // HEAD_DIM
        head_cols = heads * HEAD_DIM
        y_cols = width // tp
        bf16, f32 = jnp.bfloat16, jnp.float32
        hbm = pl.BlockSpec(memory_space=pl.ANY)
        return pl.pallas_call(
            functools.partial(kernel, tp, cp),
            out_shape=pltpu.VMEM((rows, width), bf16),
            in_specs=[hbm, pl.BlockSpec(memory_space=pltpu.VMEM), hbm, hbm, hbm, hbm],
            out_specs=hbm,
            scratch_shapes=[
                pltpu.VMEM((rows, width), bf16),
                pltpu.VMEM((2, width, groups * HEAD_DIM), bf16),
                pltpu.VMEM((head_cols // COL_TILE, width, COL_TILE), bf16),
                pltpu.VMEM((tp * head_cols, y_cols), bf16),
                pltpu.VMEM((cp, groups, rows, HEAD_DIM), bf16),
                pltpu.VMEM((cp, groups, HEAD_DIM, rows), bf16),
                pltpu.VMEM((cp, 1, rows), jnp.int32),
                pltpu.VMEM((rows, HEAD_DIM), jnp.int32),
                pltpu.VMEM((rows, rows), f32),
                pltpu.VMEM((cp, rows, HEAD_DIM), bf16),
                pltpu.VMEM((rows, rows // 2), f32),
                pltpu.VMEM((rows, rows // 2), f32),
                pltpu.VMEM((2, rows, groups * HEAD_DIM), f32),
                pltpu.VMEM((heads, rows, 2 * HEAD_DIM), bf16),
                pltpu.VMEM((rows, tp * head_cols), bf16),
                pltpu.VMEM((rows, y_cols), bf16),
                pltpu.VMEM((head_cols // cp * 3 // 4, y_cols), bf16),
                pltpu.VMEM((head_cols // cp * 3 // 4, y_cols), bf16),
                pltpu.VMEM((PAIR, 1, rows), f32),
                pltpu.VMEM((PAIR, 1, rows), f32),
                pltpu.VMEM((PAIR, HEAD_DIM, rows), f32),
                pltpu.SemaphoreType.DMA((48,)),
                pltpu.SemaphoreType.DMA((240,)),
                pltpu.SemaphoreType.DMA((240,)),
            ],
            compiler_params=pltpu.CompilerParams(collective_id=0, has_side_effects=True, vmem_limit_bytes=56 * 2**20),
        )(x_loc, seg_loc.reshape(1, rows), w_query, w_key, w_value, w_out)

    return jax.shard_map(local_attention, mesh=mesh, in_specs=(P(('dp', 'cp'), None), P(('dp', 'cp')), P(None, 'tp'), P(None, 'tp'), P(None, 'tp'), P('tp', None)), out_specs=P(('dp', 'cp'), None), check_vma=False)
```

```python
import functools

import jax
import jax.numpy as jnp
from jax import lax
from jax.experimental import pallas as pl
from jax.experimental.pallas import tpu as pltpu
from jax.sharding import PartitionSpec as P


HEAD_DIM = 128
COL_TILE = 256
DEPTH_CUTS = 4
PAIR = 2
MESH = pl.DeviceIdType.MESH
SCALE = HEAD_DIM**-0.5 * 1.4426950408889634
NEG_INF = float("-inf")


class Sems:
    def __init__(self, ref):
        self.ref, self.names = ref, {}

    def __getitem__(self, name):
        return self.ref.at[self.names.setdefault(name, len(self.names))]


def kernel(tp, cp, x_hbm, seg_in, wq_hbm, wk_hbm, wv_hbm, wo_hbm, y_ref,
           x_v, wkv_v, wq_v, w_full, k_all, vt_all, segs, seg_col, bias, k_mask, s_even, s_odd, kv_acc, q_v, o_all, y_own, relay_up, relay_dn,
           m_s, l_s, acc_s, load_sem, send_sem, recv_sem):
    t, p = lax.axis_index("tp"), lax.axis_index("cp")
    chips = cp // 2
    col, core = p // 2, lax.rem(p, 2)
    up, dn, far = lax.rem(t + 1, tp), lax.rem(t + tp - 1, tp), lax.rem(t + 2, tp)
    right_chip, left_chip, far_chip = lax.rem(col + 1, chips), lax.rem(col + chips - 1, chips), lax.rem(col + 2, chips)
    right, left, across = right_chip * 2 + core, left_chip * 2 + core, far_chip * 2 + core
    mate = col * 2 + 1 - core
    mate_right, mate_left, mate_across = right_chip * 2 + 1 - core, left_chip * 2 + 1 - core, far_chip * 2 + 1 - core

    rows = x_v.shape[0]
    heads = q_v.shape[0]
    groups = k_all.shape[1]
    per_group = heads // groups
    head_cols = heads * HEAD_DIM
    y_cols = w_full.shape[1]
    piece = head_cols // cp
    half = piece // 2
    half_rows = rows // 2

    loads, sends, recvs = Sems(load_sem), Sems(send_sem), Sems(recv_sem)

    def at_tp(i):
        return {"tp": i, "cp": p}

    def at_cp(i):
        return {"tp": t, "cp": i}

    def send(src, dst, name, dev, kind):
        pltpu.make_async_remote_copy(src_ref=src, dst_ref=dst, send_sem=sends[kind], recv_sem=recvs[name],
                                     device_id=dev, device_id_type=MESH).start()

    def waiter(ref, kind, name):
        return pltpu.make_async_remote_copy(src_ref=ref, dst_ref=ref, send_sem=sends[kind], recv_sem=recvs[name],
                                            device_id=at_cp(p), device_id_type=MESH)

    def arrived(ref, name):
        waiter(ref, "kv", name).wait_recv()

    def sent(ref, kind):
        waiter(ref, kind, "seg").wait_send()

    def heads_of(n):
        return o_all.at[:, :n * HEAD_DIM]

    def rows_of(n):
        return w_full.at[:n]

    def load(src, dst, name):
        c = pltpu.make_async_copy(src, dst, loads[name])
        c.start()
        return c

    depth = x_v.shape[1] // DEPTH_CUTS
    cuts = [pl.ds(i * depth, depth) for i in range(DEPTH_CUTS)]
    load_kv = [(load(x_hbm.at[:, c], x_v.at[:, c], ("x", i)), load(wk_hbm.at[c, :], wkv_v.at[0, c, :], ("k", i)),
                load(wv_hbm.at[c, :], wkv_v.at[1, c, :], ("v", i))) for i, c in enumerate(cuts)]
    q_tiles = head_cols // COL_TILE

    barrier = pltpu.get_barrier_semaphore()
    peers = [at_tp(up), at_tp(dn)] + [at_cp(lax.rem(p + k, cp)) for k in range(1, cp)]
    for dev in peers:
        pl.semaphore_signal(barrier, inc=1, device_id=dev, device_id_type=MESH)

    def w_rows(owner, share, start, count):
        return w_full.at[pl.ds(pl.multiple_of(owner * head_cols + share * piece + start, 16), count), :]

    def w_src(dest, share, start, count):
        return wo_hbm.at[pl.ds(pl.multiple_of(share * piece + start, 16), count),
                         pl.ds(pl.multiple_of(dest * y_cols, 128), y_cols)]

    def w_to_relay():
        send(w_src(far, p, 0, half), relay_up, "w_relay", at_tp(up), "w")
        send(w_src(far, p, half, half), relay_dn, "w_relay", at_tp(dn), "w")

    def w_direct(share, count, name):
        send(w_src(up, share, 0, count), w_rows(t, share, 0, count), name, at_tp(up), "w")
        send(w_src(dn, share, 0, count), w_rows(t, share, 0, count), name, at_tp(dn), "w")

    def w_relay():
        arrived(rows_of(2 * half), "w_relay")
        send(relay_up, w_rows(dn, p, 0, half), "w_own", at_tp(up), "w")
        send(relay_dn, w_rows(up, p, half, half), "w_own", at_tp(dn), "w")

    class Ring:
        def __init__(self, tag, kind, parts, wait_of, shared=None):
            self.tag, self.kind, self.parts, self.wait_of = tag, kind, parts, wait_of
            self.shared = shared or tag

        def pass_on(self, owner, k, name, dev):
            for ref in self.parts(owner, k):
                send(ref, ref, name, dev, self.kind)

        def start(self):
            self.pass_on(p, None, (self.tag, "L"), at_cp(right))
            self.pass_on(p, None, (self.tag, "R"), at_cp(left))
            self.pass_on(p, None, (self.shared, "M"), at_cp(mate))

        def near(self):
            arrived(self.wait_of(1), (self.tag, "L"))
            self.pass_on(left, 0, (self.shared, "F"), at_cp(right))
            self.pass_on(left, None, (self.shared, "M"), at_cp(mate))
            arrived(self.wait_of(1), (self.tag, "R"))
            self.pass_on(right, 1, (self.shared, "F"), at_cp(left))
            self.pass_on(right, None, (self.shared, "M"), at_cp(mate))

        def far(self, name):
            self.pass_on(across, None, (self.shared, name), at_cp(mate))

    def kv_ring(g):
        def parts(owner, k):
            both = [k_all.at[owner, g], vt_all.at[owner, g]]
            return both if k is None else both[k:k + 1]
        return Ring(("kv", g), "kv", parts, lambda n: heads_of(2 * n))

    def w_ring(j):
        owner = lax.rem(t + j, tp)
        first = 0 if j == 2 else half

        def parts(share, k):
            if k is None:
                return [w_rows(owner, share, 0, piece)]
            count = (piece - first) // 2
            return [w_rows(owner, share, first + k * count, count)]
        return Ring(("w", j), "w", parts, lambda n: rows_of(piece * n), "w")

    def project(w_ref, store):
        @pl.loop(0, rows // half_rows)
        def _(i):
            r = pl.ds(pl.multiple_of(i * half_rows, 16), half_rows)
            store(r, jnp.dot(x_v[r, :], w_ref[...], preferred_element_type=jnp.float32))

    def store_k(r, val):
        for g in range(groups):
            k_all[p, g, r, :] = val[:, g * HEAD_DIM:(g + 1) * HEAD_DIM].astype(jnp.bfloat16)

    def store_v(r, val):
        for g in range(groups):
            vt_all[p, g, :, r] = val[:, g * HEAD_DIM:(g + 1) * HEAD_DIM].T.astype(jnp.bfloat16)

    for i, c in enumerate(cuts):
        with jax.named_scope("wait_x"):
            for copy in load_kv[i]:
                copy.wait()
        with jax.named_scope("proj_kv"):
            @pl.loop(0, 2)
            def _(half_of):
                r = pl.ds(pl.multiple_of(half_of * half_rows, 16), half_rows)
                for kind, store in enumerate((store_k, store_v)):
                    val = jnp.dot(x_v[r, c], wkv_v[kind, c, :], preferred_element_type=jnp.float32)
                    if i > 0:
                        val += kv_acc[kind, r, :]
                    if i + 1 < len(cuts):
                        kv_acc[kind, r, :] = val
                    else:
                        store(r, val)
        if i == 1:
            load_q = [load(wq_hbm.at[:, pl.ds(n * COL_TILE, COL_TILE)], wq_v.at[n], ("q", n)) for n in range(q_tiles)]
        if i + 2 == len(cuts):
            pl.semaphore_wait(barrier, len(peers))

            for k in range(1, cp):
                send(seg_in, segs.at[p], "seg", at_cp(lax.rem(p + k, cp)), "seg")
            load_seg = load(seg_in, segs.at[p], "seg")


            w_to_relay()
    kv = [kv_ring(g) for g in range(groups)]
    w = [w_ring(j) for j in range(1, tp)]
    kv[0].start()
    own_cols = pl.ds(pl.multiple_of(t * y_cols, 128), y_cols)
    load_o = load(wo_hbm.at[:, own_cols], w_full.at[pl.ds(pl.multiple_of(t * head_cols, 128), head_cols), :], "o")

    def q_tile(n):
        load_q[n].wait()

        def store(r, val):
            for k in range(COL_TILE // HEAD_DIM):
                q_v[n * (COL_TILE // HEAD_DIM) + k, r, :HEAD_DIM] = val[:, k * HEAD_DIM:(k + 1) * HEAD_DIM].astype(jnp.bfloat16)
        with jax.named_scope(f"q{n}"):
            project(wq_v.at[n], store)

    def wide(v, n):
        return jnp.concatenate([v] * (n // v.shape[1]), axis=1)

    lane = lax.broadcasted_iota(jnp.int32, (rows, HEAD_DIM), 1)
    first_doc = seg_in[:, :1]

    def set_bias():
        seg_col[...] = jnp.broadcast_to(seg_in[...], (HEAD_DIM, rows)).T

        @pl.loop(0, rows // HEAD_DIM)
        def _(i):
            r = pl.ds(pl.multiple_of(i * HEAD_DIM, HEAD_DIM), HEAD_DIM)
            allowed = wide(seg_col[r, :], rows) == seg_in[...]
            allowed &= (lax.broadcasted_iota(jnp.int32, (HEAD_DIM, rows), 0) + i * HEAD_DIM
                        <= lax.broadcasted_iota(jnp.int32, (HEAD_DIM, rows), 1))
            bias[r, :] = jnp.where(allowed, 0.0, NEG_INF)

    def set_mask(block):
        of_key = jnp.broadcast_to(segs[block], (HEAD_DIM, rows)).T
        shut = (of_key != first_doc) & (lane == 0)
        k_mask[block] = jnp.where(shut, NEG_INF, 0.0).astype(jnp.bfloat16)

    def visit(pair, blocks, diagonal=False):
        g = pair * PAIR // per_group
        units = [(block, h, i) for block in blocks for h in range(PAIR) for i in range(2)]
        scratch = [s_even, s_odd]

        def keys(i):
            return half_rows if diagonal and i == 0 else rows

        def scores(n):
            block, h, i = units[n]
            c = slice(i * half_rows, (i + 1) * half_rows)
            q = q_v[pair * PAIR + h, c, :]
            k = k_all[block, g, :keys(i), :]
            if diagonal:
                s = lax.dot_general(k, q[:, :HEAD_DIM], (((1,), (1,)), ((), ())), preferred_element_type=jnp.float32)
                s += bias[:keys(i), c]
            else:
                k = jnp.concatenate([k, k_mask[block]], axis=1)
                s = lax.dot_general(k, q, (((1,), (1,)), ((), ())), preferred_element_type=jnp.float32)
            scratch[n % 2][:keys(i), :] = s
            return jnp.max(s, axis=0, keepdims=True)

        def absorb(n, top):
            block, h, i = units[n]
            c = slice(i * half_rows, (i + 1) * half_rows)
            if diagonal:
                new_max = shift = top
            else:
                in_first = seg_in[:, c] == first_doc
                old_max = m_s[h, :, c]
                new_max = jnp.where(in_first, jnp.maximum(old_max, top), old_max)
                shift = jnp.where(in_first, new_max, -NEG_INF)
            prob = jnp.exp2(scratch[n % 2][:keys(i), :] * SCALE - shift * SCALE)
            total = jnp.sum(prob, axis=0, keepdims=True)
            out = jnp.dot(vt_all[block, g, :, :keys(i)], prob.astype(jnp.bfloat16), preferred_element_type=jnp.float32)
            if not diagonal:
                rescale = jnp.exp2((old_max - new_max) * SCALE)
                total += l_s[h, :, c] * rescale
                out += acc_s[h, :, c] * rescale
            m_s[h, :, c] = new_max
            l_s[h, :, c] = total
            acc_s[h, :, c] = out

        top = scores(0)
        for n in range(len(units)):
            ahead = scores(n + 1) if n + 1 < len(units) else None
            absorb(n, top)
            top = ahead

    def visit_mate(pair):
        @pl.when(core == 1)
        def _():
            if pair == 0:
                set_mask(mate)
            visit(pair, [mate])

    def visit_chips(pair, count, chip_of):
        @pl.loop(0, count)
        def _(i):
            chip = chip_of(i)

            @pl.when(chip < col)
            def _():
                if pair == 0:
                    set_mask(chip * 2)
                    set_mask(chip * 2 + 1)
                visit(pair, [chip * 2, chip * 2 + 1])

    def visit_near(pair):
        visit_mate(pair)
        visit_chips(pair, 2, lambda i: jnp.where(i == 0, left_chip, right_chip))

    def visit_far(pair):
        visit_chips(pair, 1, lambda i: far_chip + i)

    def visit_all(pair):
        visit_mate(pair)
        visit_chips(pair, chips, lambda i: i)

    def o_cols(owner, h):
        return o_all.at[:, pl.ds(pl.multiple_of(owner * head_cols + h * HEAD_DIM, 128), HEAD_DIM)]

    def o_finish(pair):
        for k in range(PAIR):
            h = pair * PAIR + k
            o_all[:, pl.ds(pl.multiple_of(t * head_cols + h * HEAD_DIM, 128), HEAD_DIM)] = (
                acc_s[k] / l_s[k]).T.astype(jnp.bfloat16)
            send(o_cols(t, h), o_cols(t, h), ("o", pair), at_tp(up), "o")
            send(o_cols(t, h), o_cols(t, h), ("o", pair), at_tp(dn), "o")

    q_v[:, :, HEAD_DIM:] = jnp.where(lax.broadcasted_iota(jnp.int32, (heads, rows, HEAD_DIM), 2) == 0, 1.0, 0.0).astype(jnp.bfloat16)
    scope = jax.named_scope

    def o_relay_pair(pair):
        with scope(f"o_relay{pair}"):
            arrived(heads_of(2 * PAIR), ("o", pair))
            for h in range(pair * PAIR, (pair + 1) * PAIR):
                if h % 2 == 0:
                    send(o_cols(dn, h), o_cols(dn, h), "o_far", at_tp(up), "o")
                else:
                    send(o_cols(up, h), o_cols(up, h), "o_far", at_tp(dn), "o")

    q_tile(0)
    w_direct(p, piece, "w_own")
    with scope("diag0"):
        set_bias()
        visit(0, [p], diagonal=True)
    with scope("w_relay"):
        w_relay()
        w_direct(across, half, "w_extra")
    q_tile(1)
    q_tile(2)
    with scope("kv0_near"):
        kv[0].near()
    with scope("kv0_mate"):
        load_seg.wait()
        arrived(segs.at[:cp - 1], "seg")
        arrived(heads_of(6), (kv[0].tag, "M"))
        kv[1].start()
    with scope("near0"):
        visit_near(0)
    with scope("kv0_far"):
        arrived(heads_of(2), (kv[0].tag, "F"))
        kv[0].far("MF")
    with scope("w_tp_own"):
        arrived(rows_of(3 * piece), "w_own")
        w[0].start()
    q_tile(3)
    with scope("kv0_mf"):
        arrived(heads_of(2), (kv[0].tag, "MF"))
    with scope("far0"):
        visit_far(0)
    with scope("o_fin0"):
        o_finish(0)
    with scope("kv1_near"):
        kv[1].near()
    with scope("pair1"):
        visit(1, [p], diagonal=True)
        visit_all(1)
        o_finish(1)
    with scope("kv1_far"):
        arrived(heads_of(2), (kv[1].tag, "F"))
        kv[1].far("MF")
        w[1].start()
        w[2].start()
    o_relay_pair(0)
    with scope("diag2"):
        visit(2, [p], diagonal=True)
    with scope("kv1_mate"):
        arrived(heads_of(6), (kv[1].tag, "M"))
        arrived(heads_of(2), (kv[1].tag, "MF"))
    with scope("pair2"):
        visit_all(2)
        o_finish(2)
    with scope("w1_near"):
        w[0].near()
    o_relay_pair(1)
    with scope("pair3"):
        visit(3, [p], diagonal=True)
        visit_all(3)
        o_finish(3)
    with scope("w2_near"):
        w[1].near()
    o_relay_pair(2)
    with scope("w3_near"):
        w[2].near()
    o_relay_pair(3)
    with scope("w_far"):
        arrived(rows_of(2 * half), "w_extra")
        arrived(rows_of(2 * half + piece), ("w", "F"))
        for part in w:
            part.far("M")
    with scope("w_mate"):
        arrived(rows_of(12 * piece), ("w", "M"))
    with scope("o_far"):
        arrived(heads_of(heads), "o_far")
        load_o.wait()

    def y_at(owner, n, k):
        return y_ref.at[pl.ds(k * half_rows, half_rows),
                        pl.ds(pl.multiple_of(owner * y_cols + n * COL_TILE, 128), COL_TILE)]

    tiles = [(n, k) for n in range(y_cols // COL_TILE) for k in range(2)]
    copies = []
    for n, k in tiles:
        r, c = slice(k * half_rows, (k + 1) * half_rows), slice(n * COL_TILE, (n + 1) * COL_TILE)
        with scope("y_mm"):
            y_own[r, c] = jnp.dot(o_all[r, :], w_full[:, c], preferred_element_type=jnp.float32).astype(jnp.bfloat16)
        send(y_own.at[r, c], y_at(t, n, k), ("y", n, k) if k == 0 else "y_rest", at_tp(up), "y")
        send(y_own.at[r, c], y_at(t, n, k), ("y", n, k) if k == 1 else "y_rest", at_tp(dn), "y")
        copies.append(load(y_own.at[r, c], y_at(t, n, k), "y"))
    for n, k in tiles:
        with scope(f"y_relay{n}"):
            arrived(y_at(dn, n, k), ("y", n, k))
            if k == 0:
                send(y_at(dn, n, k), y_at(dn, n, k), "y_far", at_tp(up), "y")
            else:
                send(y_at(up, n, k), y_at(up, n, k), "y_far", at_tp(dn), "y")
    with scope("y_rest"):
        arrived(y_own, "y_rest")
    with scope("y_far"):
        arrived(y_own, "y_far")
    with scope("drain"):
        pltpu.make_async_copy(y_own, y_own, loads["y"]).wait()
        sent(segs.at[:cp - 1], "seg")
        sent(heads_of(14 * groups), "kv")
        sent(rows_of(5 * piece + (tp - 1) * 6 * piece + 2 * half + piece), "w")
        sent(heads_of(3 * heads), "o")
        sent(y_ref.at[:, :3 * y_cols], "y")


def solution(mesh):
    tp, cp = mesh.shape["tp"], mesh.shape["cp"]

    def local_attention(x_loc, seg_loc, w_query, w_key, w_value, w_out):
        rows, width = x_loc.shape
        heads = w_query.shape[1] // HEAD_DIM
        groups = w_key.shape[1] // HEAD_DIM
        head_cols = heads * HEAD_DIM
        y_cols = width // tp
        bf16, f32 = jnp.bfloat16, jnp.float32
        hbm = pl.BlockSpec(memory_space=pl.ANY)
        return pl.pallas_call(
            functools.partial(kernel, tp, cp),
            out_shape=pltpu.VMEM((rows, width), bf16),
            in_specs=[hbm, pl.BlockSpec(memory_space=pltpu.VMEM), hbm, hbm, hbm, hbm],
            out_specs=hbm,
            scratch_shapes=[
                pltpu.VMEM((rows, width), bf16),
                pltpu.VMEM((2, width, groups * HEAD_DIM), bf16),
                pltpu.VMEM((head_cols // COL_TILE, width, COL_TILE), bf16),
                pltpu.VMEM((tp * head_cols, y_cols), bf16),
                pltpu.VMEM((cp, groups, rows, HEAD_DIM), bf16),
                pltpu.VMEM((cp, groups, HEAD_DIM, rows), bf16),
                pltpu.VMEM((cp, 1, rows), jnp.int32),
                pltpu.VMEM((rows, HEAD_DIM), jnp.int32),
                pltpu.VMEM((rows, rows), f32),
                pltpu.VMEM((cp, rows, HEAD_DIM), bf16),
                pltpu.VMEM((rows, rows // 2), f32),
                pltpu.VMEM((rows, rows // 2), f32),
                pltpu.VMEM((2, rows, groups * HEAD_DIM), f32),
                pltpu.VMEM((heads, rows, 2 * HEAD_DIM), bf16),
                pltpu.VMEM((rows, tp * head_cols), bf16),
                pltpu.VMEM((rows, y_cols), bf16),
                pltpu.VMEM((head_cols // cp // 2, y_cols), bf16),
                pltpu.VMEM((head_cols // cp // 2, y_cols), bf16),
                pltpu.VMEM((PAIR, 1, rows), f32),
                pltpu.VMEM((PAIR, 1, rows), f32),
                pltpu.VMEM((PAIR, HEAD_DIM, rows), f32),
                pltpu.SemaphoreType.DMA((19,)),
                pltpu.SemaphoreType.DMA((5,)),
                pltpu.SemaphoreType.DMA((40,)),
            ],
            compiler_params=pltpu.CompilerParams(collective_id=0, has_side_effects=True, vmem_limit_bytes=56 * 2**20),
        )(x_loc, seg_loc.reshape(1, rows), w_query, w_key, w_value, w_out)

    return jax.shard_map(local_attention, mesh=mesh, in_specs=(P(('dp', 'cp'), None), P(('dp', 'cp')), P(None, 'tp'), P(None, 'tp'), P(None, 'tp'), P('tp', None)), out_specs=P(('dp', 'cp'), None), check_vma=False)
```

```python
import functools

import jax
import jax.numpy as jnp
from jax import lax
from jax.experimental import pallas as pl
from jax.experimental.pallas import tpu as pltpu
from jax.sharding import PartitionSpec as P


HEAD_DIM = 128
COL_TILE = 256
DEPTH_CUTS = 4
PAIR = 2
MESH = pl.DeviceIdType.MESH
SCALE = HEAD_DIM**-0.5 * 1.4426950408889634
NEG_INF = float("-inf")


class Sems:
    def __init__(self, ref):
        self.ref, self.names = ref, {}

    def __getitem__(self, name):
        return self.ref.at[self.names.setdefault(name, len(self.names))]


def kernel(tp, cp, x_hbm, seg_in, wq_hbm, wk_hbm, wv_hbm, wo_hbm, y_ref,
           x_v, wkv_v, wq_v, w_full, k_all, vt_all, segs, seg_col, bias, k_mask, s_even, s_odd, kv_acc, q_v, o_all, y_own, relay_up, relay_dn,
           m_s, l_s, acc_s, load_sem, send_sem, recv_sem):
    t, p = lax.axis_index("tp"), lax.axis_index("cp")
    chips = cp // 2
    col, core = p // 2, lax.rem(p, 2)
    up, dn, far = lax.rem(t + 1, tp), lax.rem(t + tp - 1, tp), lax.rem(t + 2, tp)
    right_chip, left_chip, far_chip = lax.rem(col + 1, chips), lax.rem(col + chips - 1, chips), lax.rem(col + 2, chips)
    right, left, across = right_chip * 2 + core, left_chip * 2 + core, far_chip * 2 + core
    mate = col * 2 + 1 - core
    mate_right, mate_left, mate_across = right_chip * 2 + 1 - core, left_chip * 2 + 1 - core, far_chip * 2 + 1 - core

    rows = x_v.shape[0]
    heads = q_v.shape[0]
    groups = k_all.shape[1]
    per_group = heads // groups
    head_cols = heads * HEAD_DIM
    y_cols = w_full.shape[1]
    piece = head_cols // cp
    half = piece // 2
    half_rows = rows // 2

    loads, sends, recvs = Sems(load_sem), Sems(send_sem), Sems(recv_sem)

    def at_tp(i):
        return {"tp": i, "cp": p}

    def at_cp(i):
        return {"tp": t, "cp": i}

    def send(src, dst, name, dev, kind):
        pltpu.make_async_remote_copy(src_ref=src, dst_ref=dst, send_sem=sends[kind], recv_sem=recvs[name],
                                     device_id=dev, device_id_type=MESH).start()

    def waiter(ref, kind, name):
        return pltpu.make_async_remote_copy(src_ref=ref, dst_ref=ref, send_sem=sends[kind], recv_sem=recvs[name],
                                            device_id=at_cp(p), device_id_type=MESH)

    def arrived(ref, name):
        waiter(ref, "kv", name).wait_recv()

    def sent(ref, kind):
        waiter(ref, kind, "seg").wait_send()

    def heads_of(n):
        return o_all.at[:, :n * HEAD_DIM]

    def rows_of(n):
        return w_full.at[:n]

    def load(src, dst, name):
        c = pltpu.make_async_copy(src, dst, loads[name])
        c.start()
        return c

    depth = x_v.shape[1] // DEPTH_CUTS
    cuts = [pl.ds(i * depth, depth) for i in range(DEPTH_CUTS)]
    load_kv = [(load(x_hbm.at[:, c], x_v.at[:, c], ("x", i)), load(wk_hbm.at[c, :], wkv_v.at[0, c, :], ("k", i)),
                load(wv_hbm.at[c, :], wkv_v.at[1, c, :], ("v", i))) for i, c in enumerate(cuts)]
    q_tiles = head_cols // COL_TILE

    barrier = pltpu.get_barrier_semaphore()
    peers = [at_tp(up), at_tp(dn)] + [at_cp(lax.rem(p + k, cp)) for k in range(1, cp)]
    for dev in peers:
        pl.semaphore_signal(barrier, inc=1, device_id=dev, device_id_type=MESH)

    def w_rows(owner, share, start, count):
        return w_full.at[pl.ds(pl.multiple_of(owner * head_cols + share * piece + start, 16), count), :]

    def w_src(dest, share, start, count):
        return wo_hbm.at[pl.ds(pl.multiple_of(share * piece + start, 16), count),
                         pl.ds(pl.multiple_of(dest * y_cols, 128), y_cols)]

    def w_to_relay():
        send(w_src(far, p, 0, half), relay_up, "w_relay", at_tp(up), "w")
        send(w_src(far, p, half, half), relay_dn, "w_relay", at_tp(dn), "w")

    def w_direct(share, count, name):
        send(w_src(up, share, 0, count), w_rows(t, share, 0, count), name, at_tp(up), "w")
        send(w_src(dn, share, 0, count), w_rows(t, share, 0, count), name, at_tp(dn), "w")

    def w_relay():
        arrived(rows_of(2 * half), "w_relay")
        send(relay_up, w_rows(dn, p, 0, half), "w_own", at_tp(up), "w")
        send(relay_dn, w_rows(up, p, half, half), "w_own", at_tp(dn), "w")

    class Ring:
        def __init__(self, tag, kind, parts, wait_of, shared=None):
            self.tag, self.kind, self.parts, self.wait_of = tag, kind, parts, wait_of
            self.shared = shared or tag

        def pass_on(self, owner, k, name, dev):
            for ref in self.parts(owner, k):
                send(ref, ref, name, dev, self.kind)

        def start(self):
            self.pass_on(p, None, (self.tag, "L"), at_cp(right))
            self.pass_on(p, None, (self.tag, "R"), at_cp(left))
            self.pass_on(p, None, (self.shared, "M"), at_cp(mate))

        def near(self):
            arrived(self.wait_of(1), (self.tag, "L"))
            self.pass_on(left, 0, (self.shared, "F"), at_cp(right))
            self.pass_on(left, None, (self.shared, "M"), at_cp(mate))
            arrived(self.wait_of(1), (self.tag, "R"))
            self.pass_on(right, 1, (self.shared, "F"), at_cp(left))
            self.pass_on(right, None, (self.shared, "M"), at_cp(mate))

        def far(self, name):
            self.pass_on(across, None, (self.shared, name), at_cp(mate))

    def kv_ring(g):
        def parts(owner, k):
            both = [k_all.at[owner, g], vt_all.at[owner, g]]
            return both if k is None else both[k:k + 1]
        return Ring(("kv", g), "kv", parts, lambda n: heads_of(2 * n))

    def w_ring(j):
        owner = lax.rem(t + j, tp)
        first = 0 if j == 2 else half

        def parts(share, k):
            if k is None:
                return [w_rows(owner, share, 0, piece)]
            count = (piece - first) // 2
            return [w_rows(owner, share, first + k * count, count)]
        return Ring(("w", j), "w", parts, lambda n: rows_of(piece * n), "w")

    def project(w_ref, store):
        @pl.loop(0, rows // half_rows)
        def _(i):
            r = pl.ds(pl.multiple_of(i * half_rows, 16), half_rows)
            store(r, jnp.dot(x_v[r, :], w_ref[...], preferred_element_type=jnp.float32))

    def store_k(r, val):
        for g in range(groups):
            k_all[p, g, r, :] = val[:, g * HEAD_DIM:(g + 1) * HEAD_DIM].astype(jnp.bfloat16)

    def store_v(r, val):
        for g in range(groups):
            vt_all[p, g, :, r] = val[:, g * HEAD_DIM:(g + 1) * HEAD_DIM].T.astype(jnp.bfloat16)

    for i, c in enumerate(cuts):
        with jax.named_scope("wait_x"):
            for copy in load_kv[i]:
                copy.wait()
        with jax.named_scope("proj_kv"):
            @pl.loop(0, 2)
            def _(half_of):
                r = pl.ds(pl.multiple_of(half_of * half_rows, 16), half_rows)
                for kind, store in enumerate((store_k, store_v)):
                    val = jnp.dot(x_v[r, c], wkv_v[kind, c, :], preferred_element_type=jnp.float32)
                    if i > 0:
                        val += kv_acc[kind, r, :]
                    if i + 1 < len(cuts):
                        kv_acc[kind, r, :] = val
                    else:
                        store(r, val)
        if i == 1:
            load_q = [load(wq_hbm.at[:, pl.ds(n * COL_TILE, COL_TILE)], wq_v.at[n], ("q", n)) for n in range(q_tiles)]
        if i + 2 == len(cuts):
            pl.semaphore_wait(barrier, len(peers))

            for k in range(1, cp):
                send(seg_in, segs.at[p], "seg", at_cp(lax.rem(p + k, cp)), "seg")
            load_seg = load(seg_in, segs.at[p], "seg")


            w_to_relay()
    kv = [kv_ring(g) for g in range(groups)]
    w = [w_ring(j) for j in range(1, tp)]
    kv[0].start()
    own_cols = pl.ds(pl.multiple_of(t * y_cols, 128), y_cols)
    load_o = load(wo_hbm.at[:, own_cols], w_full.at[pl.ds(pl.multiple_of(t * head_cols, 128), head_cols), :], "o")

    def q_tile(n):
        load_q[n].wait()

        def store(r, val):
            for k in range(COL_TILE // HEAD_DIM):
                q_v[n * (COL_TILE // HEAD_DIM) + k, r, :HEAD_DIM] = val[:, k * HEAD_DIM:(k + 1) * HEAD_DIM].astype(jnp.bfloat16)
        with jax.named_scope(f"q{n}"):
            project(wq_v.at[n], store)

    def wide(v, n):
        return jnp.concatenate([v] * (n // v.shape[1]), axis=1)

    lane = lax.broadcasted_iota(jnp.int32, (rows, HEAD_DIM), 1)
    first_doc = seg_in[:, :1]

    def set_bias():
        seg_col[...] = jnp.broadcast_to(seg_in[...], (HEAD_DIM, rows)).T

        @pl.loop(0, rows // HEAD_DIM)
        def _(i):
            r = pl.ds(pl.multiple_of(i * HEAD_DIM, HEAD_DIM), HEAD_DIM)
            allowed = wide(seg_col[r, :], rows) == seg_in[...]
            allowed &= (lax.broadcasted_iota(jnp.int32, (HEAD_DIM, rows), 0) + i * HEAD_DIM
                        <= lax.broadcasted_iota(jnp.int32, (HEAD_DIM, rows), 1))
            bias[r, :] = jnp.where(allowed, 0.0, NEG_INF)

    def set_mask(block):
        of_key = jnp.broadcast_to(segs[block], (HEAD_DIM, rows)).T
        shut = (of_key != first_doc) & (lane == 0)
        k_mask[block] = jnp.where(shut, NEG_INF, 0.0).astype(jnp.bfloat16)

    def visit(pair, blocks, diagonal=False):
        g = pair * PAIR // per_group
        units = [(block, h, i) for block in blocks for h in range(PAIR) for i in range(2)]
        scratch = [s_even, s_odd]

        def keys(i):
            return half_rows if diagonal and i == 0 else rows

        def scores(n):
            block, h, i = units[n]
            c = slice(i * half_rows, (i + 1) * half_rows)
            q = q_v[pair * PAIR + h, c, :]
            k = k_all[block, g, :keys(i), :]
            if diagonal:
                s = lax.dot_general(k, q[:, :HEAD_DIM], (((1,), (1,)), ((), ())), preferred_element_type=jnp.float32)
                s += bias[:keys(i), c]
            else:
                k = jnp.concatenate([k, k_mask[block]], axis=1)
                s = lax.dot_general(k, q, (((1,), (1,)), ((), ())), preferred_element_type=jnp.float32)
            scratch[n % 2][:keys(i), :] = s
            return jnp.max(s, axis=0, keepdims=True)

        def absorb(n, top):
            block, h, i = units[n]
            c = slice(i * half_rows, (i + 1) * half_rows)
            if diagonal:
                new_max = shift = top
            else:
                in_first = seg_in[:, c] == first_doc
                old_max = m_s[h, :, c]
                new_max = jnp.where(in_first, jnp.maximum(old_max, top), old_max)
                shift = jnp.where(in_first, new_max, -NEG_INF)
            prob = jnp.exp2(scratch[n % 2][:keys(i), :] * SCALE - shift * SCALE)
            total = jnp.sum(prob, axis=0, keepdims=True)
            out = jnp.dot(vt_all[block, g, :, :keys(i)], prob.astype(jnp.bfloat16), preferred_element_type=jnp.float32)
            if not diagonal:
                rescale = jnp.exp2((old_max - new_max) * SCALE)
                total += l_s[h, :, c] * rescale
                out += acc_s[h, :, c] * rescale
            m_s[h, :, c] = new_max
            l_s[h, :, c] = total
            acc_s[h, :, c] = out

        top = scores(0)
        for n in range(len(units)):
            ahead = scores(n + 1) if n + 1 < len(units) else None
            absorb(n, top)
            top = ahead

    def visit_mate(pair):
        @pl.when(core == 1)
        def _():
            if pair == 0:
                set_mask(mate)
            visit(pair, [mate])

    def visit_chips(pair, count, chip_of):
        @pl.loop(0, count)
        def _(i):
            chip = chip_of(i)

            @pl.when(chip < col)
            def _():
                if pair == 0:
                    set_mask(chip * 2)
                    set_mask(chip * 2 + 1)
                visit(pair, [chip * 2, chip * 2 + 1])

    def visit_near(pair):
        visit_mate(pair)
        visit_chips(pair, 2, lambda i: jnp.where(i == 0, left_chip, right_chip))

    def visit_far(pair):
        visit_chips(pair, 1, lambda i: far_chip + i)

    def visit_all(pair):
        visit_mate(pair)
        visit_chips(pair, chips, lambda i: i)

    def o_cols(owner, h):
        return o_all.at[:, pl.ds(pl.multiple_of(owner * head_cols + h * HEAD_DIM, 128), HEAD_DIM)]

    def o_finish(pair):
        for k in range(PAIR):
            h = pair * PAIR + k
            o_all[:, pl.ds(pl.multiple_of(t * head_cols + h * HEAD_DIM, 128), HEAD_DIM)] = (
                acc_s[k] / l_s[k]).T.astype(jnp.bfloat16)
            send(o_cols(t, h), o_cols(t, h), ("o", pair), at_tp(up), "o")
            send(o_cols(t, h), o_cols(t, h), ("o", pair), at_tp(dn), "o")

    q_v[:, :, HEAD_DIM:] = jnp.where(lax.broadcasted_iota(jnp.int32, (heads, rows, HEAD_DIM), 2) == 0, 1.0, 0.0).astype(jnp.bfloat16)
    scope = jax.named_scope

    def o_relay_pair(pair):
        with scope(f"o_relay{pair}"):
            arrived(heads_of(2 * PAIR), ("o", pair))
            for h in range(pair * PAIR, (pair + 1) * PAIR):
                if h % 2 == 0:
                    send(o_cols(dn, h), o_cols(dn, h), "o_far", at_tp(up), "o")
                else:
                    send(o_cols(up, h), o_cols(up, h), "o_far", at_tp(dn), "o")

    q_tile(0)
    w_direct(p, piece, "w_own")
    with scope("diag0"):
        set_bias()
        visit(0, [p], diagonal=True)
    q_tile(1)
    q_tile(2)
    with scope("kv0_near"):
        kv[0].near()
    with scope("w_relay"):
        w_relay()
        w_direct(across, half, "w_extra")
    with scope("kv0_mate"):
        load_seg.wait()
        arrived(segs.at[:cp - 1], "seg")
        arrived(heads_of(6), (kv[0].tag, "M"))
        kv[1].start()
    with scope("near0"):
        visit_near(0)
    with scope("kv0_far"):
        arrived(heads_of(2), (kv[0].tag, "F"))
        kv[0].far("MF")
    q_tile(3)
    with scope("kv0_mf"):
        arrived(heads_of(2), (kv[0].tag, "MF"))
    with scope("far0"):
        visit_far(0)
    with scope("o_fin0"):
        o_finish(0)
    with scope("kv1_near"):
        kv[1].near()
    with scope("diag1"):
        visit(1, [p], diagonal=True)
    with scope("w_tp_own"):
        arrived(rows_of(3 * piece), "w_own")
        w[0].start()
    with scope("pair1"):
        visit_all(1)
        o_finish(1)
    with scope("kv1_far"):
        arrived(heads_of(2), (kv[1].tag, "F"))
        kv[1].far("MF")
        w[1].start()
        w[2].start()
    o_relay_pair(0)
    with scope("diag2"):
        visit(2, [p], diagonal=True)
    with scope("kv1_mate"):
        arrived(heads_of(6), (kv[1].tag, "M"))
        arrived(heads_of(2), (kv[1].tag, "MF"))
    with scope("pair2"):
        visit_all(2)
        o_finish(2)
    with scope("w1_near"):
        w[0].near()
    o_relay_pair(1)
    with scope("pair3"):
        visit(3, [p], diagonal=True)
        visit_all(3)
        o_finish(3)
    with scope("w2_near"):
        w[1].near()
    o_relay_pair(2)
    with scope("w3_near"):
        w[2].near()
    o_relay_pair(3)
    with scope("w_far"):
        arrived(rows_of(2 * half), "w_extra")
        arrived(rows_of(2 * half + piece), ("w", "F"))
        for part in w:
            part.far("M")
    with scope("w_mate"):
        arrived(rows_of(12 * piece), ("w", "M"))
    with scope("o_far"):
        arrived(heads_of(heads), "o_far")
        load_o.wait()

    def y_at(owner, n, k):
        return y_ref.at[pl.ds(k * half_rows, half_rows),
                        pl.ds(pl.multiple_of(owner * y_cols + n * COL_TILE, 128), COL_TILE)]

    tiles = [(n, k) for n in range(y_cols // COL_TILE) for k in range(2)]
    copies = []
    for n, k in tiles:
        r, c = slice(k * half_rows, (k + 1) * half_rows), slice(n * COL_TILE, (n + 1) * COL_TILE)
        with scope("y_mm"):
            y_own[r, c] = jnp.dot(o_all[r, :], w_full[:, c], preferred_element_type=jnp.float32).astype(jnp.bfloat16)
        send(y_own.at[r, c], y_at(t, n, k), ("y", n, k) if k == 0 else "y_rest", at_tp(up), "y")
        send(y_own.at[r, c], y_at(t, n, k), ("y", n, k) if k == 1 else "y_rest", at_tp(dn), "y")
        copies.append(load(y_own.at[r, c], y_at(t, n, k), "y"))
    for n, k in tiles:
        with scope(f"y_relay{n}"):
            arrived(y_at(dn, n, k), ("y", n, k))
            if k == 0:
                send(y_at(dn, n, k), y_at(dn, n, k), "y_far", at_tp(up), "y")
            else:
                send(y_at(up, n, k), y_at(up, n, k), "y_far", at_tp(dn), "y")
    with scope("y_rest"):
        arrived(y_own, "y_rest")
    with scope("y_far"):
        arrived(y_own, "y_far")
    with scope("drain"):
        pltpu.make_async_copy(y_own, y_own, loads["y"]).wait()
        sent(segs.at[:cp - 1], "seg")
        sent(heads_of(14 * groups), "kv")
        sent(rows_of(5 * piece + (tp - 1) * 6 * piece + 2 * half + piece), "w")
        sent(heads_of(3 * heads), "o")
        sent(y_ref.at[:, :3 * y_cols], "y")


def solution(mesh):
    tp, cp = mesh.shape["tp"], mesh.shape["cp"]

    def local_attention(x_loc, seg_loc, w_query, w_key, w_value, w_out):
        rows, width = x_loc.shape
        heads = w_query.shape[1] // HEAD_DIM
        groups = w_key.shape[1] // HEAD_DIM
        head_cols = heads * HEAD_DIM
        y_cols = width // tp
        bf16, f32 = jnp.bfloat16, jnp.float32
        hbm = pl.BlockSpec(memory_space=pl.ANY)
        return pl.pallas_call(
            functools.partial(kernel, tp, cp),
            out_shape=pltpu.VMEM((rows, width), bf16),
            in_specs=[hbm, pl.BlockSpec(memory_space=pltpu.VMEM), hbm, hbm, hbm, hbm],
            out_specs=hbm,
            scratch_shapes=[
                pltpu.VMEM((rows, width), bf16),
                pltpu.VMEM((2, width, groups * HEAD_DIM), bf16),
                pltpu.VMEM((head_cols // COL_TILE, width, COL_TILE), bf16),
                pltpu.VMEM((tp * head_cols, y_cols), bf16),
                pltpu.VMEM((cp, groups, rows, HEAD_DIM), bf16),
                pltpu.VMEM((cp, groups, HEAD_DIM, rows), bf16),
                pltpu.VMEM((cp, 1, rows), jnp.int32),
                pltpu.VMEM((rows, HEAD_DIM), jnp.int32),
                pltpu.VMEM((rows, rows), f32),
                pltpu.VMEM((cp, rows, HEAD_DIM), bf16),
                pltpu.VMEM((rows, rows // 2), f32),
                pltpu.VMEM((rows, rows // 2), f32),
                pltpu.VMEM((2, rows, groups * HEAD_DIM), f32),
                pltpu.VMEM((heads, rows, 2 * HEAD_DIM), bf16),
                pltpu.VMEM((rows, tp * head_cols), bf16),
                pltpu.VMEM((rows, y_cols), bf16),
                pltpu.VMEM((head_cols // cp // 2, y_cols), bf16),
                pltpu.VMEM((head_cols // cp // 2, y_cols), bf16),
                pltpu.VMEM((PAIR, 1, rows), f32),
                pltpu.VMEM((PAIR, 1, rows), f32),
                pltpu.VMEM((PAIR, HEAD_DIM, rows), f32),
                pltpu.SemaphoreType.DMA((19,)),
                pltpu.SemaphoreType.DMA((5,)),
                pltpu.SemaphoreType.DMA((40,)),
            ],
            compiler_params=pltpu.CompilerParams(collective_id=0, has_side_effects=True, vmem_limit_bytes=56 * 2**20),
        )(x_loc, seg_loc.reshape(1, rows), w_query, w_key, w_value, w_out)

    return jax.shard_map(local_attention, mesh=mesh, in_specs=(P(('dp', 'cp'), None), P(('dp', 'cp')), P(None, 'tp'), P(None, 'tp'), P(None, 'tp'), P('tp', None)), out_specs=P(('dp', 'cp'), None), check_vma=False)
```

```python
import functools

import jax
import jax.numpy as jnp
from jax import lax
from jax.experimental import pallas as pl
from jax.experimental.pallas import tpu as pltpu
from jax.sharding import PartitionSpec as P


HEAD_DIM = 128
COL_TILE = 256
DEPTH_CUTS = 4
PAIR = 2
MESH = pl.DeviceIdType.MESH
SCALE = HEAD_DIM**-0.5 * 1.4426950408889634
NEG_INF = float("-inf")


class Sems:
    def __init__(self, ref):
        self.ref, self.names = ref, {}

    def __getitem__(self, name):
        return self.ref.at[self.names.setdefault(name, len(self.names))]


def kernel(tp, cp, x_hbm, seg_in, wq_hbm, wk_hbm, wv_hbm, wo_hbm, y_ref,
           x_v, wkv_v, wq_v, w_full, k_all, vt_all, segs, seg_col, bias, k_mask, s_even, s_odd, kv_acc, q_v, o_all, y_own, relay_up, relay_dn,
           m_s, l_s, acc_s, load_sem, send_sem, recv_sem):
    t, p = lax.axis_index("tp"), lax.axis_index("cp")
    chips = cp // 2
    col, core = p // 2, lax.rem(p, 2)
    up, dn, far = lax.rem(t + 1, tp), lax.rem(t + tp - 1, tp), lax.rem(t + 2, tp)
    right_chip, left_chip, far_chip = lax.rem(col + 1, chips), lax.rem(col + chips - 1, chips), lax.rem(col + 2, chips)
    right, left, across = right_chip * 2 + core, left_chip * 2 + core, far_chip * 2 + core
    mate = col * 2 + 1 - core
    mate_right, mate_left, mate_across = right_chip * 2 + 1 - core, left_chip * 2 + 1 - core, far_chip * 2 + 1 - core

    rows = x_v.shape[0]
    heads = q_v.shape[0]
    groups = k_all.shape[1]
    per_group = heads // groups
    head_cols = heads * HEAD_DIM
    y_cols = w_full.shape[1]
    piece = head_cols // cp
    half = piece // 2
    half_rows = rows // 2

    loads, sends, recvs = Sems(load_sem), Sems(send_sem), Sems(recv_sem)

    def at_tp(i):
        return {"tp": i, "cp": p}

    def at_cp(i):
        return {"tp": t, "cp": i}

    def send(src, dst, name, dev, kind):
        pltpu.make_async_remote_copy(src_ref=src, dst_ref=dst, send_sem=sends[kind], recv_sem=recvs[name],
                                     device_id=dev, device_id_type=MESH).start()

    def waiter(ref, kind, name):
        return pltpu.make_async_remote_copy(src_ref=ref, dst_ref=ref, send_sem=sends[kind], recv_sem=recvs[name],
                                            device_id=at_cp(p), device_id_type=MESH)

    def arrived(ref, name):
        waiter(ref, "kv", name).wait_recv()

    def sent(ref, kind):
        waiter(ref, kind, "seg").wait_send()

    def heads_of(n):
        return o_all.at[:, :n * HEAD_DIM]

    def rows_of(n):
        return w_full.at[:n]

    def load(src, dst, name):
        c = pltpu.make_async_copy(src, dst, loads[name])
        c.start()
        return c

    depth = x_v.shape[1] // DEPTH_CUTS
    cuts = [pl.ds(i * depth, depth) for i in range(DEPTH_CUTS)]
    load_kv = [(load(x_hbm.at[:, c], x_v.at[:, c], ("x", i)), load(wk_hbm.at[c, :], wkv_v.at[0, c, :], ("k", i)),
                load(wv_hbm.at[c, :], wkv_v.at[1, c, :], ("v", i))) for i, c in enumerate(cuts)]
    q_tiles = head_cols // COL_TILE

    barrier = pltpu.get_barrier_semaphore()
    peers = [at_tp(up), at_tp(dn)] + [at_cp(lax.rem(p + k, cp)) for k in range(1, cp)]
    for dev in peers:
        pl.semaphore_signal(barrier, inc=1, device_id=dev, device_id_type=MESH)

    def w_rows(owner, share, start, count):
        return w_full.at[pl.ds(pl.multiple_of(owner * head_cols + share * piece + start, 16), count), :]

    def w_src(dest, share, start, count):
        return wo_hbm.at[pl.ds(pl.multiple_of(share * piece + start, 16), count),
                         pl.ds(pl.multiple_of(dest * y_cols, 128), y_cols)]

    def w_to_relay():
        send(w_src(far, p, 0, half), relay_up, "w_relay", at_tp(up), "w")
        send(w_src(far, p, half, half), relay_dn, "w_relay", at_tp(dn), "w")

    def w_direct(share, count, name):
        send(w_src(up, share, 0, count), w_rows(t, share, 0, count), name, at_tp(up), "w")
        send(w_src(dn, share, 0, count), w_rows(t, share, 0, count), name, at_tp(dn), "w")

    def w_relay():
        arrived(rows_of(2 * half), "w_relay")
        send(relay_up, w_rows(dn, p, 0, half), "w_own", at_tp(up), "w")
        send(relay_dn, w_rows(up, p, half, half), "w_own", at_tp(dn), "w")

    class Ring:
        def __init__(self, tag, kind, parts, wait_of, shared=None):
            self.tag, self.kind, self.parts, self.wait_of = tag, kind, parts, wait_of
            self.shared = shared or tag

        def pass_on(self, owner, k, name, dev):
            for ref in self.parts(owner, k):
                send(ref, ref, name, dev, self.kind)

        def start(self):
            self.pass_on(p, None, (self.tag, "L"), at_cp(right))
            self.pass_on(p, None, (self.tag, "R"), at_cp(left))
            self.pass_on(p, None, (self.shared, "M"), at_cp(mate))

        def near(self):
            arrived(self.wait_of(1), (self.tag, "L"))
            self.pass_on(left, 0, (self.shared, "F"), at_cp(right))
            self.pass_on(left, None, (self.shared, "M"), at_cp(mate))
            arrived(self.wait_of(1), (self.tag, "R"))
            self.pass_on(right, 1, (self.shared, "F"), at_cp(left))
            self.pass_on(right, None, (self.shared, "M"), at_cp(mate))

        def far(self, name):
            self.pass_on(across, None, (self.shared, name), at_cp(mate))

    def kv_ring(g):
        def parts(owner, k):
            both = [k_all.at[owner, g], vt_all.at[owner, g]]
            return both if k is None else both[k:k + 1]
        return Ring(("kv", g), "kv", parts, lambda n: heads_of(2 * n))

    def w_ring(j):
        owner = lax.rem(t + j, tp)
        first = 0 if j == 2 else half

        def parts(share, k):
            if k is None:
                return [w_rows(owner, share, 0, piece)]
            count = (piece - first) // 2
            return [w_rows(owner, share, first + k * count, count)]
        return Ring(("w", j), "w", parts, lambda n: rows_of(piece * n), "w")

    def project(w_ref, store):
        @pl.loop(0, rows // half_rows)
        def _(i):
            r = pl.ds(pl.multiple_of(i * half_rows, 16), half_rows)
            store(r, jnp.dot(x_v[r, :], w_ref[...], preferred_element_type=jnp.float32))

    def store_k(r, val):
        for g in range(groups):
            k_all[p, g, r, :] = val[:, g * HEAD_DIM:(g + 1) * HEAD_DIM].astype(jnp.bfloat16)

    def store_v(r, val):
        for g in range(groups):
            vt_all[p, g, :, r] = val[:, g * HEAD_DIM:(g + 1) * HEAD_DIM].T.astype(jnp.bfloat16)

    for i, c in enumerate(cuts):
        with jax.named_scope("wait_x"):
            for copy in load_kv[i]:
                copy.wait()
        with jax.named_scope("proj_kv"):
            @pl.loop(0, 2)
            def _(half_of):
                r = pl.ds(pl.multiple_of(half_of * half_rows, 16), half_rows)
                for kind, store in enumerate((store_k, store_v)):
                    val = jnp.dot(x_v[r, c], wkv_v[kind, c, :], preferred_element_type=jnp.float32)
                    if i > 0:
                        val += kv_acc[kind, r, :]
                    if i + 1 < len(cuts):
                        kv_acc[kind, r, :] = val
                    else:
                        store(r, val)
        if i == 1:
            load_q = [load(wq_hbm.at[:, pl.ds(n * COL_TILE, COL_TILE)], wq_v.at[n], ("q", n)) for n in range(q_tiles)]
        if i + 2 == len(cuts):
            pl.semaphore_wait(barrier, len(peers))

            for k in range(1, cp):
                send(seg_in, segs.at[p], "seg", at_cp(lax.rem(p + k, cp)), "seg")
            load_seg = load(seg_in, segs.at[p], "seg")


            w_to_relay()
    kv = [kv_ring(g) for g in range(groups)]
    w = [w_ring(j) for j in range(1, tp)]
    kv[0].start()
    own_cols = pl.ds(pl.multiple_of(t * y_cols, 128), y_cols)
    load_o = load(wo_hbm.at[:, own_cols], w_full.at[pl.ds(pl.multiple_of(t * head_cols, 128), head_cols), :], "o")

    def q_tile(n):
        load_q[n].wait()

        def store(r, val):
            for k in range(COL_TILE // HEAD_DIM):
                q_v[n * (COL_TILE // HEAD_DIM) + k, r, :HEAD_DIM] = val[:, k * HEAD_DIM:(k + 1) * HEAD_DIM].astype(jnp.bfloat16)
        with jax.named_scope(f"q{n}"):
            project(wq_v.at[n], store)

    def wide(v, n):
        return jnp.concatenate([v] * (n // v.shape[1]), axis=1)

    lane = lax.broadcasted_iota(jnp.int32, (rows, HEAD_DIM), 1)
    first_doc = seg_in[:, :1]

    def set_bias():
        seg_col[...] = jnp.broadcast_to(seg_in[...], (HEAD_DIM, rows)).T

        @pl.loop(0, rows // HEAD_DIM)
        def _(i):
            r = pl.ds(pl.multiple_of(i * HEAD_DIM, HEAD_DIM), HEAD_DIM)
            allowed = wide(seg_col[r, :], rows) == seg_in[...]
            allowed &= (lax.broadcasted_iota(jnp.int32, (HEAD_DIM, rows), 0) + i * HEAD_DIM
                        <= lax.broadcasted_iota(jnp.int32, (HEAD_DIM, rows), 1))
            bias[r, :] = jnp.where(allowed, 0.0, NEG_INF)

    def set_mask(block):
        of_key = jnp.broadcast_to(segs[block], (HEAD_DIM, rows)).T
        shut = (of_key != first_doc) & (lane == 0)
        k_mask[block] = jnp.where(shut, NEG_INF, 0.0).astype(jnp.bfloat16)

    def visit(pair, blocks, diagonal=False):
        g = pair * PAIR // per_group
        units = [(block, h, i) for block in blocks for h in range(PAIR) for i in range(2)]
        scratch = [s_even, s_odd]

        def keys(i):
            return half_rows if diagonal and i == 0 else rows

        def scores(n):
            block, h, i = units[n]
            c = slice(i * half_rows, (i + 1) * half_rows)
            q = q_v[pair * PAIR + h, c, :]
            k = k_all[block, g, :keys(i), :]
            if diagonal:
                s = lax.dot_general(k, q[:, :HEAD_DIM], (((1,), (1,)), ((), ())), preferred_element_type=jnp.float32)
                s += bias[:keys(i), c]
            else:
                k = jnp.concatenate([k, k_mask[block]], axis=1)
                s = lax.dot_general(k, q, (((1,), (1,)), ((), ())), preferred_element_type=jnp.float32)
            scratch[n % 2][:keys(i), :] = s
            return jnp.max(s, axis=0, keepdims=True)

        def absorb(n, top):
            block, h, i = units[n]
            c = slice(i * half_rows, (i + 1) * half_rows)
            if diagonal:
                new_max = shift = top
            else:
                in_first = seg_in[:, c] == first_doc
                old_max = m_s[h, :, c]
                new_max = jnp.where(in_first, jnp.maximum(old_max, top), old_max)
                shift = jnp.where(in_first, new_max, -NEG_INF)
            prob = jnp.exp2(scratch[n % 2][:keys(i), :] * SCALE - shift * SCALE)
            total = jnp.sum(prob, axis=0, keepdims=True)
            out = jnp.dot(vt_all[block, g, :, :keys(i)], prob.astype(jnp.bfloat16), preferred_element_type=jnp.float32)
            if not diagonal:
                rescale = jnp.exp2((old_max - new_max) * SCALE)
                total += l_s[h, :, c] * rescale
                out += acc_s[h, :, c] * rescale
            m_s[h, :, c] = new_max
            l_s[h, :, c] = total
            acc_s[h, :, c] = out

        top = scores(0)
        for n in range(len(units)):
            ahead = scores(n + 1) if n + 1 < len(units) else None
            absorb(n, top)
            top = ahead

    def visit_mate(pair):
        @pl.when(core == 1)
        def _():
            if pair == 0:
                set_mask(mate)
            visit(pair, [mate])

    def visit_chips(pair, count, chip_of):
        @pl.loop(0, count)
        def _(i):
            chip = chip_of(i)

            @pl.when(chip < col)
            def _():
                if pair == 0:
                    set_mask(chip * 2)
                    set_mask(chip * 2 + 1)
                visit(pair, [chip * 2, chip * 2 + 1])

    def visit_near(pair):
        visit_mate(pair)
        visit_chips(pair, 2, lambda i: jnp.where(i == 0, left_chip, right_chip))

    def visit_far(pair):
        visit_chips(pair, 1, lambda i: far_chip + i)

    def visit_all(pair):
        visit_mate(pair)
        visit_chips(pair, chips, lambda i: i)

    def o_cols(owner, h):
        return o_all.at[:, pl.ds(pl.multiple_of(owner * head_cols + h * HEAD_DIM, 128), HEAD_DIM)]

    def o_finish(pair):
        for k in range(PAIR):
            h = pair * PAIR + k
            o_all[:, pl.ds(pl.multiple_of(t * head_cols + h * HEAD_DIM, 128), HEAD_DIM)] = (
                acc_s[k] / l_s[k]).T.astype(jnp.bfloat16)
            send(o_cols(t, h), o_cols(t, h), ("o", pair), at_tp(up), "o")
            send(o_cols(t, h), o_cols(t, h), ("o", pair), at_tp(dn), "o")

    q_v[:, :, HEAD_DIM:] = jnp.where(lax.broadcasted_iota(jnp.int32, (heads, rows, HEAD_DIM), 2) == 0, 1.0, 0.0).astype(jnp.bfloat16)
    scope = jax.named_scope

    def o_relay_pair(pair):
        with scope(f"o_relay{pair}"):
            arrived(heads_of(2 * PAIR), ("o", pair))
            for h in range(pair * PAIR, (pair + 1) * PAIR):
                if h % 2 == 0:
                    send(o_cols(dn, h), o_cols(dn, h), "o_far", at_tp(up), "o")
                else:
                    send(o_cols(up, h), o_cols(up, h), "o_far", at_tp(dn), "o")

    q_tile(0)
    w_direct(p, piece, "w_own")
    with scope("diag0"):
        set_bias()
        visit(0, [p], diagonal=True)
    q_tile(1)
    q_tile(2)
    with scope("kv0_near"):
        kv[0].near()
    with scope("w_relay"):
        w_relay()
        w_direct(across, half, "w_extra")
    with scope("kv0_mate"):
        load_seg.wait()
        arrived(segs.at[:cp - 1], "seg")
        arrived(heads_of(6), (kv[0].tag, "M"))
        kv[1].start()
    with scope("near0"):
        visit_near(0)
    with scope("kv0_far"):
        arrived(heads_of(2), (kv[0].tag, "F"))
        kv[0].far("MF")
    q_tile(3)
    with scope("kv0_mf"):
        arrived(heads_of(2), (kv[0].tag, "MF"))
    with scope("far0"):
        visit_far(0)
    with scope("o_fin0"):
        o_finish(0)
    with scope("diag1"):
        visit(1, [p], diagonal=True)
    with scope("kv1_near"):
        kv[1].near()
    with scope("w_tp_own"):
        arrived(rows_of(3 * piece), "w_own")
        w[0].start()
    with scope("pair1"):
        visit_all(1)
        o_finish(1)
    with scope("kv1_far"):
        arrived(heads_of(2), (kv[1].tag, "F"))
        kv[1].far("MF")
        w[1].start()
        w[2].start()
    with scope("diag2"):
        visit(2, [p], diagonal=True)
    with scope("kv1_mate"):
        arrived(heads_of(6), (kv[1].tag, "M"))
        arrived(heads_of(2), (kv[1].tag, "MF"))
    with scope("pair2"):
        visit_all(2)
        o_finish(2)
    o_relay_pair(0)
    with scope("w1_near"):
        w[0].near()
    with scope("pair3"):
        visit(3, [p], diagonal=True)
        visit_all(3)
        o_finish(3)
    o_relay_pair(1)
    with scope("w2_near"):
        w[1].near()
    o_relay_pair(2)
    with scope("w3_near"):
        w[2].near()
    o_relay_pair(3)
    with scope("w_far"):
        arrived(rows_of(2 * half), "w_extra")
        arrived(rows_of(2 * half + piece), ("w", "F"))
        for part in w:
            part.far("M")
    with scope("w_mate"):
        arrived(rows_of(12 * piece), ("w", "M"))
    with scope("o_far"):
        arrived(heads_of(heads), "o_far")
        load_o.wait()

    def y_at(owner, n, k):
        return y_ref.at[pl.ds(k * half_rows, half_rows),
                        pl.ds(pl.multiple_of(owner * y_cols + n * COL_TILE, 128), COL_TILE)]

    tiles = [(n, k) for n in range(y_cols // COL_TILE) for k in range(2)]
    copies = []
    for n, k in tiles:
        r, c = slice(k * half_rows, (k + 1) * half_rows), slice(n * COL_TILE, (n + 1) * COL_TILE)
        with scope("y_mm"):
            y_own[r, c] = jnp.dot(o_all[r, :], w_full[:, c], preferred_element_type=jnp.float32).astype(jnp.bfloat16)
        send(y_own.at[r, c], y_at(t, n, k), ("y", n, k) if k == 0 else "y_rest", at_tp(up), "y")
        send(y_own.at[r, c], y_at(t, n, k), ("y", n, k) if k == 1 else "y_rest", at_tp(dn), "y")
        copies.append(load(y_own.at[r, c], y_at(t, n, k), "y"))
    for n, k in tiles:
        with scope(f"y_relay{n}"):
            arrived(y_at(dn, n, k), ("y", n, k))
            if k == 0:
                send(y_at(dn, n, k), y_at(dn, n, k), "y_far", at_tp(up), "y")
            else:
                send(y_at(up, n, k), y_at(up, n, k), "y_far", at_tp(dn), "y")
    with scope("y_rest"):
        arrived(y_own, "y_rest")
    with scope("y_far"):
        arrived(y_own, "y_far")
    with scope("drain"):
        pltpu.make_async_copy(y_own, y_own, loads["y"]).wait()
        sent(segs.at[:cp - 1], "seg")
        sent(heads_of(14 * groups), "kv")
        sent(rows_of(5 * piece + (tp - 1) * 6 * piece + 2 * half + piece), "w")
        sent(heads_of(3 * heads), "o")
        sent(y_ref.at[:, :3 * y_cols], "y")


def solution(mesh):
    tp, cp = mesh.shape["tp"], mesh.shape["cp"]

    def local_attention(x_loc, seg_loc, w_query, w_key, w_value, w_out):
        rows, width = x_loc.shape
        heads = w_query.shape[1] // HEAD_DIM
        groups = w_key.shape[1] // HEAD_DIM
        head_cols = heads * HEAD_DIM
        y_cols = width // tp
        bf16, f32 = jnp.bfloat16, jnp.float32
        hbm = pl.BlockSpec(memory_space=pl.ANY)
        return pl.pallas_call(
            functools.partial(kernel, tp, cp),
            out_shape=pltpu.VMEM((rows, width), bf16),
            in_specs=[hbm, pl.BlockSpec(memory_space=pltpu.VMEM), hbm, hbm, hbm, hbm],
            out_specs=hbm,
            scratch_shapes=[
                pltpu.VMEM((rows, width), bf16),
                pltpu.VMEM((2, width, groups * HEAD_DIM), bf16),
                pltpu.VMEM((head_cols // COL_TILE, width, COL_TILE), bf16),
                pltpu.VMEM((tp * head_cols, y_cols), bf16),
                pltpu.VMEM((cp, groups, rows, HEAD_DIM), bf16),
                pltpu.VMEM((cp, groups, HEAD_DIM, rows), bf16),
                pltpu.VMEM((cp, 1, rows), jnp.int32),
                pltpu.VMEM((rows, HEAD_DIM), jnp.int32),
                pltpu.VMEM((rows, rows), f32),
                pltpu.VMEM((cp, rows, HEAD_DIM), bf16),
                pltpu.VMEM((rows, rows // 2), f32),
                pltpu.VMEM((rows, rows // 2), f32),
                pltpu.VMEM((2, rows, groups * HEAD_DIM), f32),
                pltpu.VMEM((heads, rows, 2 * HEAD_DIM), bf16),
                pltpu.VMEM((rows, tp * head_cols), bf16),
                pltpu.VMEM((rows, y_cols), bf16),
                pltpu.VMEM((head_cols // cp // 2, y_cols), bf16),
                pltpu.VMEM((head_cols // cp // 2, y_cols), bf16),
                pltpu.VMEM((PAIR, 1, rows), f32),
                pltpu.VMEM((PAIR, 1, rows), f32),
                pltpu.VMEM((PAIR, HEAD_DIM, rows), f32),
                pltpu.SemaphoreType.DMA((19,)),
                pltpu.SemaphoreType.DMA((5,)),
                pltpu.SemaphoreType.DMA((40,)),
            ],
            compiler_params=pltpu.CompilerParams(collective_id=0, has_side_effects=True, vmem_limit_bytes=56 * 2**20),
        )(x_loc, seg_loc.reshape(1, rows), w_query, w_key, w_value, w_out)

    return jax.shard_map(local_attention, mesh=mesh, in_specs=(P(('dp', 'cp'), None), P(('dp', 'cp')), P(None, 'tp'), P(None, 'tp'), P(None, 'tp'), P('tp', None)), out_specs=P(('dp', 'cp'), None), check_vma=False)
```

```python
import functools

import jax
import jax.numpy as jnp
from jax import lax
from jax.experimental import pallas as pl
from jax.experimental.pallas import tpu as pltpu
from jax.sharding import PartitionSpec as P

HEAD_DIM = 128
COL_TILE = 256
DEPTH_CUTS = 4
PAIR = 2
MESH = pl.DeviceIdType.MESH
SCALE = HEAD_DIM**-0.5 * 1.4426950408889634
NEG_INF = float("-inf")


class Sems:
    def __init__(self, ref):
        self.ref, self.names = ref, {}

    def __getitem__(self, name):
        return self.ref.at[self.names.setdefault(name, len(self.names))]


def kernel(tp, cp, x_hbm, seg_in, wq_hbm, wk_hbm, wv_hbm, wo_hbm, y_ref,
           x_v, wkv_v, wq_v, w_full, k_all, vt_all, segs, seg_col, bias, k_mask, s_even, s_odd, kv_acc, q_v, o_all, y_own, relay_up, relay_dn,
           m_s, l_s, acc_s, load_sem, send_sem, recv_sem):
    t, p = lax.axis_index("tp"), lax.axis_index("cp")
    chips = cp // 2
    col, core = p // 2, lax.rem(p, 2)
    up, dn, far = lax.rem(t + 1, tp), lax.rem(t + tp - 1, tp), lax.rem(t + 2, tp)
    right_chip, left_chip, far_chip = lax.rem(col + 1, chips), lax.rem(col + chips - 1, chips), lax.rem(col + 2, chips)
    right, left, across = right_chip * 2 + core, left_chip * 2 + core, far_chip * 2 + core
    mate = col * 2 + 1 - core
    mate_right, mate_left, mate_across = right_chip * 2 + 1 - core, left_chip * 2 + 1 - core, far_chip * 2 + 1 - core

    rows = x_v.shape[0]
    heads = q_v.shape[0]
    groups = k_all.shape[1]
    per_group = heads // groups
    head_cols = heads * HEAD_DIM
    y_cols = w_full.shape[1]
    piece = head_cols // cp
    half = piece // 2
    half_rows = rows // 2

    loads, sends, recvs = Sems(load_sem), Sems(send_sem), Sems(recv_sem)

    def at_tp(i):
        return {"tp": i, "cp": p}

    def at_cp(i):
        return {"tp": t, "cp": i}

    def send(src, dst, name, dev, kind):
        pltpu.make_async_remote_copy(src_ref=src, dst_ref=dst, send_sem=sends[kind], recv_sem=recvs[name],
                                     device_id=dev, device_id_type=MESH).start()

    def waiter(ref, kind, name):
        return pltpu.make_async_remote_copy(src_ref=ref, dst_ref=ref, send_sem=sends[kind], recv_sem=recvs[name],
                                            device_id=at_cp(p), device_id_type=MESH)

    def arrived(ref, name):
        waiter(ref, "kv", name).wait_recv()

    def sent(ref, kind):
        waiter(ref, kind, "seg").wait_send()

    def heads_of(n):
        return o_all.at[:, :n * HEAD_DIM]

    def rows_of(n):
        return w_full.at[:n]

    def load(src, dst, name):
        c = pltpu.make_async_copy(src, dst, loads[name])
        c.start()
        return c

    depth = x_v.shape[1] // DEPTH_CUTS
    cuts = [pl.ds(i * depth, depth) for i in range(DEPTH_CUTS)]
    load_kv = [(load(x_hbm.at[:, c], x_v.at[:, c], ("x", i)), load(wk_hbm.at[c, :], wkv_v.at[0, c, :], ("k", i)),
                load(wv_hbm.at[c, :], wkv_v.at[1, c, :], ("v", i))) for i, c in enumerate(cuts)]
    q_tiles = head_cols // COL_TILE

    barrier = pltpu.get_barrier_semaphore()
    peers = [at_tp(up), at_tp(dn)] + [at_cp(lax.rem(p + k, cp)) for k in range(1, cp)]
    for dev in peers:
        pl.semaphore_signal(barrier, inc=1, device_id=dev, device_id_type=MESH)

    def w_rows(owner, share, start, count):
        return w_full.at[pl.ds(pl.multiple_of(owner * head_cols + share * piece + start, 16), count), :]

    def w_src(dest, share, start, count):
        return wo_hbm.at[pl.ds(pl.multiple_of(share * piece + start, 16), count),
                         pl.ds(pl.multiple_of(dest * y_cols, 128), y_cols)]

    def w_to_relay():
        send(w_src(far, p, 0, half), relay_up, "w_relay", at_tp(up), "w")
        send(w_src(far, p, half, half), relay_dn, "w_relay", at_tp(dn), "w")

    def w_direct(share, count, name):
        send(w_src(up, share, 0, count), w_rows(t, share, 0, count), name, at_tp(up), "w")
        send(w_src(dn, share, 0, count), w_rows(t, share, 0, count), name, at_tp(dn), "w")

    def w_relay():
        arrived(rows_of(2 * half), "w_relay")
        send(relay_up, w_rows(dn, p, 0, half), "w_own", at_tp(up), "w")
        send(relay_dn, w_rows(up, p, half, half), "w_own", at_tp(dn), "w")

    class Ring:
        def __init__(self, tag, kind, parts, wait_of, shared=None):
            self.tag, self.kind, self.parts, self.wait_of = tag, kind, parts, wait_of
            self.shared = shared or tag

        def pass_on(self, owner, k, name, dev):
            for ref in self.parts(owner, k):
                send(ref, ref, name, dev, self.kind)

        def start(self):
            self.pass_on(p, None, (self.tag, "L"), at_cp(right))
            self.pass_on(p, None, (self.tag, "R"), at_cp(left))
            self.pass_on(p, None, (self.shared, "M"), at_cp(mate))

        def near(self):
            arrived(self.wait_of(1), (self.tag, "L"))
            self.pass_on(left, 0, (self.shared, "F"), at_cp(right))
            self.pass_on(left, None, (self.shared, "M"), at_cp(mate))
            arrived(self.wait_of(1), (self.tag, "R"))
            self.pass_on(right, 1, (self.shared, "F"), at_cp(left))
            self.pass_on(right, None, (self.shared, "M"), at_cp(mate))

        def far(self, name):
            self.pass_on(across, None, (self.shared, name), at_cp(mate))

    def kv_ring(g):
        def parts(owner, k):
            both = [k_all.at[owner, g], vt_all.at[owner, g]]
            return both if k is None else both[k:k + 1]
        return Ring(("kv", g), "kv", parts, lambda n: heads_of(2 * n))

    def w_ring(j):
        owner = lax.rem(t + j, tp)
        first = 0 if j == 2 else half

        def parts(share, k):
            if k is None:
                return [w_rows(owner, share, 0, piece)]
            count = (piece - first) // 2
            return [w_rows(owner, share, first + k * count, count)]
        return Ring(("w", j), "w", parts, lambda n: rows_of(piece * n), "w")

    def project(w_ref, store):
        @pl.loop(0, rows // half_rows)
        def _(i):
            r = pl.ds(pl.multiple_of(i * half_rows, 16), half_rows)
            store(r, jnp.dot(x_v[r, :], w_ref[...], preferred_element_type=jnp.float32))

    def store_k(r, val):
        for g in range(groups):
            k_all[p, g, r, :] = val[:, g * HEAD_DIM:(g + 1) * HEAD_DIM].astype(jnp.bfloat16)

    def store_v(r, val):
        for g in range(groups):
            vt_all[p, g, :, r] = val[:, g * HEAD_DIM:(g + 1) * HEAD_DIM].T.astype(jnp.bfloat16)

    for i, c in enumerate(cuts):
        with jax.named_scope("wait_x"):
            for copy in load_kv[i]:
                copy.wait()
        with jax.named_scope("proj_kv"):
            @pl.loop(0, 2)
            def _(half_of):
                r = pl.ds(pl.multiple_of(half_of * half_rows, 16), half_rows)
                for kind, store in enumerate((store_k, store_v)):
                    val = jnp.dot(x_v[r, c], wkv_v[kind, c, :], preferred_element_type=jnp.float32)
                    if i > 0:
                        val += kv_acc[kind, r, :]
                    if i + 1 < len(cuts):
                        kv_acc[kind, r, :] = val
                    else:
                        store(r, val)
        if i == 1:
            load_q = [load(wq_hbm.at[:, pl.ds(n * COL_TILE, COL_TILE)], wq_v.at[n], ("q", n)) for n in range(q_tiles)]
        if i + 2 == len(cuts):
            pl.semaphore_wait(barrier, len(peers))

            for k in range(1, cp):
                send(seg_in, segs.at[p], "seg", at_cp(lax.rem(p + k, cp)), "seg")
            load_seg = load(seg_in, segs.at[p], "seg")


            w_to_relay()
    kv = [kv_ring(g) for g in range(groups)]
    w = [w_ring(j) for j in range(1, tp)]
    kv[0].start()
    own_cols = pl.ds(pl.multiple_of(t * y_cols, 128), y_cols)
    load_o = load(wo_hbm.at[:, own_cols], w_full.at[pl.ds(pl.multiple_of(t * head_cols, 128), head_cols), :], "o")

    def q_tile(n):
        load_q[n].wait()

        def store(r, val):
            for k in range(COL_TILE // HEAD_DIM):
                q_v[n * (COL_TILE // HEAD_DIM) + k, r, :HEAD_DIM] = val[:, k * HEAD_DIM:(k + 1) * HEAD_DIM].astype(jnp.bfloat16)
        with jax.named_scope(f"q{n}"):
            project(wq_v.at[n], store)

    def wide(v, n):
        return jnp.concatenate([v] * (n // v.shape[1]), axis=1)

    lane = lax.broadcasted_iota(jnp.int32, (rows, HEAD_DIM), 1)
    first_doc = seg_in[:, :1]

    def set_bias():
        seg_col[...] = jnp.broadcast_to(seg_in[...], (HEAD_DIM, rows)).T

        @pl.loop(0, rows // HEAD_DIM)
        def _(i):
            r = pl.ds(pl.multiple_of(i * HEAD_DIM, HEAD_DIM), HEAD_DIM)
            allowed = wide(seg_col[r, :], rows) == seg_in[...]
            allowed &= (lax.broadcasted_iota(jnp.int32, (HEAD_DIM, rows), 0) + i * HEAD_DIM
                        <= lax.broadcasted_iota(jnp.int32, (HEAD_DIM, rows), 1))
            bias[r, :] = jnp.where(allowed, 0.0, NEG_INF)

    def set_mask(block):
        of_key = jnp.broadcast_to(segs[block], (HEAD_DIM, rows)).T
        shut = (of_key != first_doc) & (lane == 0)
        k_mask[block] = jnp.where(shut, NEG_INF, 0.0).astype(jnp.bfloat16)

    def visit(pair, blocks, diagonal=False):
        g = pair * PAIR // per_group
        units = [(block, h, i) for block in blocks for h in range(PAIR) for i in range(2)]
        scratch = [s_even, s_odd]

        def keys(i):
            return half_rows if diagonal and i == 0 else rows

        def scores(n):
            block, h, i = units[n]
            c = slice(i * half_rows, (i + 1) * half_rows)
            q = q_v[pair * PAIR + h, c, :]
            k = k_all[block, g, :keys(i), :]
            if diagonal:
                s = lax.dot_general(k, q[:, :HEAD_DIM], (((1,), (1,)), ((), ())), preferred_element_type=jnp.float32)
                s += bias[:keys(i), c]
            else:
                k = jnp.concatenate([k, k_mask[block]], axis=1)
                s = lax.dot_general(k, q, (((1,), (1,)), ((), ())), preferred_element_type=jnp.float32)
            scratch[n % 2][:keys(i), :] = s
            return jnp.max(s, axis=0, keepdims=True)

        def absorb(n, top):
            block, h, i = units[n]
            c = slice(i * half_rows, (i + 1) * half_rows)
            if diagonal:
                new_max = shift = top
            else:
                in_first = seg_in[:, c] == first_doc
                old_max = m_s[h, :, c]
                new_max = jnp.where(in_first, jnp.maximum(old_max, top), old_max)
                shift = jnp.where(in_first, new_max, -NEG_INF)
            prob = jnp.exp2(scratch[n % 2][:keys(i), :] * SCALE - shift * SCALE)
            total = jnp.sum(prob, axis=0, keepdims=True)
            out = jnp.dot(vt_all[block, g, :, :keys(i)], prob.astype(jnp.bfloat16), preferred_element_type=jnp.float32)
            if not diagonal:
                rescale = jnp.exp2((old_max - new_max) * SCALE)
                total += l_s[h, :, c] * rescale
                out += acc_s[h, :, c] * rescale
            m_s[h, :, c] = new_max
            l_s[h, :, c] = total
            acc_s[h, :, c] = out

        top = scores(0)
        for n in range(len(units)):
            ahead = scores(n + 1) if n + 1 < len(units) else None
            absorb(n, top)
            top = ahead

    def visit_mate(pair):
        @pl.when(core == 1)
        def _():
            if pair == 0:
                set_mask(mate)
            visit(pair, [mate])

    def visit_chips(pair, count, chip_of):
        @pl.loop(0, count)
        def _(i):
            chip = chip_of(i)

            @pl.when(chip < col)
            def _():
                if pair == 0:
                    set_mask(chip * 2)
                    set_mask(chip * 2 + 1)
                visit(pair, [chip * 2, chip * 2 + 1])

    def visit_sides(pair):
        visit_chips(pair, 2, lambda i: jnp.where(i == 0, left_chip, right_chip))

    def visit_near(pair):
        visit_mate(pair)
        visit_sides(pair)

    def visit_far(pair):
        visit_chips(pair, 1, lambda i: far_chip + i)

    def visit_all(pair):
        visit_mate(pair)
        visit_chips(pair, chips, lambda i: i)

    def o_cols(owner, h):
        return o_all.at[:, pl.ds(pl.multiple_of(owner * head_cols + h * HEAD_DIM, 128), HEAD_DIM)]

    def o_finish(pair):
        for k in range(PAIR):
            h = pair * PAIR + k
            o_all[:, pl.ds(pl.multiple_of(t * head_cols + h * HEAD_DIM, 128), HEAD_DIM)] = (
                acc_s[k] / l_s[k]).T.astype(jnp.bfloat16)
            send(o_cols(t, h), o_cols(t, h), ("o", pair), at_tp(up), "o")
            send(o_cols(t, h), o_cols(t, h), ("o", pair), at_tp(dn), "o")

    q_v[:, :, HEAD_DIM:] = jnp.where(lax.broadcasted_iota(jnp.int32, (heads, rows, HEAD_DIM), 2) == 0, 1.0, 0.0).astype(jnp.bfloat16)
    scope = jax.named_scope

    def o_relay_pair(pair):
        with scope(f"o_relay{pair}"):
            arrived(heads_of(2 * PAIR), ("o", pair))
            for h in range(pair * PAIR, (pair + 1) * PAIR):
                if h % 2 == 0:
                    send(o_cols(dn, h), o_cols(dn, h), "o_far", at_tp(up), "o")
                else:
                    send(o_cols(up, h), o_cols(up, h), "o_far", at_tp(dn), "o")

    q_tile(0)
    w_direct(p, piece, "w_own")
    with scope("diag0"):
        set_bias()
        visit(0, [p], diagonal=True)
    q_tile(1)
    q_tile(2)
    with scope("kv0_near"):
        kv[0].near()
    with scope("w_relay"):
        w_relay()
        w_direct(across, half, "w_extra")
    with scope("kv0_mate"):
        load_seg.wait()
        arrived(segs.at[:cp - 1], "seg")
        arrived(heads_of(6), (kv[0].tag, "M"))
        kv[1].start()
    with scope("near0"):
        visit_near(0)
    with scope("kv0_far"):
        arrived(heads_of(2), (kv[0].tag, "F"))
        kv[0].far("MF")
    q_tile(3)
    with scope("kv0_mf"):
        arrived(heads_of(2), (kv[0].tag, "MF"))
    with scope("far0"):
        visit_far(0)
    with scope("o_fin0"):
        o_finish(0)
    with scope("diag1"):
        visit(1, [p], diagonal=True)
    with scope("kv1_near"):
        kv[1].near()
    with scope("w_tp_own"):
        arrived(rows_of(3 * piece), "w_own")
        w[0].start()
    with scope("pair1"):
        visit_all(1)
        o_finish(1)
    with scope("kv1_far"):
        arrived(heads_of(2), (kv[1].tag, "F"))
        kv[1].far("MF")
        w[1].start()
        w[2].start()
    with scope("diag2"):
        visit(2, [p], diagonal=True)
    with scope("kv1_mate"):
        arrived(heads_of(6), (kv[1].tag, "M"))
        arrived(heads_of(2), (kv[1].tag, "MF"))
    with scope("pair2"):
        visit_mate(2)
        visit_far(2)
    o_relay_pair(0)
    with scope("sides2"):
        visit_sides(2)
        o_finish(2)
    with scope("w1_near"):
        w[0].near()
    with scope("pair3"):
        visit(3, [p], diagonal=True)
        visit_mate(3)
        visit_far(3)
    o_relay_pair(1)
    with scope("sides3"):
        visit_sides(3)
        o_finish(3)
    with scope("w2_near"):
        w[1].near()
    o_relay_pair(2)
    with scope("w3_near"):
        w[2].near()
    o_relay_pair(3)
    with scope("w_far"):
        arrived(rows_of(2 * half), "w_extra")
        arrived(rows_of(2 * half + piece), ("w", "F"))
        for part in w:
            part.far("M")
    with scope("w_mate"):
        arrived(rows_of(12 * piece), ("w", "M"))
    with scope("o_far"):
        arrived(heads_of(heads), "o_far")
        load_o.wait()

    def y_at(owner, n, k):
        return y_ref.at[pl.ds(k * half_rows, half_rows),
                        pl.ds(pl.multiple_of(owner * y_cols + n * COL_TILE, 128), COL_TILE)]

    tiles = [(n, k) for n in range(y_cols // COL_TILE) for k in range(2)]
    copies = []
    for n, k in tiles:
        r, c = slice(k * half_rows, (k + 1) * half_rows), slice(n * COL_TILE, (n + 1) * COL_TILE)
        with scope("y_mm"):
            y_own[r, c] = jnp.dot(o_all[r, :], w_full[:, c], preferred_element_type=jnp.float32).astype(jnp.bfloat16)
        send(y_own.at[r, c], y_at(t, n, k), ("y", n, k) if k == 0 else "y_rest", at_tp(up), "y")
        send(y_own.at[r, c], y_at(t, n, k), ("y", n, k) if k == 1 else "y_rest", at_tp(dn), "y")
        copies.append(load(y_own.at[r, c], y_at(t, n, k), "y"))
    for n, k in tiles:
        with scope(f"y_relay{n}"):
            arrived(y_at(dn, n, k), ("y", n, k))
            if k == 0:
                send(y_at(dn, n, k), y_at(dn, n, k), "y_far", at_tp(up), "y")
            else:
                send(y_at(up, n, k), y_at(up, n, k), "y_far", at_tp(dn), "y")
    with scope("y_rest"):
        arrived(y_own, "y_rest")
    with scope("y_far"):
        arrived(y_own, "y_far")
    with scope("drain"):
        pltpu.make_async_copy(y_own, y_own, loads["y"]).wait()
        sent(segs.at[:cp - 1], "seg")
        sent(heads_of(14 * groups), "kv")
        sent(rows_of(5 * piece + (tp - 1) * 6 * piece + 2 * half + piece), "w")
        sent(heads_of(3 * heads), "o")
        sent(y_ref.at[:, :3 * y_cols], "y")


def solution(mesh):
    tp, cp = mesh.shape["tp"], mesh.shape["cp"]

    def local_attention(x_loc, seg_loc, w_query, w_key, w_value, w_out):
        rows, width = x_loc.shape
        heads = w_query.shape[1] // HEAD_DIM
        groups = w_key.shape[1] // HEAD_DIM
        head_cols = heads * HEAD_DIM
        y_cols = width // tp
        bf16, f32 = jnp.bfloat16, jnp.float32
        hbm = pl.BlockSpec(memory_space=pl.ANY)
        return pl.pallas_call(
            functools.partial(kernel, tp, cp),
            out_shape=pltpu.VMEM((rows, width), bf16),
            in_specs=[hbm, pl.BlockSpec(memory_space=pltpu.VMEM), hbm, hbm, hbm, hbm],
            out_specs=hbm,
            scratch_shapes=[
                pltpu.VMEM((rows, width), bf16),
                pltpu.VMEM((2, width, groups * HEAD_DIM), bf16),
                pltpu.VMEM((head_cols // COL_TILE, width, COL_TILE), bf16),
                pltpu.VMEM((tp * head_cols, y_cols), bf16),
                pltpu.VMEM((cp, groups, rows, HEAD_DIM), bf16),
                pltpu.VMEM((cp, groups, HEAD_DIM, rows), bf16),
                pltpu.VMEM((cp, 1, rows), jnp.int32),
                pltpu.VMEM((rows, HEAD_DIM), jnp.int32),
                pltpu.VMEM((rows, rows), f32),
                pltpu.VMEM((cp, rows, HEAD_DIM), bf16),
                pltpu.VMEM((rows, rows // 2), f32),
                pltpu.VMEM((rows, rows // 2), f32),
                pltpu.VMEM((2, rows, groups * HEAD_DIM), f32),
                pltpu.VMEM((heads, rows, 2 * HEAD_DIM), bf16),
                pltpu.VMEM((rows, tp * head_cols), bf16),
                pltpu.VMEM((rows, y_cols), bf16),
                pltpu.VMEM((head_cols // cp // 2, y_cols), bf16),
                pltpu.VMEM((head_cols // cp // 2, y_cols), bf16),
                pltpu.VMEM((PAIR, 1, rows), f32),
                pltpu.VMEM((PAIR, 1, rows), f32),
                pltpu.VMEM((PAIR, HEAD_DIM, rows), f32),
                pltpu.SemaphoreType.DMA((19,)),
                pltpu.SemaphoreType.DMA((5,)),
                pltpu.SemaphoreType.DMA((40,)),
            ],
            compiler_params=pltpu.CompilerParams(collective_id=0, has_side_effects=True, vmem_limit_bytes=56 * 2**20),
        )(x_loc, seg_loc.reshape(1, rows), w_query, w_key, w_value, w_out)

    return jax.shard_map(local_attention, mesh=mesh, in_specs=(P(('dp', 'cp'), None), P(('dp', 'cp')), P(None, 'tp'), P(None, 'tp'), P(None, 'tp'), P('tp', None)), out_specs=P(('dp', 'cp'), None), check_vma=False)
```

```python
import functools

import jax
import jax.numpy as jnp
from jax import lax
from jax.experimental import pallas as pl
from jax.experimental.pallas import tpu as pltpu
from jax.sharding import PartitionSpec as P

HEAD_DIM = 128
COL_TILE = 256
DEPTH_CUTS = 4
PAIR = 2
MESH = pl.DeviceIdType.MESH
SCALE = HEAD_DIM**-0.5 * 1.4426950408889634
NEG_INF = float("-inf")


class Sems:
    def __init__(self, ref):
        self.ref, self.names = ref, {}

    def __getitem__(self, name):
        return self.ref.at[self.names.setdefault(name, len(self.names))]


def kernel(tp, cp, x_hbm, seg_in, wq_hbm, wk_hbm, wv_hbm, wo_hbm, y_ref,
           x_v, wkv_v, wq_v, w_full, k_all, vt_all, segs, seg_col, bias, k_mask, s_even, s_odd, kv_acc, q_v, o_all, y_own, relay_up, relay_dn,
           m_s, l_s, acc_s, load_sem, send_sem, recv_sem):
    t, p = lax.axis_index("tp"), lax.axis_index("cp")
    chips = cp // 2
    col, core = p // 2, lax.rem(p, 2)
    up, dn, far = lax.rem(t + 1, tp), lax.rem(t + tp - 1, tp), lax.rem(t + 2, tp)
    right_chip, left_chip, far_chip = lax.rem(col + 1, chips), lax.rem(col + chips - 1, chips), lax.rem(col + 2, chips)
    right, left, across = right_chip * 2 + core, left_chip * 2 + core, far_chip * 2 + core
    mate = col * 2 + 1 - core
    mate_right, mate_left, mate_across = right_chip * 2 + 1 - core, left_chip * 2 + 1 - core, far_chip * 2 + 1 - core

    rows = x_v.shape[0]
    heads = q_v.shape[0]
    groups = k_all.shape[1]
    per_group = heads // groups
    head_cols = heads * HEAD_DIM
    y_cols = w_full.shape[1]
    piece = head_cols // cp
    half = piece // 2
    half_rows = rows // 2

    loads, sends, recvs = Sems(load_sem), Sems(send_sem), Sems(recv_sem)

    def at_tp(i):
        return {"tp": i, "cp": p}

    def at_cp(i):
        return {"tp": t, "cp": i}

    def send(src, dst, name, dev, kind):
        pltpu.make_async_remote_copy(src_ref=src, dst_ref=dst, send_sem=sends[kind], recv_sem=recvs[name],
                                     device_id=dev, device_id_type=MESH).start()

    def waiter(ref, kind, name):
        return pltpu.make_async_remote_copy(src_ref=ref, dst_ref=ref, send_sem=sends[kind], recv_sem=recvs[name],
                                            device_id=at_cp(p), device_id_type=MESH)

    def arrived(ref, name):
        waiter(ref, "kv", name).wait_recv()

    def sent(ref, kind):
        waiter(ref, kind, "seg").wait_send()

    def heads_of(n):
        return o_all.at[:, :n * HEAD_DIM]

    def rows_of(n):
        return w_full.at[:n]

    def load(src, dst, name):
        c = pltpu.make_async_copy(src, dst, loads[name])
        c.start()
        return c

    depth = x_v.shape[1] // DEPTH_CUTS
    cuts = [pl.ds(i * depth, depth) for i in range(DEPTH_CUTS)]
    load_kv = [(load(x_hbm.at[:, c], x_v.at[:, c], ("x", i)), load(wk_hbm.at[c, :], wkv_v.at[0, c, :], ("k", i)),
                load(wv_hbm.at[c, :], wkv_v.at[1, c, :], ("v", i))) for i, c in enumerate(cuts)]
    q_tiles = head_cols // COL_TILE

    barrier = pltpu.get_barrier_semaphore()
    peers = [at_tp(up), at_tp(dn)] + [at_cp(lax.rem(p + k, cp)) for k in range(1, cp)]
    for dev in peers:
        pl.semaphore_signal(barrier, inc=1, device_id=dev, device_id_type=MESH)

    def w_rows(owner, share, start, count):
        return w_full.at[pl.ds(pl.multiple_of(owner * head_cols + share * piece + start, 16), count), :]

    def w_src(dest, share, start, count):
        return wo_hbm.at[pl.ds(pl.multiple_of(share * piece + start, 16), count),
                         pl.ds(pl.multiple_of(dest * y_cols, 128), y_cols)]

    def w_to_relay():
        send(w_src(far, p, 0, half), relay_up, "w_relay", at_tp(up), "w")
        send(w_src(far, p, half, half), relay_dn, "w_relay", at_tp(dn), "w")

    def w_direct(share, count, name):
        send(w_src(up, share, 0, count), w_rows(t, share, 0, count), name, at_tp(up), "w")
        send(w_src(dn, share, 0, count), w_rows(t, share, 0, count), name, at_tp(dn), "w")

    def w_relay():
        arrived(rows_of(2 * half), "w_relay")
        send(relay_up, w_rows(dn, p, 0, half), "w_own", at_tp(up), "w")
        send(relay_dn, w_rows(up, p, half, half), "w_own", at_tp(dn), "w")

    class Ring:
        def __init__(self, tag, kind, parts, wait_of, shared=None):
            self.tag, self.kind, self.parts, self.wait_of = tag, kind, parts, wait_of
            self.shared = shared or tag

        def pass_on(self, owner, k, name, dev):
            for ref in self.parts(owner, k):
                send(ref, ref, name, dev, self.kind)

        def start(self):
            self.pass_on(p, None, (self.tag, "L"), at_cp(right))
            self.pass_on(p, None, (self.tag, "R"), at_cp(left))
            self.pass_on(p, None, (self.shared, "M"), at_cp(mate))

        def near(self):
            arrived(self.wait_of(1), (self.tag, "L"))
            self.pass_on(left, 0, (self.shared, "F"), at_cp(right))
            self.pass_on(left, None, (self.shared, "M"), at_cp(mate))
            arrived(self.wait_of(1), (self.tag, "R"))
            self.pass_on(right, 1, (self.shared, "F"), at_cp(left))
            self.pass_on(right, None, (self.shared, "M"), at_cp(mate))

        def far(self, name):
            self.pass_on(across, None, (self.shared, name), at_cp(mate))

    def kv_ring(g):
        def parts(owner, k):
            both = [k_all.at[owner, g], vt_all.at[owner, g]]
            return both if k is None else both[k:k + 1]
        return Ring(("kv", g), "kv", parts, lambda n: heads_of(2 * n))

    def w_ring(j):
        owner = lax.rem(t + j, tp)
        first = 0 if j == 2 else half

        def parts(share, k):
            if k is None:
                return [w_rows(owner, share, 0, piece)]
            count = (piece - first) // 2
            return [w_rows(owner, share, first + k * count, count)]
        return Ring(("w", j), "w", parts, lambda n: rows_of(piece * n), "w")

    def project(w_ref, store):
        @pl.loop(0, rows // half_rows)
        def _(i):
            r = pl.ds(pl.multiple_of(i * half_rows, 16), half_rows)
            store(r, jnp.dot(x_v[r, :], w_ref[...], preferred_element_type=jnp.float32))

    def store_k(r, val):
        for g in range(groups):
            k_all[p, g, r, :] = val[:, g * HEAD_DIM:(g + 1) * HEAD_DIM].astype(jnp.bfloat16)

    def store_v(r, val):
        for g in range(groups):
            vt_all[p, g, :, r] = val[:, g * HEAD_DIM:(g + 1) * HEAD_DIM].T.astype(jnp.bfloat16)

    for i, c in enumerate(cuts):
        with jax.named_scope("wait_x"):
            for copy in load_kv[i]:
                copy.wait()
        with jax.named_scope("proj_kv"):
            @pl.loop(0, 2)
            def _(half_of):
                r = pl.ds(pl.multiple_of(half_of * half_rows, 16), half_rows)
                for kind, store in enumerate((store_k, store_v)):
                    val = jnp.dot(x_v[r, c], wkv_v[kind, c, :], preferred_element_type=jnp.float32)
                    if i > 0:
                        val += kv_acc[kind, r, :]
                    if i + 1 < len(cuts):
                        kv_acc[kind, r, :] = val
                    else:
                        store(r, val)
        if i == 1:
            load_q = [load(wq_hbm.at[:, pl.ds(n * COL_TILE, COL_TILE)], wq_v.at[n], ("q", n)) for n in range(q_tiles)]
        if i + 2 == len(cuts):
            pl.semaphore_wait(barrier, len(peers))

            for k in range(1, cp):
                send(seg_in, segs.at[p], "seg", at_cp(lax.rem(p + k, cp)), "seg")
            load_seg = load(seg_in, segs.at[p], "seg")


            w_to_relay()
    kv = [kv_ring(g) for g in range(groups)]
    w = [w_ring(j) for j in range(1, tp)]
    kv[0].start()
    own_cols = pl.ds(pl.multiple_of(t * y_cols, 128), y_cols)
    load_o = load(wo_hbm.at[:, own_cols], w_full.at[pl.ds(pl.multiple_of(t * head_cols, 128), head_cols), :], "o")

    def q_tile(n):
        load_q[n].wait()

        def store(r, val):
            for k in range(COL_TILE // HEAD_DIM):
                q_v[n * (COL_TILE // HEAD_DIM) + k, r, :HEAD_DIM] = val[:, k * HEAD_DIM:(k + 1) * HEAD_DIM].astype(jnp.bfloat16)
        with jax.named_scope(f"q{n}"):
            project(wq_v.at[n], store)

    def wide(v, n):
        return jnp.concatenate([v] * (n // v.shape[1]), axis=1)

    lane = lax.broadcasted_iota(jnp.int32, (rows, HEAD_DIM), 1)
    first_doc = seg_in[:, :1]

    def set_bias():
        seg_col[...] = jnp.broadcast_to(seg_in[...], (HEAD_DIM, rows)).T

        @pl.loop(0, rows // HEAD_DIM)
        def _(i):
            r = pl.ds(pl.multiple_of(i * HEAD_DIM, HEAD_DIM), HEAD_DIM)
            allowed = wide(seg_col[r, :], rows) == seg_in[...]
            allowed &= (lax.broadcasted_iota(jnp.int32, (HEAD_DIM, rows), 0) + i * HEAD_DIM
                        <= lax.broadcasted_iota(jnp.int32, (HEAD_DIM, rows), 1))
            bias[r, :] = jnp.where(allowed, 0.0, NEG_INF)

    def set_mask(block):
        of_key = jnp.broadcast_to(segs[block], (HEAD_DIM, rows)).T
        shut = (of_key != first_doc) & (lane == 0)
        k_mask[block] = jnp.where(shut, NEG_INF, 0.0).astype(jnp.bfloat16)

    def visit(pair, blocks, diagonal=False):
        g = pair * PAIR // per_group
        units = [(block, h, i) for block in blocks for h in range(PAIR) for i in range(2)]
        scratch = [s_even, s_odd]

        def keys(i):
            return half_rows if diagonal and i == 0 else rows

        def scores(n):
            block, h, i = units[n]
            c = slice(i * half_rows, (i + 1) * half_rows)
            q = q_v[pair * PAIR + h, c, :]
            k = k_all[block, g, :keys(i), :]
            if diagonal:
                s = lax.dot_general(k, q[:, :HEAD_DIM], (((1,), (1,)), ((), ())), preferred_element_type=jnp.float32)
                s += bias[:keys(i), c]
            else:
                k = jnp.concatenate([k, k_mask[block]], axis=1)
                s = lax.dot_general(k, q, (((1,), (1,)), ((), ())), preferred_element_type=jnp.float32)
            scratch[n % 2][:keys(i), :] = s
            return jnp.max(s, axis=0, keepdims=True)

        def absorb(n, top):
            block, h, i = units[n]
            c = slice(i * half_rows, (i + 1) * half_rows)
            if diagonal:
                new_max = shift = top
            else:
                in_first = seg_in[:, c] == first_doc
                old_max = m_s[h, :, c]
                new_max = jnp.where(in_first, jnp.maximum(old_max, top), old_max)
                shift = jnp.where(in_first, new_max, -NEG_INF)
            prob = jnp.exp2(scratch[n % 2][:keys(i), :] * SCALE - shift * SCALE)
            total = jnp.sum(prob, axis=0, keepdims=True)
            out = jnp.dot(vt_all[block, g, :, :keys(i)], prob.astype(jnp.bfloat16), preferred_element_type=jnp.float32)
            if not diagonal:
                rescale = jnp.exp2((old_max - new_max) * SCALE)
                total += l_s[h, :, c] * rescale
                out += acc_s[h, :, c] * rescale
            m_s[h, :, c] = new_max
            l_s[h, :, c] = total
            acc_s[h, :, c] = out

        top = scores(0)
        for n in range(len(units)):
            ahead = scores(n + 1) if n + 1 < len(units) else None
            absorb(n, top)
            top = ahead

    def visit_mate(pair):
        @pl.when(core == 1)
        def _():
            if pair == 0:
                set_mask(mate)
            visit(pair, [mate])

    def visit_chips(pair, count, chip_of):
        @pl.loop(0, count)
        def _(i):
            chip = chip_of(i)

            @pl.when(chip < col)
            def _():
                if pair == 0:
                    set_mask(chip * 2)
                    set_mask(chip * 2 + 1)
                visit(pair, [chip * 2, chip * 2 + 1])

    def visit_near(pair):
        visit_mate(pair)
        visit_chips(pair, 2, lambda i: jnp.where(i == 0, left_chip, right_chip))

    def visit_far(pair):
        visit_chips(pair, 1, lambda i: far_chip + i)

    def visit_all(pair):
        visit_mate(pair)
        visit_chips(pair, chips, lambda i: i)

    def o_cols(owner, h):
        return o_all.at[:, pl.ds(pl.multiple_of(owner * head_cols + h * HEAD_DIM, 128), HEAD_DIM)]

    def o_finish(pair):
        for k in range(PAIR):
            h = pair * PAIR + k
            o_all[:, pl.ds(pl.multiple_of(t * head_cols + h * HEAD_DIM, 128), HEAD_DIM)] = (
                acc_s[k] / l_s[k]).T.astype(jnp.bfloat16)
            send(o_cols(t, h), o_cols(t, h), ("o", pair), at_tp(up), "o")
            send(o_cols(t, h), o_cols(t, h), ("o", pair), at_tp(dn), "o")

    q_v[:, :, HEAD_DIM:] = jnp.where(lax.broadcasted_iota(jnp.int32, (heads, rows, HEAD_DIM), 2) == 0, 1.0, 0.0).astype(jnp.bfloat16)
    scope = jax.named_scope

    def o_relay_pair(pair):
        with scope(f"o_relay{pair}"):
            arrived(heads_of(2 * PAIR), ("o", pair))
            for h in range(pair * PAIR, (pair + 1) * PAIR):
                if h % 2 == 0:
                    send(o_cols(dn, h), o_cols(dn, h), "o_far", at_tp(up), "o")
                else:
                    send(o_cols(up, h), o_cols(up, h), "o_far", at_tp(dn), "o")

    q_tile(0)
    w_direct(p, piece, "w_own")
    with scope("diag0"):
        set_bias()
        visit(0, [p], diagonal=True)
    q_tile(1)
    q_tile(2)
    with scope("kv0_near"):
        kv[0].near()
    with scope("w_relay"):
        w_relay()
        w_direct(across, half, "w_extra")
    with scope("kv0_mate"):
        load_seg.wait()
        arrived(segs.at[:cp - 1], "seg")
        arrived(heads_of(6), (kv[0].tag, "M"))
        kv[1].start()
    with scope("near0"):
        visit_near(0)
    with scope("kv0_far"):
        arrived(heads_of(2), (kv[0].tag, "F"))
        kv[0].far("MF")
    q_tile(3)
    with scope("kv0_mf"):
        arrived(heads_of(2), (kv[0].tag, "MF"))
    with scope("far0"):
        visit_far(0)
    with scope("o_fin0"):
        o_finish(0)
    with scope("diag1"):
        visit(1, [p], diagonal=True)
    with scope("kv1_near"):
        kv[1].near()
    with scope("w_tp_own"):
        arrived(rows_of(3 * piece), "w_own")
        w[0].start()
    with scope("pair1"):
        visit_all(1)
        o_finish(1)
    with scope("kv1_far"):
        arrived(heads_of(2), (kv[1].tag, "F"))
        kv[1].far("MF")
        w[1].start()
        w[2].start()
    o_relay_pair(0)
    with scope("diag2"):
        visit(2, [p], diagonal=True)
    with scope("kv1_mate"):
        arrived(heads_of(6), (kv[1].tag, "M"))
        arrived(heads_of(2), (kv[1].tag, "MF"))
    with scope("pair2"):
        visit_all(2)
        o_finish(2)
    with scope("w1_near"):
        w[0].near()
    o_relay_pair(1)
    with scope("pair3"):
        visit(3, [p], diagonal=True)
        visit_all(3)
        o_finish(3)
    with scope("w2_near"):
        w[1].near()
    o_relay_pair(2)
    with scope("w3_near"):
        w[2].near()
    o_relay_pair(3)
    with scope("w_far"):
        arrived(rows_of(2 * half), "w_extra")
        arrived(rows_of(2 * half + piece), ("w", "F"))
        for part in w:
            part.far("M")
    with scope("w_mate"):
        arrived(rows_of(12 * piece), ("w", "M"))
    with scope("o_far"):
        arrived(heads_of(heads), "o_far")
        load_o.wait()

    def y_at(owner, n, k):
        return y_ref.at[pl.ds(k * half_rows, half_rows),
                        pl.ds(pl.multiple_of(owner * y_cols + n * COL_TILE, 128), COL_TILE)]

    tiles = [(n, k) for n in range(y_cols // COL_TILE) for k in range(2)]
    copies = []
    for n, k in tiles:
        r, c = slice(k * half_rows, (k + 1) * half_rows), slice(n * COL_TILE, (n + 1) * COL_TILE)
        with scope("y_mm"):
            y_own[r, c] = jnp.dot(o_all[r, :], w_full[:, c], preferred_element_type=jnp.float32).astype(jnp.bfloat16)
        send(y_own.at[r, c], y_at(t, n, k), ("y", n, k) if k == 0 else "y_rest", at_tp(up), "y")
        send(y_own.at[r, c], y_at(t, n, k), ("y", n, k) if k == 1 else "y_rest", at_tp(dn), "y")
        copies.append(load(y_own.at[r, c], y_at(t, n, k), "y"))
    for n, k in tiles:
        with scope(f"y_relay{n}"):
            arrived(y_at(dn, n, k), ("y", n, k))
            if k == 0:
                send(y_at(dn, n, k), y_at(dn, n, k), "y_far", at_tp(up), "y")
            else:
                send(y_at(up, n, k), y_at(up, n, k), "y_far", at_tp(dn), "y")
    with scope("y_rest"):
        arrived(y_own, "y_rest")
    with scope("y_far"):
        arrived(y_own, "y_far")
    with scope("drain"):
        pltpu.make_async_copy(y_own, y_own, loads["y"]).wait()
        sent(segs.at[:cp - 1], "seg")
        sent(heads_of(14 * groups), "kv")
        sent(rows_of(5 * piece + (tp - 1) * 6 * piece + 2 * half + piece), "w")
        sent(heads_of(3 * heads), "o")
        sent(y_ref.at[:, :3 * y_cols], "y")


def solution(mesh):
    tp, cp = mesh.shape["tp"], mesh.shape["cp"]

    def local_attention(x_loc, seg_loc, w_query, w_key, w_value, w_out):
        rows, width = x_loc.shape
        heads = w_query.shape[1] // HEAD_DIM
        groups = w_key.shape[1] // HEAD_DIM
        head_cols = heads * HEAD_DIM
        y_cols = width // tp
        bf16, f32 = jnp.bfloat16, jnp.float32
        hbm = pl.BlockSpec(memory_space=pl.ANY)
        return pl.pallas_call(
            functools.partial(kernel, tp, cp),
            out_shape=pltpu.VMEM((rows, width), bf16),
            in_specs=[hbm, pl.BlockSpec(memory_space=pltpu.VMEM), hbm, hbm, hbm, hbm],
            out_specs=hbm,
            scratch_shapes=[
                pltpu.VMEM((rows, width), bf16),
                pltpu.VMEM((2, width, groups * HEAD_DIM), bf16),
                pltpu.VMEM((head_cols // COL_TILE, width, COL_TILE), bf16),
                pltpu.VMEM((tp * head_cols, y_cols), bf16),
                pltpu.VMEM((cp, groups, rows, HEAD_DIM), bf16),
                pltpu.VMEM((cp, groups, HEAD_DIM, rows), bf16),
                pltpu.VMEM((cp, 1, rows), jnp.int32),
                pltpu.VMEM((rows, HEAD_DIM), jnp.int32),
                pltpu.VMEM((rows, rows), f32),
                pltpu.VMEM((cp, rows, HEAD_DIM), bf16),
                pltpu.VMEM((rows, rows // 2), f32),
                pltpu.VMEM((rows, rows // 2), f32),
                pltpu.VMEM((2, rows, groups * HEAD_DIM), f32),
                pltpu.VMEM((heads, rows, 2 * HEAD_DIM), bf16),
                pltpu.VMEM((rows, tp * head_cols), bf16),
                pltpu.VMEM((rows, y_cols), bf16),
                pltpu.VMEM((head_cols // cp // 2, y_cols), bf16),
                pltpu.VMEM((head_cols // cp // 2, y_cols), bf16),
                pltpu.VMEM((PAIR, 1, rows), f32),
                pltpu.VMEM((PAIR, 1, rows), f32),
                pltpu.VMEM((PAIR, HEAD_DIM, rows), f32),
                pltpu.SemaphoreType.DMA((19,)),
                pltpu.SemaphoreType.DMA((5,)),
                pltpu.SemaphoreType.DMA((40,)),
            ],
            compiler_params=pltpu.CompilerParams(collective_id=0, has_side_effects=True, vmem_limit_bytes=56 * 2**20),
        )(x_loc, seg_loc.reshape(1, rows), w_query, w_key, w_value, w_out)

    return jax.shard_map(local_attention, mesh=mesh, in_specs=(P(('dp', 'cp'), None), P(('dp', 'cp')), P(None, 'tp'), P(None, 'tp'), P(None, 'tp'), P('tp', None)), out_specs=P(('dp', 'cp'), None), check_vma=False)
```
